32 devices in a mesh: seq: 8 (over z, y), ch: 4 (over x, core).
Axes of the slice: x: 2, y: 2, z: 4, core: 2. Of those that a mesh axis runs over, the one named last changes fastest.
Arguments:
- inputs: bfloat16 [8192, 768], P(('seq', 'ch')), may hold values from -6 to 6
- gain_one: float32 [768], replicated, may hold values from 0.5 to 1.5
- shift_one: float32 [768], replicated, may hold values from -1.5 to 1.5
- conv_weight: bfloat16 [3, 768, 384], P(None, None, 'ch'), may hold values from -0.125 to 0.125
- gain_two: float32 [384], P('ch'), may hold values from 0.5 to 1.5
- shift_two: float32 [384], P('ch'), may hold values from -1.5 to 1.5
- mix_weight: bfloat16 [384, 768], P('ch'), may hold values from -0.3125 to 0.3125
- head_weight: bfloat16 [768, 6956], P('ch'), may hold values from -0.21875 to 0.21875
- head_bias: float32 [6956], replicated, may hold values from -2 to 2
- species: int32 [8], replicated, may hold values from 0 to 1, as said below
- counts: int32 [8192, 5313], P(('seq', 'ch')), may hold values from 0 to 3
Outputs:
- outputs: bfloat16 [8192, 768], P(('seq', 'ch'))
- input_grad: float32 [8192, 768], P(('seq', 'ch'))
- gain_one_grad: float32 [768], replicated
- shift_one_grad: float32 [768], replicated
- conv_weight_grad: float32 [3, 768, 384], P(None, None, 'ch')
- gain_two_grad: float32 [384], P('ch')
- shift_two_grad: float32 [384], P('ch')
- mix_weight_grad: float32 [384, 768], P('ch')
- head_weight_grad: float32 [768, 6956], P(('seq', 'ch'))
- head_bias_grad: float32 [6956], replicated
The draws below stay inside these ranges and needn't reach their ends.
Inputs may be any that keep to these rules, and one draw needn't show every extreme that they name: Each window holds one species, given by species[w]; both species occur in every draw.
All inputs are finite; a program needn't handle non-finite values.
Results may differ from the reference program's by a relative error of at most 0.014.
Values may be sent and summed in bfloat16 or wider, within the bound.
A program may use at most 192 MiB of HBM per device.

```python
import jax
import jax.numpy as jnp
from jax import lax

D = 768
H = 384
HUMAN = 5313
MOUSE = 1643
DILATION_STEP = 11
TAPS = 3
WINDOW_BINS = 1024
SHIFT = 512
BINS = 8192
NWIN = 8
TRACKS = 6956


def draw_species(key, part):
    order = jax.random.permutation(key, NWIN)
    return (jnp.mod(order, 3) == 0).astype(jnp.int32)


def plant(entries, stream_key, least, largest):
    index_at = [jax.random.randint(jax.random.fold_in(stream_key, axis), (), 0, length) for axis, length in enumerate(entries.shape)]
    main_axis = entries.shape.index(max(entries.shape))
    neighbour = index_at[:main_axis] + [(index_at[main_axis] + 1) % entries.shape[main_axis]] + index_at[main_axis + 1:]
    return entries.at[tuple(index_at)].set(least).at[tuple(neighbour)].set(largest)


def raised(array, own_key, source, target, shards_of, factor):
    def block_of(axis_at):
        return (jnp.arange(array.shape[axis_at]) // (array.shape[axis_at] // shards_of)).reshape((-1,) + (1,) * (array.ndim - 1 - axis_at))

    first = jax.random.permutation(own_key, shards_of)[block_of(target)]
    second = (block_of(target) + shards_of // 2) % shards_of
    return jnp.where((block_of(source) == first) | (block_of(source) == second), factor * array, array)


def steps_of(own_key, shape, pieces, low, largest):
    loudness = 1.0
    for axis_at, shards_of in pieces:
        heights = jax.random.uniform(jax.random.fold_in(jax.random.fold_in(own_key, 6), axis_at), (shards_of,), jnp.float32, low / len(pieces), largest / len(pieces))
        loudness = loudness * jnp.repeat(jnp.exp(heights), shape[axis_at] // shards_of).reshape((-1,) + (1,) * (len(shape) - 1 - axis_at))
    return loudness


def noise(own_key, shape, scale, reach, split=(), dtype=jnp.bfloat16):
    values = jax.random.normal(own_key, shape, jnp.float32) * scale
    if len(split) > 0:
        values = steps_of(own_key, shape, split, -0.22, 0.18) * values
    return jnp.clip(values, min=-reach, max=reach).astype(dtype)


def bell_draw_with(rng, extent, scale, bound, split, heavy, held_as=jnp.bfloat16):
    result = scale * jax.random.normal(rng, extent, jnp.float32)
    if split:
        result = result * steps_of(rng, extent, split, -0.22, 0.18)
    return jnp.clip(raised(result, jax.random.fold_in(rng, 3), *heavy), -bound, bound).astype(held_as)


def setup_inputs(seed: int = 0) -> dict:
    key_of = jax.random.split(jax.random.key(seed), 12)
    inputs = bell_draw_with(key_of[0], (BINS, D), 1.0, 6.0, ((0, 32),), (0, 1, 32, 2.75))
    gain_one = jnp.clip(1.0 + 0.1 * jax.random.normal(key_of[1], (D,), jnp.float32), 0.5, 1.5)
    shift_one = noise(key_of[2], (D,), 0.3, 1.5, (), jnp.float32)
    conv_weight = noise(key_of[3], (TAPS, D, H), (TAPS * D) ** -0.5, 0.125, ((2, 4),))
    gain_two = jnp.clip(1.0 + 0.1 * jax.random.normal(key_of[4], (H,), jnp.float32), 0.5, 1.5)
    shift_two = noise(key_of[5], (H,), 0.3, 1.5, ((0, 4),), jnp.float32)
    mix_weight = noise(key_of[6], (H, D), H ** -0.5, 0.3125, ((0, 4),))
    head_weight = noise(key_of[7], (D, TRACKS), D ** -0.5, 0.21875, ((0, 4),))
    head_bias = noise(key_of[8], (TRACKS,), 0.5, 2.0, (), jnp.float32)
    species = draw_species(jax.random.fold_in(key_of[11], 71), 0)
    counts = plant(jax.random.randint(key_of[10], (BINS, HUMAN), 0, 4), jax.random.fold_in(key_of[10], 1), 0, 3).astype(jnp.int32)
    return {"inputs": inputs, "gain_one": gain_one, "shift_one": shift_one, "conv_weight": conv_weight, "gain_two": gain_two, "shift_two": shift_two, "mix_weight": mix_weight, "head_weight": head_weight, "head_bias": head_bias, "species": species, "counts": counts}


norm_eps = 1e-05
highest = lax.Precision.HIGHEST

@jax.custom_vjp
def low(v):
    return lax.optimization_barrier(v.astype(jnp.bfloat16)).astype(jnp.float32)

@jax.custom_vjp
def low_back(v):
    return v

def low_keep(v):
    return (low(v), None)

def low_pass(kept, grad):
    return (grad,)

def back_keep(v):
    return (v, None)

def back_low(kept, grad):
    return (low(grad),)
low.defvjp(low_keep, low_pass)
low_back.defvjp(back_keep, back_low)

def batch_norm(values, gain, offset):
    center = lax.optimization_barrier(jnp.mean(values, 0))
    deviation = values - center
    spread = lax.optimization_barrier(jnp.mean(deviation * deviation, 0))
    return deviation * lax.rsqrt(spread + norm_eps) * gain + offset

def poisson_sum(logits, target):
    rate = jax.nn.softplus(logits)
    return jnp.sum(rate - target * jnp.log(rate))

def reference(inputs, gain_one, shift_one, conv_weight, gain_two, shift_two, mix_weight, head_weight, head_bias, species, counts):
    targets = jnp.roll(counts.astype(jnp.float32), -SHIFT, 0).reshape(NWIN, WINDOW_BINS, HUMAN)

    def forward(input_f, gain_a, shift_a, conv_f, gain_b, shift_b, mix_f, head_f, bias_f):
        act_one = low(jax.nn.gelu(batch_norm(input_f, gain_a, shift_a)))
        window_list = jnp.roll(act_one, -SHIFT, 0).reshape(NWIN, WINDOW_BINS, D)
        padded_input = jnp.pad(window_list, ((0, 0), (DILATION_STEP, DILATION_STEP), (0, 0)))
        conv_sum = jnp.zeros((NWIN, WINDOW_BINS, H), jnp.float32)
        for kernel_tap_index in range(TAPS):
            part = padded_input[:, kernel_tap_index * DILATION_STEP:kernel_tap_index * DILATION_STEP + WINDOW_BINS]
            conv_sum = conv_sum + jnp.einsum('nwi,ij->nwj', part, conv_f[kernel_tap_index], precision=highest)
        conv_out = low_back(jnp.roll(conv_sum.reshape(BINS, H), SHIFT, 0))
        act_two = low(jax.nn.gelu(batch_norm(conv_out, gain_b, shift_b)))
        branch = low_back(jnp.dot(act_two, mix_f, precision=highest, preferred_element_type=jnp.float32))
        outputs = low(input_f + branch)
        feats = jnp.roll(outputs, -SHIFT, 0).reshape(NWIN, WINDOW_BINS, D)

        def window_loss(total, item):
            feat, target, kind = item

            def human_loss(unused):
                logits = low_back(jnp.dot(feat, head_f[:, :HUMAN], precision=highest, preferred_element_type=jnp.float32) + bias_f[:HUMAN])
                return poisson_sum(logits, target)

            def mouse_loss(unused):
                logits = low_back(jnp.dot(feat, head_f[:, HUMAN:], precision=highest, preferred_element_type=jnp.float32) + bias_f[HUMAN:])
                return poisson_sum(logits, target[:, :MOUSE])
            return (total + lax.cond(kind == 0, human_loss, mouse_loss, 0), None)
        loss, _ = lax.scan(jax.checkpoint(window_loss), jnp.zeros((), jnp.float32), (feats, targets, species))
        return (loss, outputs)
    primals = (inputs.astype(jnp.float32), gain_one, shift_one, conv_weight.astype(jnp.float32), gain_two, shift_two, mix_weight.astype(jnp.float32), head_weight.astype(jnp.float32), head_bias)
    loss, pullback, outputs = jax.vjp(forward, *primals, has_aux=True)
    grads = pullback(jnp.ones((), jnp.float32))
    return (outputs.astype(jnp.bfloat16), grads[0], grads[1], grads[2], grads[3], grads[4], grads[5], grads[6], grads[7], grads[8])
```

```python
import functools
import math
import types

import jax
import jax.numpy as jnp
from jax import lax
from jax.experimental import pallas as pl
from jax.experimental.pallas import tpu as pltpu
from jax.sharding import PartitionSpec as P

HUMAN = 5313
MOUSE = 1643
STEP = 11
TAPS = 3
WINDOW_BINS = 1024
SHIFT = 512
EPS = 1e-05

LANES = 128
NCHUNK = 7
HW = 384
MW = 128
CW = HW + MW
HALF_H = NCHUNK * HW
HALF_M = NCHUNK * MW
HALO = 32
EDGE = 16
MESH = pl.DeviceIdType.MESH
F32 = jnp.float32
BF16 = jnp.bfloat16
K0 = math.sqrt(2.0 / math.pi)
K1 = K0 * 0.044715


def nn(a, b):
    return lax.dot_general(a, b, (((1,), (0,)), ((), ())), preferred_element_type=F32)


def nt(a, b):
    return lax.dot_general(a, b, (((1,), (1,)), ((), ())), preferred_element_type=F32)


def gelu(v):
    return 0.5 * v * (1.0 + jnp.tanh(v * (K0 + K1 * (v * v))))


def gelu_slope(v):
    v2 = v * v
    th = jnp.tanh(v * (K0 + K1 * v2))
    return 0.5 * (1.0 + th) + 0.5 * v * (1.0 - th * th) * (K0 + 3.0 * K1 * v2)


def poisson_grad(logits, target):
    t = jnp.exp(-jnp.abs(logits))
    series = t * (1.0 - t * (0.5 - t * (1.0 / 3.0 - t * 0.25)))
    rate = jnp.maximum(logits, 0.0) + jnp.where(t < 0.015625, series, jnp.log(1.0 + t))
    sig = jnp.where(logits >= 0.0, 1.0, t) / (1.0 + t)
    return sig * (1.0 - target / rate)


def take(ref, sem):
    pltpu.make_async_copy(ref, ref, sem).wait()


def kernel_body(seqs, chs, fused, names, *refs):
    r = types.SimpleNamespace(**dict(zip(names, refs, strict=True)))
    r.sa, r.sb, r.ba, r.bb = ([getattr(r, f"{n}{i}") for i in range(4)] for n in ("sa", "sb", "ba", "bb"))
    S, C = seqs, chs
    s = lax.axis_index("seq")
    c = lax.axis_index("ch")
    xi = c // 2
    k = lax.rem(c, 2)
    other = c + 1 - 2 * k
    xnb = lax.rem(c + 2, C)
    xo = 1 - xi
    y = lax.rem(s, 2)
    z = s // 2
    ynb = s + 1 - 2 * y
    zb = lax.rem(z, 2)
    znb = s + 2 - 4 * zb
    dnb = znb + 1 - 2 * y
    q = lax.rem(s, 4)
    q_y = q + 1 - 2 * y
    q_z = q + 2 - 4 * zb
    q_d = q_z + 1 - 2 * y
    rows, width = r.x.shape
    n_dev = S * C
    total_bins = rows * n_dev
    inv_bins = 1.0 / total_bins
    me = s * C + c
    left = lax.rem(me + n_dev - 1, n_dev)
    right = lax.rem(me + 1, n_dev)
    left_dev = (left // C, lax.rem(left, C))
    right_dev = (right // C, lax.rem(right, C))
    row0 = me * rows
    window = lax.rem(row0 + total_bins - SHIFT, total_bins) // WINDOW_BINS
    left_same = lax.rem(row0 + total_bins - 1 + total_bins - SHIFT, total_bins) // WINDOW_BINS == window
    right_same = lax.rem(row0 + rows + total_bins - SHIFT, total_bins) // WINDOW_BINS == window
    mine_h = r.flags[0] == 0
    x_h = r.flags[1] == 0
    y_h = r.flags[2] == 0
    hp = C * LANES

    def put(src, dst, send, recv, dev):
        pltpu.make_async_remote_copy(
            src_ref=src, dst_ref=dst, send_sem=send, recv_sem=recv, device_id=dev, device_id_type=MESH
        ).start()

    barrier = pltpu.get_barrier_semaphore()

    def greet(dev):
        pl.semaphore_signal(barrier, inc=1, device_id=dev, device_id_type=MESH)

    for i in range(1, C):
        greet((s, lax.rem(c + i, C)))

    @pl.loop(1, S)
    def _(i):
        greet((lax.rem(s + i, S), c))

    greet(left_dev)
    greet(right_dev)

    W, TG = r.wbuf, r.tgb

    def human_at(half, j):
        return pl.ds(pl.multiple_of(half * HALF_H + j * HW, LANES), HW)

    def mouse_at(half, j):
        return pl.ds(pl.multiple_of(half * HALF_M + j * MW, LANES), MW)

    @pl.loop(0, NCHUNK)
    def _(j):
        pltpu.make_async_copy(r.hw.at[:, :, human_at(k, j)], W.at[j, c, :, :, pl.ds(0, HW)], r.wl.at[j]).start()
        pltpu.make_async_copy(r.mw.at[:, :, mouse_at(k, j)], W.at[j, c, :, :, pl.ds(HW, MW)], r.wl.at[j]).start()
        pltpu.make_async_copy(r.tg.at[:, human_at(k, j)], TG.at[j, k, :, pl.ds(0, HW)], r.tl.at[j]).start()
        pltpu.make_async_copy(r.tg.at[:, mouse_at(k, j)], TG.at[j, k, :, pl.ds(HW, MW)], r.tl.at[j]).start()

    CM = r.cmf
    cr = r.cm.shape[1]
    pltpu.make_async_copy(r.cm, CM.at[:, c, pl.ds(0, cr)], r.cml).start()
    for t in range(4):
        for p in range(C):
            CM[t, p, cr:LANES, :] = jnp.zeros((LANES - cr, width), BF16)

    def spread(ref, vecs):
        n = vecs[0].shape[1] // LANES
        for i, v in enumerate(vecs):
            for t in range(n):
                ref[i * n + t : i * n + t + 1, :] = v[:, t * LANES : (t + 1) * LANES]
        if ref.shape[0] > n * len(vecs):
            ref[n * len(vecs) :, :] = jnp.zeros((ref.shape[0] - n * len(vecs), LANES), F32)

    def collect(v, n):
        m = n // LANES
        return [jnp.concatenate([v[i * m + t : i * m + t + 1, :] for t in range(m)], axis=1) for i in range(2)]

    def sum_start(i):
        src, bufs = r.sa[i], r.ba[i]
        for p in range(1, C):
            put(src, bufs.at[c], r.ars.at[2 * i], r.arr.at[2 * i], (s, lax.rem(c + p, C)))
        bufs[c] = src[...]

    def sum_middle(i):
        src, bufs, far = r.sb[i], r.ba[i], r.bb[i]
        take(bufs.at[pl.ds(0, C - 1)], r.arr.at[2 * i])
        v = bufs[0]
        for p in range(1, C):
            v = v + bufs[p]
        src[...] = v

        @pl.loop(1, S)
        def _(p):
            put(src, far.at[s], r.ars.at[2 * i + 1], r.arr.at[2 * i + 1], (lax.rem(s + p, S), c))

        far[s] = v

    def sum_end(i, n):
        far = r.bb[i]
        take(far.at[pl.ds(0, S - 1)], r.arr.at[2 * i + 1])
        if S <= 8:
            v = far[0]
            for p in range(1, S):
                v = v + far[p]
        else:
            v = lax.fori_loop(1, S, lambda p, a: a + far[p], far[0])
        return v, *collect(v, n)

    BLK = 32

    def block(i, shift=0):
        return pl.ds(pl.multiple_of(i * BLK + shift, 16), BLK)

    def row_sums(terms):
        def step(i, carry):
            return tuple(a + jnp.sum(t, 0, keepdims=True) for a, t in zip(carry, terms(i), strict=True))

        return step

    zero_w = jnp.zeros((1, width), F32)

    def x_terms(i):
        v = r.x[block(i), :].astype(F32)
        return v, v * v

    s1, q1 = lax.fori_loop(0, rows // BLK, row_sums(x_terms), (zero_w, zero_w))
    spread(r.sa0, (s1, q1))

    pl.semaphore_wait(barrier, C - 1 + S - 1 + 2)

    sum_start(0)
    put(r.x.at[pl.ds(rows - HALO, HALO)], r.xl, r.hs.at[0], r.hr.at[0], right_dev)
    put(r.x.at[pl.ds(0, HALO)], r.xr, r.hs.at[1], r.hr.at[1], left_dev)
    half_w = width // 2
    put(r.cm.at[q], CM.at[q, c, pl.ds(0, cr)], r.cms.at[0], r.cmr.at[0], (s, xnb))
    put(
        r.cm.at[q_d, :, pl.ds(0, half_w)],
        CM.at[q_d, c, pl.ds(0, cr), pl.ds(0, half_w)],
        r.cms.at[1],
        r.cmr.at[1],
        (s, xnb),
    )
    put(r.cm, CM.at[:, c, pl.ds(0, cr)], r.cms.at[2], r.cmr.at[2], (s, other))
    for p in range(1, C):
        put(r.gs2, r.gsb.at[c], r.gss, r.gsr, (s, lax.rem(c + p, C)))
    r.gsb[c] = r.gs2[...]

    @pl.loop(0, NCHUNK)
    def _(j):
        put(
            r.hw.at[:, :, human_at(1 - k, j)], W.at[j, c, :, :, pl.ds(0, HW)],
            r.wps, r.wp.at[j], (s, other),
        )
        put(
            r.mw.at[:, :, mouse_at(1 - k, j)], W.at[j, c, :, :, pl.ds(HW, MW)],
            r.wps, r.wp.at[j], (s, other),
        )
        put(
            r.tg.at[:, human_at(1 - k, j)], TG.at[j, k, :, pl.ds(0, HW)],
            r.tps, r.tp.at[j], (s, other),
        )
        put(
            r.tg.at[:, mouse_at(1 - k, j)], TG.at[j, k, :, pl.ds(HW, MW)],
            r.tps, r.tp.at[j], (s, other),
        )

    HALFC = CW // 2

    def heads_along_x(j):
        for h in range(2):
            dev = (s, xo * 2 + h)
            hc = pl.multiple_of(h * HALF_H + j * HW, LANES)
            put(r.hw.at[q, :, human_at(h, j)], W.at[j, c, q, :, pl.ds(0, HW)], r.wxs, r.wx.at[j], dev)
            put(r.mw.at[q, :, mouse_at(h, j)], W.at[j, c, q, :, pl.ds(HW, MW)], r.wxs, r.wx.at[j], dev)
            put(
                r.hw.at[q_d, :, pl.ds(hc, HALFC)], W.at[j, c, q_d, :, pl.ds(0, HALFC)],
                r.wxs, r.wx.at[j], dev,
            )

    def relay_heads(j):
        take(W.at[j, pl.ds(0, 3), 0], r.wx.at[j])
        far = pl.ds(xo * 2, 2)
        put(W.at[j, far, q], W.at[j, far, q], r.wrs.at[0], r.wy.at[j], (ynb, c))
        put(W.at[j, far, q], W.at[j, far, q], r.wrs.at[1], r.wz.at[j], (znb, c))
        put(
            W.at[j, far, q, :, pl.ds(HALFC, HALFC)], W.at[j, far, q, :, pl.ds(HALFC, HALFC)],
            r.wrs.at[2], r.wd.at[j], (dnb, c),
        )

    for j in range(2):
        heads_along_x(j)

    sum_middle(0)
    _, t1, u1 = sum_end(0, width)
    mean1 = t1 * inv_bins
    scale1 = lax.rsqrt(u1 * inv_bins - mean1 * mean1 + EPS)
    gain1 = r.gs1[0:1, :]
    off1 = r.gs1[1:2, :]

    take(CM.at[0, 0, pl.ds(0, cr)], r.cmr.at[0])
    put(CM.at[q, xnb, pl.ds(0, cr)], CM.at[q, xnb, pl.ds(0, cr)], r.cms.at[3], r.cmr.at[3], (ynb, c))
    put(CM.at[q, xnb, pl.ds(0, cr)], CM.at[q, xnb, pl.ds(0, cr)], r.cms.at[4], r.cmr.at[4], (znb, c))
    second = pl.ds(half_w, half_w)
    put(
        CM.at[q, xnb, pl.ds(0, cr), second], CM.at[q, xnb, pl.ds(0, cr), second],
        r.cms.at[5], r.cmr.at[5], (dnb, c),
    )

    A = r.act

    def normed1_of(v):
        return (v - mean1) * scale1

    def act_rows(v):
        return gelu(normed1_of(v.astype(F32)) * gain1 + off1)

    @pl.loop(0, rows // BLK)
    def _(i):
        at = pl.multiple_of(i * BLK, BLK)
        A[pl.ds(at + HALO, BLK), :] = act_rows(r.x[pl.ds(at, BLK), :]).astype(BF16)

    take(r.xl, r.hr.at[0])
    A[0:HALO, :] = jnp.where(left_same, act_rows(r.xl[...]), 0.0).astype(BF16)
    take(r.xr, r.hr.at[1])
    A[rows + HALO : rows + 2 * HALO, :] = jnp.where(right_same, act_rows(r.xr[...]), 0.0).astype(BF16)

    take(CM.at[0, 0, pl.ds(0, cr), pl.ds(0, half_w)], r.cmr.at[1])
    take(CM.at[0, 0, pl.ds(0, cr)], r.cmr.at[3])
    take(CM.at[0, 0, pl.ds(0, cr)], r.cmr.at[4])
    take(CM.at[0, 0, pl.ds(0, cr), pl.ds(0, half_w)], r.cmr.at[5])
    put(CM.at[:, xnb, pl.ds(0, cr)], CM.at[:, xnb, pl.ds(0, cr)], r.cms.at[6], r.cmr.at[6], (s, other))
    take(r.cm, r.cml)
    take(CM.at[:, 0, pl.ds(0, cr)], r.cmr.at[2])
    take(CM.at[:, 0, pl.ds(0, cr)], r.cmr.at[6])

    ext = rows + 2 * EDGE
    PR = r.prod
    for t in range(TAPS):
        PR[t] = nt(A[...], CM[t].reshape(hp, width))
    CV = r.cv
    lo = HALO - EDGE
    CV[...] = (
        PR[0, lo - STEP : lo - STEP + ext, :] + PR[1, lo : lo + ext, :] + PR[2, lo + STEP : lo + STEP + ext, :]
    )
    zero_h = jnp.zeros((1, hp), F32)

    def c_terms(i):
        v = CV[block(i, EDGE), :]
        return v, v * v

    s2, q2 = lax.fori_loop(0, rows // BLK, row_sums(c_terms), (zero_h, zero_h))
    spread(r.sa1, (s2, q2))
    sum_start(1)
    for j in range(2, NCHUNK):
        heads_along_x(j)
    put(A.at[pl.ds(lo, ext)], r.actx, r.as_, r.ar_, (s, xnb))
    sum_middle(1)
    relay_heads(0)
    relay_heads(1)
    _, t2, u2 = sum_end(1, hp)
    mean2 = t2 * inv_bins
    scale2 = lax.rsqrt(u2 * inv_bins - mean2 * mean2 + EPS)
    take(r.gsb.at[pl.ds(0, C - 1)], r.gsr)
    gain2 = jnp.concatenate([r.gsb[p, 0:1, :] for p in range(C)], axis=1)
    off2 = jnp.concatenate([r.gsb[p, 1:2, :] for p in range(C)], axis=1)

    def normed2_of(v):
        return (v - mean2) * scale2

    A2 = r.a2

    @pl.loop(0, rows // BLK)
    def _(i):
        at = pl.multiple_of(i * BLK, BLK)
        v = normed2_of(CV[pl.ds(at + EDGE, BLK), :])
        A2[pl.ds(at, BLK), :] = gelu(v * gain2 + off2).astype(BF16)

    O = r.ob
    mixf = CM[3].reshape(hp, width)
    outputs = (r.x[...].astype(F32) + nn(A2[...], mixf)).astype(BF16)
    O[k] = outputs
    r.out[...] = outputs
    put(O.at[k], O.at[k], r.os, r.orr, (s, other))
    relay_heads(2)
    r.a2t[...] = A2[...].T
    take(O.at[0], r.orr)
    OT = r.ot
    OT[...] = O[...].reshape(2 * rows, width).T
    GO = r.go
    GO[...] = jnp.zeros(GO.shape, F32)
    WG, GL = r.wg, r.gl
    LG = r.lg
    HB = r.hbs
    HB[...] = jnp.zeros(HB.shape, F32)
    if fused:
        Z = S // 2

    def weight_chunk_send(j, along_x):
        if along_x:
            put(WG.at[j, :, :, xo], r.r1.at[j], r.s1.at[j], r.g1r.at[j], (s, xnb))
        else:
            put(WG.at[j, :, 1 - y], r.r1.at[j], r.s1.at[j], r.g1r.at[j], (ynb, c))

    def heads_chunk(j):
        take(W.at[j, 0], r.wl.at[j])
        take(W.at[j, 0], r.wp.at[j])
        take(W.at[j, pl.ds(0, 2), 0], r.wy.at[j])
        take(W.at[j, pl.ds(0, 2), 0], r.wz.at[j])
        take(W.at[j, pl.ds(0, 2), 0, :, pl.ds(0, HALFC)], r.wd.at[j])
        take(TG.at[j, 0], r.tl.at[j])
        take(TG.at[j, 0], r.tp.at[j])
        w = r.wsel
        w[:, MW:] = W[j, :, :, :, MW:HW].reshape(width, HW - MW)
        w[:, :MW] = jnp.where(
            mine_h, W[j, :, :, :, 0:MW].reshape(width, MW), W[j, :, :, :, HW:CW].reshape(width, MW)
        )
        wv = w[...]
        LG[...] = nn(O[...].reshape(2 * rows, width), wv)
        valid_n = jnp.where(mine_h, HUMAN - (k * HALF_H + j * HW), jnp.minimum(MOUSE - (k * HALF_M + j * MW), MW))
        valid = lax.broadcasted_iota(jnp.int32, (1, HW), 1) < valid_n
        brow = r.bias[pl.ds(k * NCHUNK + j, 1), :]
        bias = jnp.concatenate([jnp.where(mine_h, brow[:, :MW], brow[:, HW:]), brow[:, MW:HW]], axis=1)
        per = rows // BLK

        def step(i, acc):
            at = pl.multiple_of(i * BLK, BLK)
            core = i // per
            ta = pl.ds(pl.multiple_of(lax.rem(i, per) * BLK, BLK), BLK)
            lg = LG[pl.ds(at, BLK), :] + bias
            tg = TG[j, core, ta, :].astype(F32)
            tgt = jnp.concatenate([jnp.where(mine_h, tg[:, :MW], tg[:, HW:]), tg[:, MW:HW]], axis=1)
            g = jnp.where(valid, poisson_grad(lg, tgt), 0.0).astype(BF16)
            GL[pl.ds(at, BLK), :] = g
            return acc + jnp.sum(g.astype(F32), 0, keepdims=True)

        bsum = lax.fori_loop(0, 2 * per, step, jnp.zeros((1, HW), F32))
        bsum = jnp.concatenate([jnp.where(mine_h, bsum, 0.0), jnp.where(mine_h, 0.0, bsum[:, :MW])], axis=1)
        HB[...] = jnp.where(lax.broadcasted_iota(jnp.int32, HB.shape, 0) == j, bsum, HB[...])
        g = GL[...]
        GO[...] += nt(g, wv).reshape(GO.shape)
        WG[j] = nn(OT[...], g).astype(BF16).reshape(WG.shape[1:])

    @pl.loop(0, NCHUNK)
    def _(j):
        heads_chunk(j)

        @pl.when(j + 3 < NCHUNK)
        def _():
            relay_heads(j + 3)

    put(GO.at[1 - k], r.gor, r.gos, r.gorr, (s, other))
    put(r.hbs, r.hbx, r.hbsem.at[0], r.hbrem.at[0], (s, xnb))

    if fused:
        A1, R1, R2, R3 = r.acc1, r.r1, r.r2, r.r3
        two = A1.shape[3]
        own = two // 2

        def along_x(j):
            return j % 2 == 1

        def rs1(j):
            take(R1.at[j], r.g1r.at[j])
            ax = along_x(j)
            got_h = x_h if ax else y_h

            def step(i, _):
                zz, b = i // 2, lax.rem(i, 2)
                a = (WG[j, zz, b, xi] if ax else WG[j, zz, y, b]).astype(F32)
                g = R1[j, zz, b].astype(F32)
                A1[j, zz, b, :, 0:HW] = (jnp.where(mine_h, a, 0.0) + jnp.where(got_h, g, 0.0)).astype(BF16)
                A1[j, zz, b, :, HW:CW] = (
                    jnp.where(mine_h, 0.0, a[:, :MW]) + jnp.where(got_h, 0.0, g[:, :MW])
                ).astype(BF16)
                return 0

            lax.fori_loop(0, S, step, 0)
            if ax:
                put(A1.at[j, :, 1 - y], R2.at[j], r.s2.at[j], r.g2r.at[j], (ynb, c))
            else:
                put(A1.at[j, :, xo], R2.at[j], r.s2.at[j], r.g2r.at[j], (s, xnb))

        def rs2(j):
            take(R2.at[j], r.g2r.at[j])
            b = y if along_x(j) else xi
            for zz in range(Z):
                R2[j, zz] = (A1[j, zz, b].astype(F32) + R2[j, zz].astype(F32)).astype(BF16)
            R3[j, z] = R2[j, z]
            for p in range(1, Z):
                to = lax.rem(z + p, Z)
                put(R2.at[j, to], R3.at[j, z], r.s3.at[j], r.g3r.at[j], (to * 2 + y, c))

        def rs3(j):
            take(R3.at[j, pl.ds(0, Z - 1)], r.g3r.at[j])
            v = R3[j, 0].astype(F32)
            for p in range(1, Z):
                v = v + R3[j, p].astype(F32)
            r.fin[j] = v.reshape(2, own, CW)
            put(r.fin.at[j, 1 - k], r.fr.at[j], r.s4.at[j], r.g4r.at[j], (s, other))
            r.hg[k, j] = r.fin[j, k]

        def rs4(j):
            take(r.fr.at[j], r.g4r.at[j])
            r.hg[1 - k, j] = r.fr[j]

        def send(j):
            weight_chunk_send(j, along_x(j))

    else:

        def nothing(j):
            return None

        rs1 = rs2 = rs3 = rs4 = send = nothing

    G, GOR = r.gbe, r.gor
    take(GOR, r.gorr)

    @pl.loop(0, rows // BLK)
    def _(i):
        v = GO[k, block(i), :] + GOR[block(i), :]
        GOR[block(i), :] = v
        G[block(i, EDGE), :] = v.astype(BF16)

    put(G.at[pl.ds(EDGE, EDGE)], G.at[pl.ds(rows + EDGE, EDGE)], r.gs.at[0], r.gr.at[0], left_dev)
    put(G.at[pl.ds(rows, EDGE)], G.at[pl.ds(0, EDGE)], r.gs.at[1], r.gr.at[1], right_dev)
    GA, GP = r.ga, r.gp
    GA[EDGE : EDGE + rows, :] = nt(G[EDGE : EDGE + rows, :], mixf)

    def pull_two(at):
        v = normed2_of(CV[at, :])
        g = GA[at, :] * gelu_slope(v * gain2 + off2)
        GP[at, :] = g
        return g * v, g

    gs_, ss_ = lax.fori_loop(0, rows // BLK, row_sums(lambda i: pull_two(block(i, EDGE))), (zero_h, zero_h))
    spread(r.sa2, (gs_, ss_))
    sum_start(2)
    send(0)
    send(1)
    MP = r.mp
    mp = nn(r.a2t[...], G[EDGE : EDGE + rows, :]).astype(BF16).reshape(C, LANES, width)
    for p in range(C):
        MP[p % 2, p // 2] = mp[p, 0:cr, :]
    put(MP.at[1 - k], r.mr, r.mps.at[0], r.mpr.at[0], (s, other))
    sum_middle(2)
    HX = r.hbx
    take(HX, r.hbrem.at[0])
    HX[...] = HX[...] + HB[...]

    @pl.loop(1, S)
    def _(p):
        put(HX, r.hbf.at[s], r.hbsem.at[1], r.hbrem.at[1], (lax.rem(s + p, S), c))

    r.hbf[s] = HX[...]
    send(2)
    send(3)
    take(r.mr, r.mpr.at[0])
    MR = r.mr
    MR[...] = (MR[...].astype(F32) + MP[k].astype(F32)).astype(BF16)
    put(MR.at[xo], r.mx, r.mps.at[1], r.mpr.at[1], (s, xnb))
    take(r.xedge, r.gr.at[0])
    take(r.xedge, r.gr.at[1])
    for at in (0, rows + EDGE):
        GA[at : at + EDGE, :] = nt(G[at : at + EDGE, :], mixf)
        pull_two(slice(at, at + EDGE))
    total2, gsum2, ssum2 = sum_end(2, hp)
    r.tot[...] = total2
    r.g2[0:1, :] = r.tot[pl.ds(c, 1), :]
    r.g2[1:2, :] = r.tot[pl.ds(C + c, 1), :]
    coef2 = gain2 * scale2
    gmean2, smean2 = gsum2 * inv_bins, ssum2 * inv_bins
    GC, GB = r.gce, r.gcb

    def conv_grad(at):
        return (coef2 * (GP[at, :] - smean2 - normed2_of(CV[at, :]) * gmean2)).astype(BF16)

    hx = hp // 2

    @pl.loop(0, rows // BLK)
    def _(i):
        v = conv_grad(block(i, EDGE))
        GC[block(i, EDGE), :] = v.astype(F32)
        GB[0, block(i), :] = v[:, :hx]
        GB[1, block(i), :] = v[:, hx:]

    put(GB.at[xo], r.gcx, r.gbs, r.gbr, (s, xnb))
    GC[0:EDGE, :] = jnp.where(left_same, conv_grad(slice(0, EDGE)).astype(F32), 0.0)
    GC[rows + EDGE : ext, :] = jnp.where(right_same, conv_grad(slice(rows + EDGE, ext)).astype(F32), 0.0)

    G1 = r.ga1
    for t in range(TAPS):
        lo_t = EDGE + STEP - t * STEP
        part = nn(GC[lo_t : lo_t + rows, :].astype(BF16), CM[t].reshape(hp, width))
        G1[...] = part if t == 0 else G1[...] + part

    def pull_one(i):
        v = normed1_of(r.x[block(i), :].astype(F32))
        g = G1[block(i), :] * gelu_slope(v * gain1 + off1)
        G1[block(i), :] = g
        return g * v, g

    g1s, s1s = lax.fori_loop(0, rows // BLK, row_sums(pull_one), (zero_w, zero_w))
    spread(r.sa3, (g1s, s1s))
    sum_start(3)
    send(4)

    take(r.actx, r.ar_)
    take(r.gcx, r.gbr)
    ZP, CG = r.zpad, r.cg
    pad = ZP.shape[0] - rows
    ZP[0 : pad // 2, :] = jnp.zeros((pad // 2, hx), F32)
    ZP[rows + pad // 2 :, :] = jnp.zeros((pad // 2, hx), F32)
    for part in range(2):
        ZP[pad // 2 : pad // 2 + rows, :] = (GB[xi] if part == 0 else r.gcx[...]).astype(F32)
        rows_act = A[lo : lo + ext, :] if part == 0 else r.actx[...]
        for t in range(TAPS):
            lo_t = pad // 2 - EDGE + STEP - t * STEP
            v = nn(ZP[lo_t : lo_t + ext, :].T.astype(BF16), rows_act).reshape(2, LANES, width)
            CG[t] = v if part == 0 else CG[t] + v
    put(CG.at[:, 1 - k, pl.ds(0, cr)], r.cgr, r.cgs, r.cgrr, (s, other))
    sum_middle(3)
    take(r.mx, r.mpr.at[1])
    mix_sum = MR[xi].astype(F32) + r.mx[...].astype(F32)
    rs1(0)
    take(r.cgr, r.cgrr)
    if fused:
        CP, C1, C3, CF = r.cp, r.c1, r.c3, r.cf
        rp = CP.shape[2]
        weights = jnp.concatenate([CG[:, k, 0:cr, :] + r.cgr[...], mix_sum[None]], axis=0)
        CP[...] = weights.astype(BF16).reshape(CP.shape)
        put(CP.at[:, 1 - y], C1, r.ccs.at[0], r.ccr.at[0], (ynb, c))
    else:
        r.cmg[0:3] = CG[:, k, 0:cr, :] + r.cgr[...]
        r.cmg[3] = mix_sum
        r.wgo[...] = WG[...]
    total1, gsum1, ssum1 = sum_end(3, width)
    r.g1[0:1, :] = gsum1
    r.g1[1:2, :] = ssum1
    coef1 = gain1 * scale1
    gmean1, smean1 = gsum1 * inv_bins, ssum1 * inv_bins

    @pl.loop(0, rows // BLK)
    def _(i):
        v = normed1_of(r.x[block(i), :].astype(F32))
        r.ig[block(i), :] = GOR[block(i), :] + coef1 * (G1[block(i), :] - smean1 - v * gmean1)

    take(r.hbf.at[pl.ds(0, S - 1)], r.hbrem.at[1])
    HB3 = r.hb3
    HB3[...] = lax.fori_loop(1, S, lambda p, a: a + r.hbf[p], r.hbf[0])
    put(HB3, r.hbp, r.hbsem.at[2], r.hbrem.at[2], (s, other))
    r.hb[k] = HB3[...]

    if fused:
        rs1(1)
        send(5)
        send(6)
        rs2(0)
        take(C1, r.ccr.at[0])
        for zz in range(Z):
            C1[zz] = (C1[zz].astype(F32) + CP[zz, y].astype(F32)).astype(BF16)
        C3[z] = C1[z]
        for p in range(1, Z):
            to = lax.rem(z + p, Z)
            put(C1.at[to], C3.at[z], r.ccs.at[1], r.ccr.at[1], (to * 2 + y, c))
        rs1(2)
        rs2(1)
        rs3(0)
        take(C3.at[pl.ds(0, Z - 1)], r.ccr.at[1])
        v = C3[0].astype(F32)
        for p in range(1, Z):
            v = v + C3[p].astype(F32)
        CF[z, y] = v.astype(BF16)
        for p in range(1, Z):
            to = lax.rem(z + p, Z)
            put(CF.at[z, y], CF.at[z, y], r.ccs.at[2], r.ccr.at[2], (to * 2 + y, c))
        rs1(3)
        rs2(2)
        rs3(1)
        take(CF.at[pl.ds(0, Z - 1), 0], r.ccr.at[2])
        put(CF.at[:, y], CF.at[:, y], r.ccs.at[3], r.ccr.at[3], (ynb, c))
        rs1(4)
        rs2(3)
        rs3(2)
        take(CF.at[:, 0], r.ccr.at[3])
        r.cmg[...] = CF[...].reshape(r.cmg.shape).astype(F32)
        rs1(5)
        rs2(4)
        rs3(3)
        rs1(6)
        rs2(5)
        rs3(4)
        rs2(6)
        rs3(5)
        rs3(6)
        for j in range(NCHUNK):
            rs4(j)
    take(r.hbp, r.hbrem.at[2])
    r.hb[1 - k] = r.hbp[...]

    for i in range(4):
        take(r.ba[i].at[pl.ds(0, C - 1)], r.ars.at[2 * i])
        take(r.bb[i].at[pl.ds(0, S - 1)], r.ars.at[2 * i + 1])
    take(r.xl, r.hs.at[0])
    take(r.xr, r.hs.at[1])
    take(CM.at[0, 0, pl.ds(0, cr)], r.cms.at[0])
    take(CM.at[0, 0, pl.ds(0, cr), pl.ds(0, half_w)], r.cms.at[1])
    take(r.cm, r.cms.at[2])
    take(CM.at[0, 0, pl.ds(0, cr)], r.cms.at[3])
    take(CM.at[0, 0, pl.ds(0, cr)], r.cms.at[4])
    take(CM.at[0, 0, pl.ds(0, cr), pl.ds(0, half_w)], r.cms.at[5])
    take(r.cm, r.cms.at[6])
    take(r.gsb.at[pl.ds(0, C - 1)], r.gss)
    take(W.at[:, 0], r.wps)
    take(TG.at[:, 0], r.tps)
    take(W.at[:, pl.ds(0, 3), 0], r.wxs)
    take(W.at[:, pl.ds(0, 2), 0], r.wrs.at[0])
    take(W.at[:, pl.ds(0, 2), 0], r.wrs.at[1])
    take(W.at[:, 0, 0], r.wrs.at[2])
    take(r.actx, r.as_)
    take(O.at[0], r.os)
    take(GOR, r.gos)
    take(HX, r.hbsem.at[0])
    take(r.hbf.at[pl.ds(0, S - 1)], r.hbsem.at[1])
    take(HB3, r.hbsem.at[2])
    take(r.xedge, r.gs.at[0])
    take(r.xedge, r.gs.at[1])
    take(r.mr, r.mps.at[0])
    take(r.mx, r.mps.at[1])
    take(r.gcx, r.gbs)
    take(r.cgr, r.cgs)
    if fused:
        take(C1, r.ccs.at[0])
        take(C3.at[pl.ds(0, Z - 1)], r.ccs.at[1])
        take(CF.at[pl.ds(0, Z - 1), 0], r.ccs.at[2])
        take(CF.at[:, 0], r.ccs.at[3])
        for j in range(NCHUNK):
            take(R1.at[j], r.s1.at[j])
            take(R2.at[j], r.s2.at[j])
            take(R3.at[j, pl.ds(0, Z - 1)], r.s3.at[j])
            take(r.fr.at[j], r.s4.at[j])


def fused_step(seqs, chs, x, gs1, gs2, cm, bias, flags, hw, mw, tg):
    S, C = seqs, chs
    rows, width = x.shape
    n_dev = S * C
    hp = C * LANES
    cr = cm.shape[1]
    kr = hw.shape[1]
    ext = rows + 2 * EDGE
    Z = S // 2
    fused = width % (n_dev * 8) == 0 and (4 * cr) % (S * 16) == 0
    two = 2 * (width // n_dev)
    rp = 4 * cr // S
    vm = pltpu.VMEM
    dma = pltpu.SemaphoreType.DMA
    ins = dict(x=x, gs1=gs1, gs2=gs2, cm=cm, bias=bias, flags=flags, hw=hw, mw=mw, tg=tg)
    any_ins = ("hw", "mw", "tg")
    outs = dict(
        out=((rows, width), BF16),
        ig=((rows, width), F32),
        g1=((2, width), F32),
        g2=((2, LANES), F32),
        cmg=((4, cr, width), F32),
        hb=((2, 8, CW), F32),
    )
    if fused:
        outs["hg"] = ((2, NCHUNK, two // 2, CW), F32)
    else:
        outs["wgo"] = ((NCHUNK, Z, 2, 2, width // (4 * Z), HW), BF16)
    scratch = dict(
        xl=vm((HALO, width), BF16),
        xr=vm((HALO, width), BF16),
        xedge=vm((EDGE, width), BF16),
        gsb=vm((C, 8, LANES), F32),
        cmf=vm((4, C, LANES, width), BF16),
        wbuf=vm((NCHUNK, 4, 4, kr, CW), BF16),
        tgb=vm((NCHUNK, 2, rows, CW), BF16),
        act=vm((rows + 2 * HALO, width), BF16),
        actx=vm((ext, width), BF16),
        prod=vm((TAPS, rows + 2 * HALO, hp), F32),
        cv=vm((ext, hp), F32),
        a2=vm((rows, hp), BF16),
        a2t=vm((hp, rows), BF16),
        ob=vm((2, rows, width), BF16),
        ot=vm((width, 2 * rows), BF16),
        wsel=vm((width, HW), BF16),
        lg=vm((2 * rows, HW), F32),
        gl=vm((2 * rows, HW), BF16),
        wg=vm((NCHUNK, Z, 2, 2, width // (4 * Z), HW), BF16),
        go=vm((2, rows, width), F32),
        gor=vm((rows, width), F32),
        hbs=vm((8, CW), F32),
        hbx=vm((8, CW), F32),
        hbf=vm((S, 8, CW), F32),
        hb3=vm((8, CW), F32),
        hbp=vm((8, CW), F32),
        gbe=vm((ext, width), BF16),
        ga=vm((ext, hp), F32),
        gp=vm((ext, hp), F32),
        gce=vm((ext, hp), F32),
        gcb=vm((2, rows, hp // 2), BF16),
        gcx=vm((rows, hp // 2), BF16),
        ga1=vm((rows, width), F32),
        mp=vm((2, 2, cr, width), BF16),
        mr=vm((2, cr, width), BF16),
        mx=vm((cr, width), BF16),
        zpad=vm((rows + 64, hp // 2), F32),
        cg=vm((TAPS, 2, LANES, width), F32),
        cgr=vm((TAPS, cr, width), F32),
        tot=vm((8, LANES), F32),
    )
    for i, n in enumerate((16, 8, 8, 16)):
        scratch[f"sa{i}"] = vm((n, LANES), F32)
        scratch[f"sb{i}"] = vm((n, LANES), F32)
        scratch[f"ba{i}"] = vm((C, n, LANES), F32)
        scratch[f"bb{i}"] = vm((S, n, LANES), F32)
    sems = dict(
        ars=8, arr=8, hs=2, hr=2, cms=7, cmr=7, cml=0, gss=0, gsr=0, wl=7, wp=7, wx=7, wy=7, wz=7, wd=7, wps=0, wxs=0,
        wrs=3, tl=7, tp=7, tps=0, as_=0, ar_=0, os=0, gos=0, gorr=0, hbsem=3, hbrem=3, gs=2, gr=2, mps=2, mpr=2, gbs=0,
        gbr=0, cgs=0, cgrr=0, orr=0,
    )
    if fused:
        scratch.update(
            acc1=vm((NCHUNK, Z, 2, two, CW), BF16),
            r1=vm((NCHUNK, Z, 2, two, HW), BF16),
            r2=vm((NCHUNK, Z, two, CW), BF16),
            r3=vm((NCHUNK, Z, two, CW), BF16),
            fin=vm((NCHUNK, 2, two // 2, CW), F32),
            fr=vm((NCHUNK, two // 2, CW), F32),
            cp=vm((Z, 2, rp, width), BF16),
            c1=vm((Z, rp, width), BF16),
            c3=vm((Z, rp, width), BF16),
            cf=vm((Z, 2, rp, width), BF16),
        )
        sems.update(s1=7, s2=7, s3=7, s4=7, g1r=7, g2r=7, g3r=7, g4r=7, ccs=4, ccr=4)
    for name, n in sems.items():
        scratch[name] = dma((n,)) if n else dma
    names = [*ins, *outs, *scratch]

    def space(name):
        if name == "flags":
            return pl.BlockSpec(memory_space=pltpu.SMEM)
        return pl.BlockSpec(memory_space=pl.ANY if name in any_ins else pltpu.VMEM)

    got = pl.pallas_call(
        functools.partial(kernel_body, S, C, fused, names),
        out_shape=[jax.ShapeDtypeStruct(*v) for v in outs.values()],
        in_specs=[space(n) for n in ins],
        out_specs=[pl.BlockSpec(memory_space=pltpu.VMEM) for _ in outs],
        scratch_shapes=list(scratch.values()),
        compiler_params=pltpu.CompilerParams(
            collective_id=0, has_side_effects=True, vmem_limit_bytes=67_043_328
        ),
    )(*ins.values())
    return types.SimpleNamespace(**dict(zip(outs, got, strict=True))), fused


def on_device(
    inputs, gain_one, shift_one, conv_weight, gain_two, shift_two, mix_weight, head_weight, head_bias, species, counts
):
    S, C = lax.axis_size("seq"), lax.axis_size("ch")
    s, c = lax.axis_index("seq"), lax.axis_index("ch")
    rows, width = inputs.shape
    cols = conv_weight.shape[2]
    total_bins = rows * S * C
    depth = head_weight.shape[0]

    def species_at(seq, chip):
        first = (seq * C + chip * 2) * rows
        window = jnp.mod(first - SHIFT, total_bins) // WINDOW_BINS
        return jnp.sum(jnp.where(jnp.arange(species.shape[0], dtype=jnp.int32) == window, species, 0))

    xi = c // 2
    flags = jnp.stack([species_at(s, xi), species_at(s, 1 - xi), species_at(s + 1 - 2 * lax.rem(s, 2), xi)])
    gs1 = jnp.stack([gain_one, shift_one])
    gs2 = jnp.pad(jnp.stack([gain_two, shift_two]), ((0, 6), (0, LANES - cols)))
    cm = jnp.concatenate([jnp.transpose(conv_weight, (0, 2, 1)), mix_weight[None]], axis=0)
    hw = head_weight.reshape(4, depth // 4, head_weight.shape[1])
    mw = jnp.pad(hw[:, :, HUMAN:], ((0, 0), (0, 0), (0, 2 * HALF_M - MOUSE)))
    tg = jnp.pad(counts.astype(BF16), ((0, 0), (0, 2 * HALF_H - HUMAN)))
    bias = jnp.concatenate(
        [
            jnp.pad(head_bias[:HUMAN], (0, 2 * HALF_H - HUMAN)).reshape(2 * NCHUNK, HW),
            jnp.pad(head_bias[HUMAN:], (0, 2 * HALF_M - MOUSE)).reshape(2 * NCHUNK, MW),
        ],
        axis=1,
    )
    o, fused = fused_step(S, C, inputs, gs1, gs2, cm, bias, flags, hw, mw, tg)

    def whole(v):
        n = v.shape[2]
        h = jnp.transpose(v[..., :HW], (2, 0, 1, 3)).reshape(n, 2 * HALF_H)[:, :HUMAN]
        m = jnp.transpose(v[..., HW:], (2, 0, 1, 3)).reshape(n, 2 * HALF_M)[:, :MOUSE]
        return jnp.concatenate([h, m], axis=1)

    cmg = o.cmg
    if fused:
        head_weight_grad = whole(o.hg)
    else:
        part = o.wgo.reshape(NCHUNK, width, HW).astype(F32)
        human = flags[0] == 0
        part = jnp.concatenate(
            [jnp.where(human, part, 0.0), jnp.where(human, 0.0, part[..., :MW])], axis=2
        )
        core = (jnp.arange(2, dtype=jnp.int32) == lax.rem(c, 2)).reshape(2, 1, 1, 1)
        head_weight_grad = lax.psum_scatter(
            whole(jnp.where(core, part[None], 0.0)), ("seq", "ch"), scatter_dimension=0, tiled=True
        )
        cmg = lax.psum(cmg, "seq")
    head_bias_grad = whole(o.hb[:, :NCHUNK, None, :])[0]
    return (
        o.out,
        o.ig,
        o.g1[0],
        o.g1[1],
        jnp.transpose(cmg[:3], (0, 2, 1)),
        o.g2[0, :cols],
        o.g2[1, :cols],
        cmg[3],
        head_weight_grad,
        head_bias_grad,
    )


def solution(mesh):
    rows = P(("seq", "ch"), None)
    in_specs = (
        rows, P(), P(), P(None, None, "ch"), P("ch"), P("ch"), P("ch", None), P("ch", None), P(), P(), rows,
    )
    out_specs = (
        rows, rows, P(), P(), P(None, None, "ch"), P("ch"), P("ch"), P("ch", None), rows, P(),
    )
    return jax.shard_map(on_device, mesh=mesh, in_specs=in_specs, out_specs=out_specs, check_vma=False)
```

```python
import functools
import math
import types

import jax
import jax.numpy as jnp
from jax import lax
from jax.experimental import pallas as pl
from jax.experimental.pallas import tpu as pltpu
from jax.sharding import PartitionSpec as P

HUMAN = 5313
MOUSE = 1643
STEP = 11
TAPS = 3
WINDOW_BINS = 1024
SHIFT = 512
EPS = 1e-05

LANES = 128
NCHUNK = 7
HW = 384
MW = 128
CW = HW + MW
HALF_H = NCHUNK * HW
HALF_M = NCHUNK * MW
HALO = 32
EDGE = 16
MESH = pl.DeviceIdType.MESH
F32 = jnp.float32
BF16 = jnp.bfloat16
K0 = math.sqrt(2.0 / math.pi)
K1 = K0 * 0.044715


PLAN = {
    0: ((0, 0),),
    2: ((2, 4),),
    4: ((2, 5),),
    5: ((3, 2),),
    7: ((2, 6),),
    13: ((3, 3),),
    14: ((3, 4),),
    15: ((3, 5), (3, 6)),
    16: ((4, 0), (4, 1), (4, 2), (4, 3)),
    17: ((4, 4), (4, 5), (4, 6)),
}
LOOP = ((0, 7), (3, 4), (5, 2))
XFIRST = 3
RELAYED = 5


def nn(a, b):
    return lax.dot_general(a, b, (((1,), (0,)), ((), ())), preferred_element_type=F32)


def nt(a, b):
    return lax.dot_general(a, b, (((1,), (1,)), ((), ())), preferred_element_type=F32)


def gelu(v):
    return 0.5 * v * (1.0 + jnp.tanh(v * (K0 + K1 * (v * v))))


def gelu_slope(v):
    v2 = v * v
    th = jnp.tanh(v * (K0 + K1 * v2))
    return 0.5 * (1.0 + th) + 0.5 * v * (1.0 - th * th) * (K0 + 3.0 * K1 * v2)


def poisson_grad(logits, target):
    t = jnp.exp(-jnp.abs(logits))
    up = 1.0 + t
    series = t * (1.0 - t * (0.5 - t * (1.0 / 3.0 - t * 0.25)))
    rate = jnp.maximum(logits, 0.0) + jnp.where(t < 0.015625, series, jnp.log(up))
    return jnp.where(logits >= 0.0, 1.0, t) * (rate - target) / (up * rate)


def take(ref, sem):
    pltpu.make_async_copy(ref, ref, sem).wait()


def kernel_body(seqs, chs, fused, names, *refs):
    r = types.SimpleNamespace(**dict(zip(names, refs, strict=True)))
    r.sa, r.sb, r.ba, r.bb = ([getattr(r, f"{n}{i}") for i in range(4)] for n in ("sa", "sb", "ba", "bb"))
    S, C = seqs, chs
    s = lax.axis_index("seq")
    c = lax.axis_index("ch")
    xi = c // 2
    k = lax.rem(c, 2)
    other = c + 1 - 2 * k
    xnb = lax.rem(c + 2, C)
    xo = 1 - xi
    y = lax.rem(s, 2)
    z = s // 2
    ynb = s + 1 - 2 * y
    zb = lax.rem(z, 2)
    znb = s + 2 - 4 * zb
    dnb = znb + 1 - 2 * y
    q = lax.rem(s, 4)
    q_y = q + 1 - 2 * y
    q_z = q + 2 - 4 * zb
    q_d = q_z + 1 - 2 * y
    rows, width = r.x.shape
    n_dev = S * C
    total_bins = rows * n_dev
    inv_bins = 1.0 / total_bins
    me = s * C + c
    left = lax.rem(me + n_dev - 1, n_dev)
    right = lax.rem(me + 1, n_dev)
    left_dev = (left // C, lax.rem(left, C))
    right_dev = (right // C, lax.rem(right, C))
    row0 = me * rows
    window = lax.rem(row0 + total_bins - SHIFT, total_bins) // WINDOW_BINS
    left_same = lax.rem(row0 + total_bins - 1 + total_bins - SHIFT, total_bins) // WINDOW_BINS == window
    right_same = lax.rem(row0 + rows + total_bins - SHIFT, total_bins) // WINDOW_BINS == window

    def human_at_chip(seq, chip):
        first = (seq * C + chip * 2) * rows
        return r.species[lax.rem(first + total_bins - SHIFT, total_bins) // WINDOW_BINS] == 0

    mine_h = human_at_chip(s, xi)
    x_h = human_at_chip(s, xo)
    y_h = human_at_chip(ynb, xi)
    hp = C * LANES

    def put(src, dst, send, recv, dev):
        pltpu.make_async_remote_copy(
            src_ref=src, dst_ref=dst, send_sem=send, recv_sem=recv, device_id=dev, device_id_type=MESH
        ).start()

    barrier = pltpu.get_barrier_semaphore()

    def greet(dev):
        pl.semaphore_signal(barrier, inc=1, device_id=dev, device_id_type=MESH)

    for i in range(1, C):
        greet((s, lax.rem(c + i, C)))

    @pl.loop(1, S)
    def _(i):
        greet((lax.rem(s + i, S), c))

    greet(left_dev)
    greet(right_dev)

    W, TG = r.wbuf, r.tgb

    def human_at(half, j):
        return pl.ds(pl.multiple_of(half * HALF_H + j * HW, LANES), HW)

    def mouse_at(half, j):
        return pl.ds(pl.multiple_of(half * HALF_M + j * MW, LANES), MW)

    HV, MV, CB = r.hwv, r.mwv, r.cbuf
    load_hw = pltpu.make_async_copy(r.hw, HV, r.ld.at[0])
    load_hw.start()
    load_counts = pltpu.make_async_copy(r.counts, CB, r.ld.at[1])
    load_counts.start()
    CM, CS = r.cmf, r.cm
    cr = CS.shape[1]
    for t in range(TAPS):
        CS[t] = r.cw[t]
        CM[t, c, 0:cr, :] = r.cw[t]
    CS[TAPS] = r.mix[...]
    CM[TAPS, c, 0:cr, :] = r.mix[...]
    for t in range(4):
        for p in range(C):
            CM[t, p, cr:LANES, :] = jnp.zeros((LANES - cr, width), BF16)
    r.gs2[...] = jnp.zeros(r.gs2.shape, F32)
    r.gs2[0:1, 0:cr] = r.gain2[...].reshape(1, cr)
    r.gs2[1:2, 0:cr] = r.shift2[...].reshape(1, cr)
    M0 = HUMAN // LANES * LANES
    OFF = HUMAN - M0
    HP = r.hbpad
    tracks = HUMAN + MOUSE
    HP[:, 0:tracks] = r.bias[...].reshape(1, tracks)
    HP[:, tracks:] = jnp.zeros((1, HP.shape[1] - tracks), F32)
    BR = r.bias_rows
    for m in range(2 * NCHUNK):
        BR[m : m + 1, 0:HW] = HP[:, m * HW : (m + 1) * HW]
        v = HP[:, M0 + m * LANES : M0 + (m + 2) * LANES]
        BR[m : m + 1, HW:CW] = pltpu.roll(v, 2 * LANES - OFF, 1)[:, :MW]

    def spread(ref, vecs):
        n = vecs[0].shape[1] // LANES
        for i, v in enumerate(vecs):
            for t in range(n):
                ref[i * n + t : i * n + t + 1, :] = v[:, t * LANES : (t + 1) * LANES]
        if ref.shape[0] > n * len(vecs):
            ref[n * len(vecs) :, :] = jnp.zeros((ref.shape[0] - n * len(vecs), LANES), F32)

    def collect(v, n):
        m = n // LANES
        return [jnp.concatenate([v[i * m + t : i * m + t + 1, :] for t in range(m)], axis=1) for i in range(2)]

    def sum_start(i):
        src, bufs = r.sa[i], r.ba[i]
        for p in range(1, C):
            put(src, bufs.at[c], r.ars.at[2 * i], r.arr.at[2 * i], (s, lax.rem(c + p, C)))
        bufs[c] = src[...]

    def sum_middle(i):
        src, bufs, far = r.sb[i], r.ba[i], r.bb[i]
        take(bufs.at[pl.ds(0, C - 1)], r.arr.at[2 * i])
        v = bufs[0]
        for p in range(1, C):
            v = v + bufs[p]
        src[...] = v

        @pl.loop(1, S)
        def _(p):
            put(src, far.at[s], r.ars.at[2 * i + 1], r.arr.at[2 * i + 1], (lax.rem(s + p, S), c))

        far[s] = v

    def sum_end(i, n):
        far = r.bb[i]
        take(far.at[pl.ds(0, S - 1)], r.arr.at[2 * i + 1])
        if S <= 8:
            v = far[0]
            for p in range(1, S):
                v = v + far[p]
        else:
            v = lax.fori_loop(1, S, lambda p, a: a + far[p], far[0])
        return v, *collect(v, n)

    BLK = 32

    def block(i, shift=0):
        return pl.ds(pl.multiple_of(i * BLK + shift, 16), BLK)

    def row_sums(terms):
        def step(i, carry):
            return tuple(a + jnp.sum(t, 0, keepdims=True) for a, t in zip(carry, terms(i), strict=True))

        return step

    zero_w = jnp.zeros((1, width), F32)

    def x_terms(i):
        v = r.x[block(i), :].astype(F32)
        return v, v * v

    s1, q1 = lax.fori_loop(0, rows // BLK, row_sums(x_terms), (zero_w, zero_w))
    spread(r.sa0, (s1, q1))
    load_hw.wait()
    full = (tracks - M0) // LANES - 1
    for p in range(4):
        for m in range(2 * NCHUNK):
            if m < full:
                v = HV[p, :, M0 + m * LANES : M0 + (m + 2) * LANES].astype(F32)
                v = pltpu.roll(v, 2 * LANES - OFF, 1)[:, :MW]
            elif M0 + m * LANES < tracks:
                v = HV[p, :, M0 + m * LANES : min(tracks, M0 + (m + 2) * LANES)].astype(F32)
                v = jnp.concatenate([v, jnp.zeros((v.shape[0], 2 * LANES - v.shape[1]), F32)], axis=1)
                v = pltpu.roll(v, 2 * LANES - OFF, 1)[:, :MW]
            else:
                v = jnp.zeros((HV.shape[1], MW), F32)
            MV[p, :, m * MW : (m + 1) * MW] = v.astype(BF16)

    @pl.loop(0, NCHUNK)
    def _(j):
        pltpu.make_async_copy(HV.at[:, :, human_at(k, j)], W.at[j, c, :, :, pl.ds(0, HW)], r.wl.at[j]).start()
        pltpu.make_async_copy(MV.at[:, :, mouse_at(k, j)], W.at[j, c, :, :, pl.ds(HW, MW)], r.wl.at[j]).start()

    pl.semaphore_wait(barrier, C - 1 + S - 1 + 2)

    sum_start(0)
    put(r.x.at[pl.ds(rows - HALO, HALO)], r.xl, r.hs.at[0], r.hr.at[0], right_dev)
    put(r.x.at[pl.ds(0, HALO)], r.xr, r.hs.at[1], r.hr.at[1], left_dev)
    half_w = width // 2
    put(CS.at[q], CM.at[q, c, pl.ds(0, cr)], r.cms.at[0], r.cmr.at[0], (s, xnb))
    put(
        CS.at[q_d, :, pl.ds(0, half_w)],
        CM.at[q_d, c, pl.ds(0, cr), pl.ds(0, half_w)],
        r.cms.at[1],
        r.cmr.at[1],
        (s, xnb),
    )
    put(CS, CM.at[:, c, pl.ds(0, cr)], r.cms.at[2], r.cmr.at[2], (s, other))
    for p in range(1, C):
        put(r.gs2, r.gsb.at[c], r.gss, r.gsr, (s, lax.rem(c + p, C)))
    r.gsb[c] = r.gs2[...]

    @pl.loop(0, NCHUNK)
    def _(j):
        put(
            HV.at[:, :, human_at(1 - k, j)], W.at[j, c, :, :, pl.ds(0, HW)],
            r.wps, r.wp.at[j], (s, other),
        )
        put(
            MV.at[:, :, mouse_at(1 - k, j)], W.at[j, c, :, :, pl.ds(HW, MW)],
            r.wps, r.wp.at[j], (s, other),
        )
    HALFC = CW // 2

    def heads_along_x(j):
        for h in range(2):
            dev = (s, xo * 2 + h)
            hc = pl.multiple_of(h * HALF_H + j * HW, LANES)
            put(HV.at[q, :, human_at(h, j)], W.at[j, c, q, :, pl.ds(0, HW)], r.wxs, r.wx.at[j], dev)
            put(MV.at[q, :, mouse_at(h, j)], W.at[j, c, q, :, pl.ds(HW, MW)], r.wxs, r.wx.at[j], dev)
            put(
                HV.at[q_d, :, pl.ds(hc, HALFC)], W.at[j, c, q_d, :, pl.ds(0, HALFC)],
                r.wxs, r.wx.at[j], dev,
            )

    def relay_heads(j):
        take(W.at[j, pl.ds(0, 3), 0], r.wx.at[j])
        far = pl.ds(xo * 2, 2)
        put(W.at[j, far, q], W.at[j, far, q], r.wrs.at[0], r.wy.at[j], (ynb, c))
        put(W.at[j, far, q], W.at[j, far, q], r.wrs.at[1], r.wz.at[j], (znb, c))
        put(
            W.at[j, far, q, :, pl.ds(HALFC, HALFC)], W.at[j, far, q, :, pl.ds(HALFC, HALFC)],
            r.wrs.at[2], r.wd.at[j], (dnb, c),
        )

    for j in range(XFIRST):
        heads_along_x(j)

    def pass_weights():
        take(CM.at[0, 0, pl.ds(0, cr)], r.cmr.at[0])
        put(CM.at[q, xnb, pl.ds(0, cr)], CM.at[q, xnb, pl.ds(0, cr)], r.cms.at[3], r.cmr.at[3], (ynb, c))
        put(CM.at[q, xnb, pl.ds(0, cr)], CM.at[q, xnb, pl.ds(0, cr)], r.cms.at[4], r.cmr.at[4], (znb, c))
        second = pl.ds(half_w, half_w)
        put(
            CM.at[q, xnb, pl.ds(0, cr), second], CM.at[q, xnb, pl.ds(0, cr), second],
            r.cms.at[5], r.cmr.at[5], (dnb, c),
        )

    def targets(half, dst, j):
        at = pl.multiple_of(half * HALF_H + j * HW, 8)
        am = pl.multiple_of(half * HALF_M + j * MW, 8)
        v = CB[pl.ds(at, MW), :]
        dst[:, 0:MW] = jnp.where(mine_h, v, CB[pl.ds(am, MW), :]).astype(F32).T.astype(BF16)
        ends = (half == 1) & (j == NCHUNK - 1)

        @pl.when(ends)
        def _():
            dst[:, MW:HW] = CT[...].astype(F32).T.astype(BF16)

        @pl.when(jnp.logical_not(ends))
        def _():
            dst[:, MW:HW] = CB[pl.ds(at + MW, HW - MW), :].astype(F32).T.astype(BF16)

    load_counts.wait()
    CT = r.ctail
    whole = HUMAN - (2 * HALF_H - HW + MW)
    CT[0:whole, :] = CB[HUMAN - whole : HUMAN, :]
    CT[whole:, :] = jnp.zeros((CT.shape[0] - whole, CT.shape[1]), jnp.int32)
    sum_middle(0)
    pass_weights()

    @pl.loop(0, NCHUNK)
    def _(j):
        targets(k, TG.at[j, k], j)

    _, t1, u1 = sum_end(0, width)
    mean1 = t1 * inv_bins
    scale1 = lax.rsqrt(u1 * inv_bins - mean1 * mean1 + EPS)
    gain1 = r.gain1[...].reshape(1, width)
    off1 = r.shift1[...].reshape(1, width)

    A = r.act

    def normed1_of(v):
        return (v - mean1) * scale1

    def act_rows(v):
        return gelu(normed1_of(v.astype(F32)) * gain1 + off1)

    @pl.loop(0, rows // BLK)
    def _(i):
        at = pl.multiple_of(i * BLK, BLK)
        A[pl.ds(at + HALO, BLK), :] = act_rows(r.x[pl.ds(at, BLK), :]).astype(BF16)

    take(r.xl, r.hr.at[0])
    A[0:HALO, :] = jnp.where(left_same, act_rows(r.xl[...]), 0.0).astype(BF16)
    take(r.xr, r.hr.at[1])
    A[rows + HALO : rows + 2 * HALO, :] = jnp.where(right_same, act_rows(r.xr[...]), 0.0).astype(BF16)

    relay_heads(0)
    take(CM.at[0, 0, pl.ds(0, cr), pl.ds(0, half_w)], r.cmr.at[1])
    take(CM.at[0, 0, pl.ds(0, cr)], r.cmr.at[3])
    take(CM.at[0, 0, pl.ds(0, cr)], r.cmr.at[4])
    take(CM.at[0, 0, pl.ds(0, cr), pl.ds(0, half_w)], r.cmr.at[5])
    put(CM.at[:, xnb, pl.ds(0, cr)], CM.at[:, xnb, pl.ds(0, cr)], r.cms.at[6], r.cmr.at[6], (s, other))
    take(CM.at[:, 0, pl.ds(0, cr)], r.cmr.at[2])
    take(CM.at[:, 0, pl.ds(0, cr)], r.cmr.at[6])

    ext = rows + 2 * EDGE
    PR = r.prod
    for t in range(TAPS):
        PR[t] = nt(A[...], CM[t].reshape(hp, width))
    CV = r.cv
    lo = HALO - EDGE
    CV[...] = (
        PR[0, lo - STEP : lo - STEP + ext, :] + PR[1, lo : lo + ext, :] + PR[2, lo + STEP : lo + STEP + ext, :]
    )
    relay_heads(1)
    zero_h = jnp.zeros((1, hp), F32)

    def c_terms(i):
        v = CV[block(i, EDGE), :]
        return v, v * v

    s2, q2 = lax.fori_loop(0, rows // BLK, row_sums(c_terms), (zero_h, zero_h))
    spread(r.sa1, (s2, q2))
    sum_start(1)
    for j in range(XFIRST, NCHUNK):
        heads_along_x(j)

    @pl.loop(0, NCHUNK)
    def _(j):
        targets(1 - k, r.tgx.at[j], j)
        put(r.tgx.at[j], TG.at[j, k], r.tps, r.tp.at[j], (s, other))

    sum_middle(1)
    relay_heads(2)
    _, t2, u2 = sum_end(1, hp)
    mean2 = t2 * inv_bins
    scale2 = lax.rsqrt(u2 * inv_bins - mean2 * mean2 + EPS)
    take(r.gsb.at[pl.ds(0, C - 1)], r.gsr)
    gain2 = jnp.concatenate([r.gsb[p, 0:1, :] for p in range(C)], axis=1)
    off2 = jnp.concatenate([r.gsb[p, 1:2, :] for p in range(C)], axis=1)

    def normed2_of(v):
        return (v - mean2) * scale2

    A2 = r.a2

    @pl.loop(0, rows // BLK)
    def _(i):
        at = pl.multiple_of(i * BLK, BLK)
        v = normed2_of(CV[pl.ds(at + EDGE, BLK), :])
        A2[pl.ds(at, BLK), :] = gelu(v * gain2 + off2).astype(BF16)

    O = r.ob
    mixf = CM[3].reshape(hp, width)
    outputs = (r.x[...].astype(F32) + nn(A2[...], mixf)).astype(BF16)
    O[k] = outputs
    r.out[...] = outputs
    put(O.at[k], O.at[k], r.os, r.orr, (s, other))
    for j in range(3, RELAYED):
        relay_heads(j)
    r.a2t[...] = A2[...].T
    take(O.at[0], r.orr)
    OT = r.ot
    OT[...] = O[...].reshape(2 * rows, width).T
    GO = r.go
    GO[...] = jnp.zeros(GO.shape, F32)
    WG, GL = r.wg, r.gl
    LG = r.lg
    HB = r.hbs
    HB[...] = jnp.zeros(HB.shape, F32)
    Z = S // 2
    if fused:
        A1, R1, R2, R3 = r.acc1, r.r1, r.r2, r.r3
        two = A1.shape[3]
        own = two // 2

        def first(j, ax):
            if ax:
                put(WG.at[j, :, :, xo], R1.at[j], r.s1.at[j], r.g1r.at[j], (s, xnb))
            else:
                put(WG.at[j, :, 1 - y], R1.at[j], r.s1.at[j], r.g1r.at[j], (ynb, c))

        def second(j, ax):
            take(R1.at[j], r.g1r.at[j])
            got_h = x_h if ax else y_h

            def step(i, _):
                zz, b = i // 2, lax.rem(i, 2)
                a = (WG[j, zz, b, xi] if ax else WG[j, zz, y, b]).astype(F32)
                g = R1[j, zz, b].astype(F32)
                A1[j, zz, b, :, 0:HW] = (jnp.where(mine_h, a, 0.0) + jnp.where(got_h, g, 0.0)).astype(BF16)
                A1[j, zz, b, :, HW:CW] = (
                    jnp.where(mine_h, 0.0, a[:, :MW]) + jnp.where(got_h, 0.0, g[:, :MW])
                ).astype(BF16)
                return 0

            lax.fori_loop(0, S, step, 0)
            if ax:
                put(A1.at[j, :, 1 - y], R2.at[j], r.s2.at[j], r.g2r.at[j], (ynb, c))
            else:
                put(A1.at[j, :, xo], R2.at[j], r.s2.at[j], r.g2r.at[j], (s, xnb))

        def third(j, ax):
            take(R2.at[j], r.g2r.at[j])
            b = y if ax else xi
            for zz in range(Z):
                R2[j, zz] = (A1[j, zz, b].astype(F32) + R2[j, zz].astype(F32)).astype(BF16)
            R3[j, z] = R2[j, z]
            for p in range(1, Z):
                to = lax.rem(z + p, Z)
                put(R2.at[j, to], R3.at[j, z], r.s3.at[j], r.g3r.at[j], (to * 2 + y, c))

        def last(j):
            take(R3.at[j, pl.ds(0, Z - 1)], r.g3r.at[j])
            v = R3[j, 0].astype(F32)
            for p in range(1, Z):
                v = v + R3[j, p].astype(F32)
            r.fin[j] = v.reshape(2, own, CW)
            put(r.fin.at[j, 1 - k], r.fr.at[j], r.s4.at[j], r.g4r.at[j], (s, other))

        def either(step, j):
            @pl.when(lax.rem(j, 2) == 1)
            def _():
                step(j, True)

            @pl.when(lax.rem(j, 2) == 0)
            def _():
                step(j, False)

    def heads_chunk(j):
        take(W.at[j, 0], r.wl.at[j])
        take(W.at[j, 0], r.wp.at[j])
        take(W.at[j, pl.ds(0, 2), 0], r.wy.at[j])
        take(W.at[j, pl.ds(0, 2), 0], r.wz.at[j])
        take(W.at[j, pl.ds(0, 2), 0, :, pl.ds(0, HALFC)], r.wd.at[j])
        take(TG.at[j, 0], r.tp.at[j])
        w = r.wsel
        w[:, MW:] = W[j, :, :, :, MW:HW].reshape(width, HW - MW)
        w[:, :MW] = jnp.where(
            mine_h, W[j, :, :, :, 0:MW].reshape(width, MW), W[j, :, :, :, HW:CW].reshape(width, MW)
        )
        wv = w[...]
        LG[...] = nn(O[...].reshape(2 * rows, width), wv)
        valid_n = jnp.where(mine_h, HUMAN - (k * HALF_H + j * HW), jnp.minimum(MOUSE - (k * HALF_M + j * MW), MW))
        valid = lax.broadcasted_iota(jnp.int32, (1, HW), 1) < valid_n
        brow = BR[pl.ds(k * NCHUNK + j, 1), :]
        bias = jnp.concatenate([jnp.where(mine_h, brow[:, :MW], brow[:, HW:]), brow[:, MW:HW]], axis=1)
        per = rows // BLK

        def step(i, acc):
            at = pl.multiple_of(i * BLK, BLK)
            core = i // per
            ta = pl.ds(pl.multiple_of(lax.rem(i, per) * BLK, BLK), BLK)
            lg = LG[pl.ds(at, BLK), :] + bias
            tgt = TG[j, core, ta, :].astype(F32)
            g = jnp.where(valid, poisson_grad(lg, tgt), 0.0).astype(BF16)
            GL[pl.ds(at, BLK), :] = g
            return acc + jnp.sum(g.astype(F32).reshape(BLK // 8, 8, HW), 0)

        bsum = jnp.sum(lax.fori_loop(0, 2 * per, step, jnp.zeros((8, HW), F32)), 0, keepdims=True)
        bsum = jnp.concatenate([jnp.where(mine_h, bsum, 0.0), jnp.where(mine_h, 0.0, bsum[:, :MW])], axis=1)
        HB[...] = jnp.where(lax.broadcasted_iota(jnp.int32, HB.shape, 0) == j, bsum, HB[...])
        g = GL[...]
        GO[...] += nt(g, wv).reshape(GO.shape)
        WG[j] = nn(OT[...], g).astype(BF16).reshape(WG.shape[1:])

    act_rows_out = functools.partial(put, A.at[pl.ds(lo, ext)], r.actx, r.as_, r.ar_, (s, xnb))

    def at(slot):
        for stage, j in PLAN.get(slot, ()):
            if stage == 0:
                act_rows_out()
            elif fused:
                (first, second, third)[stage - 1](j, j % 2 == 1) if stage < 4 else last(j)

    at(0)

    @pl.loop(0, NCHUNK)
    def _(j):
        heads_chunk(j)

        @pl.when(j + RELAYED < NCHUNK)
        def _():
            relay_heads(j + RELAYED)

        if fused:
            for stage, step in ((1, first), (2, second), (3, third)):
                lag, count = LOOP[stage - 1]
                if count > 0:

                    @pl.when((j >= lag) & (j - lag < count))
                    def _(step=step, lag=lag):
                        either(step, j - lag)

    put(GO.at[1 - k], r.gor, r.gos, r.gorr, (s, other))
    put(r.hbs, r.hbx, r.hbsem.at[0], r.hbrem.at[0], (s, xnb))
    at(1)

    if fused:
        CP, C1, C3, CF = ([getattr(r, f"{n}{i}") for i in range(3)] for n in ("cp", "c1", "c3", "cf"))

        def lanes(b):
            return pl.ds(pl.multiple_of(b * half_w, LANES), half_w)

        def weights_out(i, v):
            CP[i][...] = v.astype(BF16).reshape(CP[i].shape)
            put(CP[i].at[:, :, lanes(1 - y)], C1[i], r.ccs.at[4 * i], r.ccr.at[4 * i], (ynb, c))

        def weights_along_z(i):
            take(C1[i], r.ccr.at[4 * i])
            C1[i][...] = (C1[i][...].astype(F32) + CP[i][:, :, lanes(y)].astype(F32)).astype(BF16)
            C3[i][z] = C1[i][z]
            for p in range(1, Z):
                to = lax.rem(z + p, Z)
                put(C1[i].at[to], C3[i].at[z], r.ccs.at[4 * i + 1], r.ccr.at[4 * i + 1], (to * 2 + y, c))

        def weights_back_z(i):
            take(C3[i].at[pl.ds(0, Z - 1)], r.ccr.at[4 * i + 1])
            v = C3[i][0].astype(F32)
            for p in range(1, Z):
                v = v + C3[i][p].astype(F32)
            CF[i][z, :, lanes(y)] = v.astype(BF16)
            for p in range(1, Z):
                to = lax.rem(z + p, Z)
                mine = CF[i].at[z, :, lanes(y)]
                put(mine, mine, r.ccs.at[4 * i + 2], r.ccr.at[4 * i + 2], (to * 2 + y, c))

        def weights_back_y(i):
            take(CF[i].at[pl.ds(0, Z - 1), :, pl.ds(0, half_w)], r.ccr.at[4 * i + 2])
            mine = CF[i].at[:, :, lanes(y)]
            put(mine, mine, r.ccs.at[4 * i + 3], r.ccr.at[4 * i + 3], (ynb, c))

    G, GOR = r.gbe, r.gor
    take(GOR, r.gorr)

    @pl.loop(0, rows // BLK)
    def _(i):
        v = GO[k, block(i), :] + GOR[block(i), :]
        GOR[block(i), :] = v
        G[block(i, EDGE), :] = v.astype(BF16)

    put(G.at[pl.ds(EDGE, EDGE)], G.at[pl.ds(rows + EDGE, EDGE)], r.gs.at[0], r.gr.at[0], left_dev)
    put(G.at[pl.ds(rows, EDGE)], G.at[pl.ds(0, EDGE)], r.gs.at[1], r.gr.at[1], right_dev)
    GA, GP = r.ga, r.gp
    GA[EDGE : EDGE + rows, :] = nt(G[EDGE : EDGE + rows, :], mixf)

    def pull_two(at):
        v = normed2_of(CV[at, :])
        g = GA[at, :] * gelu_slope(v * gain2 + off2)
        GP[at, :] = g
        return g * v, g

    gs_, ss_ = lax.fori_loop(0, rows // BLK, row_sums(lambda i: pull_two(block(i, EDGE))), (zero_h, zero_h))
    spread(r.sa2, (gs_, ss_))
    sum_start(2)
    at(2)
    MP = r.mp
    mp = nn(r.a2t[...], G[EDGE : EDGE + rows, :]).astype(BF16).reshape(C, LANES, width)
    for p in range(C):
        MP[p % 2, p // 2] = mp[p, 0:cr, :]
    put(MP.at[1 - k], r.mr, r.mps.at[0], r.mpr.at[0], (s, other))
    at(3)
    sum_middle(2)
    HX = r.hbx
    take(HX, r.hbrem.at[0])
    HX[...] = HX[...] + HB[...]

    @pl.loop(1, S)
    def _(p):
        put(HX, r.hbf.at[s], r.hbsem.at[1], r.hbrem.at[1], (lax.rem(s + p, S), c))

    r.hbf[s] = HX[...]
    at(4)
    take(r.mr, r.mpr.at[0])
    MR = r.mr
    MR[...] = (MR[...].astype(F32) + MP[k].astype(F32)).astype(BF16)
    put(MR.at[xo], r.mx, r.mps.at[1], r.mpr.at[1], (s, xnb))
    at(5)
    take(r.xedge, r.gr.at[0])
    take(r.xedge, r.gr.at[1])
    for e in (0, rows + EDGE):
        GA[e : e + EDGE, :] = nt(G[e : e + EDGE, :], mixf)
        pull_two(slice(e, e + EDGE))
    at(6)
    total2, gsum2, ssum2 = sum_end(2, hp)
    r.tot[...] = total2
    r.g2[...] = r.tot[pl.ds(c, 1), 0:cr].reshape(cr)
    r.b2[...] = r.tot[pl.ds(C + c, 1), 0:cr].reshape(cr)
    coef2 = gain2 * scale2
    gmean2, smean2 = gsum2 * inv_bins, ssum2 * inv_bins
    GC, GB = r.gce, r.gcb

    def conv_grad(at):
        return (coef2 * (GP[at, :] - smean2 - normed2_of(CV[at, :]) * gmean2)).astype(BF16)

    hx = hp // 2

    @pl.loop(0, rows // BLK)
    def _(i):
        v = conv_grad(block(i, EDGE))
        GC[block(i, EDGE), :] = v.astype(F32)
        GB[0, block(i), :] = v[:, :hx]
        GB[1, block(i), :] = v[:, hx:]

    put(GB.at[xo], r.gcx, r.gbs, r.gbr, (s, xnb))
    take(r.mx, r.mpr.at[1])
    mix_sum = MR[xi].astype(F32) + r.mx[...].astype(F32)
    if fused:
        weights_out(0, mix_sum)
    else:
        r.mwg[...] = mix_sum
    GC[0:EDGE, :] = jnp.where(left_same, conv_grad(slice(0, EDGE)).astype(F32), 0.0)
    GC[rows + EDGE : ext, :] = jnp.where(right_same, conv_grad(slice(rows + EDGE, ext)).astype(F32), 0.0)
    at(7)


    G1 = r.ga1
    for t in range(TAPS):
        lo_t = EDGE + STEP - t * STEP
        part = nn(GC[lo_t : lo_t + rows, :].astype(BF16), CM[t].reshape(hp, width))
        G1[...] = part if t == 0 else G1[...] + part

    def pull_one(i):
        v = normed1_of(r.x[block(i), :].astype(F32))
        g = G1[block(i), :] * gelu_slope(v * gain1 + off1)
        G1[block(i), :] = g
        return g * v, g

    g1s, s1s = lax.fori_loop(0, rows // BLK, row_sums(pull_one), (zero_w, zero_w))
    spread(r.sa3, (g1s, s1s))
    sum_start(3)
    at(8)

    take(r.actx, r.ar_)
    take(r.gcx, r.gbr)
    ZP, CG = r.zpad, r.cg
    pad = ZP.shape[0] - rows
    ZP[0 : pad // 2, :] = jnp.zeros((pad // 2, hx), F32)
    ZP[rows + pad // 2 :, :] = jnp.zeros((pad // 2, hx), F32)
    for part in range(2):
        ZP[pad // 2 : pad // 2 + rows, :] = (GB[xi] if part == 0 else r.gcx[...]).astype(F32)
        rows_act = A[lo : lo + ext, :] if part == 0 else r.actx[...]
        for t in range(TAPS):
            lo_t = pad // 2 - EDGE + STEP - t * STEP
            v = nn(ZP[lo_t : lo_t + ext, :].T.astype(BF16), rows_act).reshape(2, LANES, width)
            CG[t] = v if part == 0 else CG[t] + v
    if fused:
        weights_along_z(0)
    put(CG.at[:, 1 - k, pl.ds(0, cr)], r.cgr, r.cgs, r.cgrr, (s, other))
    at(9)
    sum_middle(3)
    at(10)
    total1, gsum1, ssum1 = sum_end(3, width)
    r.g1[...] = gsum1.reshape(width)
    r.b1[...] = ssum1.reshape(width)
    coef1 = gain1 * scale1
    gmean1, smean1 = gsum1 * inv_bins, ssum1 * inv_bins

    @pl.loop(0, rows // BLK)
    def _(i):
        v = normed1_of(r.x[block(i), :].astype(F32))
        r.ig[block(i), :] = GOR[block(i), :] + coef1 * (G1[block(i), :] - smean1 - v * gmean1)

    at(11)

    take(r.cgr, r.cgrr)
    conv_sum = [CG[t, k, 0:cr, :] + r.cgr[t] for t in range(TAPS)]
    if fused:
        weights_out(1, jnp.concatenate([conv_sum[0], conv_sum[1][0:64]], axis=0))
        weights_out(2, jnp.concatenate([conv_sum[1][64:], conv_sum[2]], axis=0))
        at(12)
    else:
        for t in range(TAPS):
            r.cwg[t] = conv_sum[t]
        r.wgo[...] = WG[...]

    take(r.hbf.at[pl.ds(0, S - 1)], r.hbrem.at[1])
    HB3 = r.hb3
    HB3[...] = lax.fori_loop(1, S, lambda p, a: a + r.hbf[p], r.hbf[0])
    put(HB3, r.hbp, r.hbsem.at[2], r.hbrem.at[2], (s, other))
    at(13)

    if fused:
        weights_along_z(1)
        weights_along_z(2)
        at(14)
        weights_back_z(0)
        weights_back_z(1)
        weights_back_z(2)
        at(15)
        weights_back_y(0)
        weights_back_y(1)
        weights_back_y(2)
        at(16)
        for i in range(3):
            take(CF[i].at[:, :, pl.ds(0, half_w)], r.ccr.at[4 * i + 3])
        r.mwg[...] = CF[0][...].reshape(cr, width).astype(F32)
        v = CF[1][...].reshape(cr + 64, width).astype(F32)
        r.cwg[0] = v[0:cr]
        r.cwg[1, 0:64, :] = v[cr:]
        v = CF[2][...].reshape(2 * cr - 64, width).astype(F32)
        r.cwg[1, 64:, :] = v[0 : cr - 64]
        r.cwg[2] = v[cr - 64 :]
        at(17)
    take(r.hbp, r.hbrem.at[2])

    def in_order(dst, human, mouse):
        for m in range(M0 // HW):
            dst[:, m * HW : (m + 1) * HW] = human(m // NCHUNK, m % NCHUNK)
        edge = M0 // HW * HW
        v = human(edge // HALF_H, edge // HW % NCHUNK)
        if edge < M0:
            dst[:, edge:M0] = v[:, 0 : M0 - edge]
        before = v[:, M0 - edge : M0 - edge + LANES]
        lane = lax.broadcasted_iota(jnp.int32, (1, LANES), 1)
        for m in range(pl.cdiv(tracks - M0, LANES)):
            here = mouse(m // NCHUNK, m % NCHUNK) if m < 2 * NCHUNK else jnp.zeros_like(before)
            moved = pltpu.roll(here, OFF, 1)
            out = jnp.where(lane < OFF, before, moved)
            n = min(LANES, tracks - M0 - m * LANES)
            dst[:, M0 + m * LANES : M0 + m * LANES + n] = out[:, 0:n]
            before = moved

    HO = r.hbo
    HO[0] = jnp.where(k == 0, HB3[...], r.hbp[...])
    HO[1] = jnp.where(k == 0, r.hbp[...], HB3[...])
    in_order(r.hbrow, lambda h, j: HO[h, j : j + 1, 0:HW], lambda h, j: HO[h, j : j + 1, HW:CW])
    r.hb[...] = r.hbrow[...].reshape(tracks)
    if fused:
        for j in range(NCHUNK):
            take(r.fr.at[j], r.g4r.at[j])

        def piece(h, j, at, n):
            return jnp.where(k == h, r.fin[j, k, :, at : at + n], r.fr[j, :, at : at + n])

        in_order(r.hg, lambda h, j: piece(h, j, 0, HW), lambda h, j: piece(h, j, HW, MW))

    for i in range(4):
        take(r.ba[i].at[pl.ds(0, C - 1)], r.ars.at[2 * i])
        take(r.bb[i].at[pl.ds(0, S - 1)], r.ars.at[2 * i + 1])
    take(r.xl, r.hs.at[0])
    take(r.xr, r.hs.at[1])
    take(CM.at[0, 0, pl.ds(0, cr)], r.cms.at[0])
    take(CM.at[0, 0, pl.ds(0, cr), pl.ds(0, half_w)], r.cms.at[1])
    take(CS, r.cms.at[2])
    take(CM.at[0, 0, pl.ds(0, cr)], r.cms.at[3])
    take(CM.at[0, 0, pl.ds(0, cr)], r.cms.at[4])
    take(CM.at[0, 0, pl.ds(0, cr), pl.ds(0, half_w)], r.cms.at[5])
    take(CS, r.cms.at[6])
    take(r.gsb.at[pl.ds(0, C - 1)], r.gss)
    take(W.at[:, 0], r.wps)
    take(TG.at[:, 0], r.tps)
    take(W.at[:, pl.ds(0, 3), 0], r.wxs)
    take(W.at[:, pl.ds(0, 2), 0], r.wrs.at[0])
    take(W.at[:, pl.ds(0, 2), 0], r.wrs.at[1])
    take(W.at[:, 0, 0], r.wrs.at[2])
    take(r.actx, r.as_)
    take(O.at[0], r.os)
    take(GOR, r.gos)
    take(HX, r.hbsem.at[0])
    take(r.hbf.at[pl.ds(0, S - 1)], r.hbsem.at[1])
    take(HB3, r.hbsem.at[2])
    take(r.xedge, r.gs.at[0])
    take(r.xedge, r.gs.at[1])
    take(r.mr, r.mps.at[0])
    take(r.mx, r.mps.at[1])
    take(r.gcx, r.gbs)
    take(r.cgr, r.cgs)
    if fused:
        for i in range(3):
            take(C1[i], r.ccs.at[4 * i])
            take(C3[i].at[pl.ds(0, Z - 1)], r.ccs.at[4 * i + 1])
            take(CF[i].at[pl.ds(0, Z - 1), :, pl.ds(0, half_w)], r.ccs.at[4 * i + 2])
            take(CF[i].at[:, :, pl.ds(0, half_w)], r.ccs.at[4 * i + 3])
        for j in range(NCHUNK):
            take(R1.at[j], r.s1.at[j])
            take(R2.at[j], r.s2.at[j])
            take(R3.at[j, pl.ds(0, Z - 1)], r.s3.at[j])
            take(r.fr.at[j], r.s4.at[j])


def fused_step(seqs, chs, **ins):
    S, C = seqs, chs
    rows, width = ins["x"].shape
    n_dev = S * C
    hp = C * LANES
    cr = ins["mix"].shape[0]
    kr = ins["hw"].shape[1]
    tracks = ins["bias"].shape[0]
    ext = rows + 2 * EDGE
    Z = S // 2
    fused = width % (n_dev * 8) == 0 and Z == 4
    two = 2 * (width // n_dev)
    vm = pltpu.VMEM
    dma = pltpu.SemaphoreType.DMA
    any_ins = ("hw", "counts")
    outs = dict(
        out=((rows, width), BF16),
        ig=((rows, width), F32),
        g1=((width,), F32),
        b1=((width,), F32),
        cwg=((TAPS, cr, width), F32),
        g2=((cr,), F32),
        b2=((cr,), F32),
        mwg=((cr, width), F32),
        hb=((tracks,), F32),
    )
    if fused:
        outs["hg"] = ((two // 2, tracks), F32)
    else:
        outs["wgo"] = ((NCHUNK, Z, 2, 2, width // (4 * Z), HW), BF16)
    scratch = dict(
        xl=vm((HALO, width), BF16),
        xr=vm((HALO, width), BF16),
        xedge=vm((EDGE, width), BF16),
        gs2=vm((8, LANES), F32),
        gsb=vm((C, 8, LANES), F32),
        cm=vm((4, cr, width), BF16),
        cmf=vm((4, C, LANES, width), BF16),
        hwv=vm((4, kr, tracks), BF16),
        mwv=vm((4, kr, 2 * HALF_M), BF16),
        cbuf=vm((HUMAN, rows), jnp.int32),
        ctail=vm((HW - MW, rows), jnp.int32),
        hbpad=vm((1, HUMAN // LANES * LANES + (2 * NCHUNK + 1) * LANES), F32),
        bias_rows=vm((16, CW), F32),
        wbuf=vm((NCHUNK, 4, 4, kr, CW), BF16),
        tgb=vm((NCHUNK, 2, rows, HW), BF16),
        tgx=vm((NCHUNK, rows, HW), BF16),
        act=vm((rows + 2 * HALO, width), BF16),
        actx=vm((ext, width), BF16),
        prod=vm((TAPS, rows + 2 * HALO, hp), F32),
        cv=vm((ext, hp), F32),
        a2=vm((rows, hp), BF16),
        a2t=vm((hp, rows), BF16),
        ob=vm((2, rows, width), BF16),
        ot=vm((width, 2 * rows), BF16),
        wsel=vm((width, HW), BF16),
        lg=vm((2 * rows, HW), F32),
        gl=vm((2 * rows, HW), BF16),
        wg=vm((NCHUNK, Z, 2, 2, width // (4 * Z), HW), BF16),
        go=vm((2, rows, width), F32),
        gor=vm((rows, width), F32),
        hbs=vm((8, CW), F32),
        hbx=vm((8, CW), F32),
        hbf=vm((S, 8, CW), F32),
        hb3=vm((8, CW), F32),
        hbp=vm((8, CW), F32),
        hbo=vm((2, 8, CW), F32),
        hbrow=vm((1, tracks), F32),
        gbe=vm((ext, width), BF16),
        ga=vm((ext, hp), F32),
        gp=vm((ext, hp), F32),
        gce=vm((ext, hp), F32),
        gcb=vm((2, rows, hp // 2), BF16),
        gcx=vm((rows, hp // 2), BF16),
        ga1=vm((rows, width), F32),
        mp=vm((2, 2, cr, width), BF16),
        mr=vm((2, cr, width), BF16),
        mx=vm((cr, width), BF16),
        zpad=vm((rows + 64, hp // 2), F32),
        cg=vm((TAPS, 2, LANES, width), F32),
        cgr=vm((TAPS, cr, width), F32),
        tot=vm((8, LANES), F32),
    )
    for i, n in enumerate((16, 8, 8, 16)):
        scratch[f"sa{i}"] = vm((n, LANES), F32)
        scratch[f"sb{i}"] = vm((n, LANES), F32)
        scratch[f"ba{i}"] = vm((C, n, LANES), F32)
        scratch[f"bb{i}"] = vm((S, n, LANES), F32)
    sems = dict(
        ars=8, arr=8, hs=2, hr=2, cms=7, cmr=7, gss=0, gsr=0, ld=2, wl=7, wp=7, wx=7, wy=7, wz=7, wd=7, wps=0, wxs=0,
        wrs=3, tp=7, tps=0, as_=0, ar_=0, os=0, gos=0, gorr=0, hbsem=3, hbrem=3, gs=2, gr=2, mps=2, mpr=2, gbs=0,
        gbr=0, cgs=0, cgrr=0, orr=0,
    )
    if fused:
        scratch.update(
            acc1=vm((NCHUNK, Z, 2, two, CW), BF16),
            r1=vm((NCHUNK, Z, 2, two, HW), BF16),
            r2=vm((NCHUNK, Z, two, CW), BF16),
            r3=vm((NCHUNK, Z, two, CW), BF16),
            fin=vm((NCHUNK, 2, two // 2, CW), F32),
            fr=vm((NCHUNK, two // 2, CW), F32),
        )
        for i, n in enumerate((cr, cr + 64, 2 * cr - 64)):
            scratch[f"cp{i}"] = vm((Z, n // Z, width), BF16)
            scratch[f"c1{i}"] = vm((Z, n // Z, width // 2), BF16)
            scratch[f"c3{i}"] = vm((Z, n // Z, width // 2), BF16)
            scratch[f"cf{i}"] = vm((Z, n // Z, width), BF16)
        sems.update(s1=7, s2=7, s3=7, s4=7, g1r=7, g2r=7, g3r=7, g4r=7, ccs=12, ccr=12)
    for name, n in sems.items():
        scratch[name] = dma((n,)) if n else dma
    names = [*ins, *outs, *scratch]

    def space(name):
        if name == "species":
            return pl.BlockSpec(memory_space=pltpu.SMEM)
        return pl.BlockSpec(memory_space=pl.ANY if name in any_ins else pltpu.VMEM)

    got = pl.pallas_call(
        functools.partial(kernel_body, S, C, fused, names),
        out_shape=[jax.ShapeDtypeStruct(*v) for v in outs.values()],
        in_specs=[space(n) for n in ins],
        out_specs=[pl.BlockSpec(memory_space=pltpu.VMEM) for _ in outs],
        scratch_shapes=list(scratch.values()),
        compiler_params=pltpu.CompilerParams(
            collective_id=0, has_side_effects=True, vmem_limit_bytes=67_043_328
        ),
    )(*ins.values())
    return types.SimpleNamespace(**dict(zip(outs, got, strict=True))), fused


def handed_on(values):
    def body(*refs):
        n = len(values)
        sems = refs[2 * n]
        for i in range(n):
            pltpu.make_async_copy(refs[i], refs[n + i], sems.at[i]).start()
        for i in range(n):
            pltpu.make_async_copy(refs[i], refs[n + i], sems.at[i]).wait()

    return pl.pallas_call(
        body,
        out_shape=[jax.ShapeDtypeStruct(v.shape, v.dtype) for v in values],
        in_specs=[pl.BlockSpec(memory_space=pltpu.VMEM) for _ in values],
        out_specs=[pl.BlockSpec(memory_space=pl.ANY) for _ in values],
        scratch_shapes=[pltpu.SemaphoreType.DMA((len(values),))],
    )(*values)


def on_device(
    inputs, gain_one, shift_one, conv_weight, gain_two, shift_two, mix_weight, head_weight, head_bias, species, counts
):
    S, C = lax.axis_size("seq"), lax.axis_size("ch")
    s, c = lax.axis_index("seq"), lax.axis_index("ch")
    rows, width = inputs.shape
    depth, tracks = head_weight.shape
    o, fused = fused_step(
        S,
        C,
        x=inputs,
        gain1=gain_one,
        shift1=shift_one,
        cw=jnp.transpose(conv_weight, (0, 2, 1)),
        gain2=gain_two,
        shift2=shift_two,
        mix=mix_weight,
        hw=head_weight.reshape(4, depth // 4, tracks),
        bias=head_bias,
        species=species,
        counts=jnp.transpose(counts),
    )
    cwg, mwg = o.cwg, o.mwg
    if fused:
        head_weight_grad = o.hg
    else:
        cwg, mwg = lax.psum((cwg, mwg), "seq")
        part = o.wgo.reshape(NCHUNK, width, HW).astype(F32)
        part = jnp.transpose(part, (1, 0, 2))
        k = lax.rem(c, 2)
        human = jnp.zeros((width, 2, HALF_H), F32).at[:, k].set(part.reshape(width, HALF_H))
        mouse = jnp.zeros((width, 2, HALF_M), F32).at[:, k].set(part[:, :, :MW].reshape(width, HALF_M))
        first = (s * C + c // 2 * 2) * rows
        window = jnp.mod(first - SHIFT, rows * S * C) // WINDOW_BINS
        is_h = jnp.sum(jnp.where(jnp.arange(species.shape[0], dtype=jnp.int32) == window, species, 0)) == 0
        human = jnp.where(is_h, human.reshape(width, 2 * HALF_H)[:, :HUMAN], 0.0)
        mouse = jnp.where(is_h, 0.0, mouse.reshape(width, 2 * HALF_M)[:, :MOUSE])
        head_weight_grad = lax.psum_scatter(
            jnp.concatenate([human, mouse], axis=1), ("seq", "ch"), scatter_dimension=0, tiled=True
        )
    if fused:
        names = list(vars(o))
        o = types.SimpleNamespace(**dict(zip(names, handed_on(list(vars(o).values())), strict=True)))
        cwg, mwg, head_weight_grad = o.cwg, o.mwg, o.hg
    return (
        o.out,
        o.ig,
        o.g1,
        o.b1,
        jnp.transpose(cwg, (0, 2, 1)),
        o.g2,
        o.b2,
        mwg,
        head_weight_grad,
        o.hb,
    )


def solution(mesh):
    rows = P(("seq", "ch"), None)
    in_specs = (
        rows, P(), P(), P(None, None, "ch"), P("ch"), P("ch"), P("ch", None), P("ch", None), P(), P(), rows,
    )
    out_specs = (
        rows, rows, P(), P(), P(None, None, "ch"), P("ch"), P("ch"), P("ch", None), rows, P(),
    )
    return jax.shard_map(on_device, mesh=mesh, in_specs=in_specs, out_specs=out_specs, check_vma=False)
```

```python
import functools
import math
import types

import jax
import jax.numpy as jnp
from jax import lax
from jax.experimental import pallas as pl
from jax.experimental.pallas import tpu as pltpu
from jax.sharding import PartitionSpec as P

HUMAN = 5313
MOUSE = 1643
STEP = 11
TAPS = 3
WINDOW_BINS = 1024
SHIFT = 512
EPS = 1e-05

LANES = 128
NCHUNK = 7
HW = 384
MW = 128
CW = HW + MW
HALF_H = NCHUNK * HW
HALF_M = NCHUNK * MW
HALO = 32
EDGE = 16
MESH = pl.DeviceIdType.MESH
F32 = jnp.float32
BF16 = jnp.bfloat16
K0 = math.sqrt(2.0 / math.pi)
K1 = K0 * 0.044715


PLAN = {
    100: ((6, 4), (6, 0), (6, 3)),
    101: ((5, 4), (6, 1), (5, 0)),
    102: ((5, 3),),
    103: ((6, 2), (6, 5), (6, 6)),
    104: ((5, 1), (5, 2), (0, 0)),
    105: ((5, 5),),
    110: ((5, 6),),
    112: ((1, 1), (1, 0)),
    114: ((1, 2),),
    2: ((2, 1), (2, 2)),
    5: ((1, 5),),
    6: ((2, 0), (3, 1), (3, 2)),
    8: ((3, 0), (1, 4), (2, 5)),
    9: ((4, 1), (4, 2)),
    10: ((1, 3),),
    12: ((1, 6),),
    13: ((3, 5),),
    14: ((2, 4), (4, 0), (2, 3)),
    15: ((2, 6), (4, 5), (3, 3), (3, 4)),
    16: ((3, 6),),
    17: ((4, 3), (4, 4), (4, 6)),
}
X_FIRST = (2, 3, 6)


def nn(a, b):
    return lax.dot_general(a, b, (((1,), (0,)), ((), ())), preferred_element_type=F32)


def nt(a, b):
    return lax.dot_general(a, b, (((1,), (1,)), ((), ())), preferred_element_type=F32)


def gelu(v):
    return 0.5 * v * (1.0 + jnp.tanh(v * (K0 + K1 * (v * v))))


def gelu_slope(v):
    v2 = v * v
    th = jnp.tanh(v * (K0 + K1 * v2))
    return 0.5 * (1.0 + th) + 0.5 * v * (1.0 - th * th) * (K0 + 3.0 * K1 * v2)


def poisson_grad(logits, target):
    t = jnp.exp(-jnp.abs(logits))
    up = 1.0 + t
    series = t * (1.0 - t * (0.5 - t * (1.0 / 3.0 - t * 0.25)))
    rate = jnp.maximum(logits, 0.0) + jnp.where(t < 0.015625, series, jnp.log(up))
    return jnp.where(logits >= 0.0, 1.0, t) * (rate - target) / (up * rate)


def take(ref, sem):
    pltpu.make_async_copy(ref, ref, sem).wait()


def kernel_body(seqs, chs, fused, names, *refs):
    r = types.SimpleNamespace(**dict(zip(names, refs, strict=True)))
    r.sa, r.sb, r.ba, r.bb = ([getattr(r, f"{n}{i}") for i in range(4)] for n in ("sa", "sb", "ba", "bb"))
    S, C = seqs, chs
    s = lax.axis_index("seq")
    c = lax.axis_index("ch")
    xi = c // 2
    k = lax.rem(c, 2)
    other = c + 1 - 2 * k
    xnb = lax.rem(c + 2, C)
    xo = 1 - xi
    y = lax.rem(s, 2)
    z = s // 2
    ynb = s + 1 - 2 * y
    zb = lax.rem(z, 2)
    znb = s + 2 - 4 * zb
    dnb = znb + 1 - 2 * y
    q = lax.rem(s, 4)
    q_y = q + 1 - 2 * y
    q_z = q + 2 - 4 * zb
    q_d = q_z + 1 - 2 * y
    rows, width = r.x.shape
    n_dev = S * C
    total_bins = rows * n_dev
    inv_bins = 1.0 / total_bins
    me = s * C + c
    left = lax.rem(me + n_dev - 1, n_dev)
    right = lax.rem(me + 1, n_dev)
    left_dev = (left // C, lax.rem(left, C))
    right_dev = (right // C, lax.rem(right, C))
    row0 = me * rows
    window = lax.rem(row0 + total_bins - SHIFT, total_bins) // WINDOW_BINS
    left_same = lax.rem(row0 + total_bins - 1 + total_bins - SHIFT, total_bins) // WINDOW_BINS == window
    right_same = lax.rem(row0 + rows + total_bins - SHIFT, total_bins) // WINDOW_BINS == window

    def human_at_chip(seq, chip):
        first = (seq * C + chip * 2) * rows
        return r.species[lax.rem(first + total_bins - SHIFT, total_bins) // WINDOW_BINS] == 0

    mine_h = human_at_chip(s, xi)
    x_h = human_at_chip(s, xo)
    y_h = human_at_chip(ynb, xi)
    hp = C * LANES

    def put(src, dst, send, recv, dev):
        pltpu.make_async_remote_copy(
            src_ref=src, dst_ref=dst, send_sem=send, recv_sem=recv, device_id=dev, device_id_type=MESH
        ).start()

    barrier = pltpu.get_barrier_semaphore()

    def greet(dev):
        pl.semaphore_signal(barrier, inc=1, device_id=dev, device_id_type=MESH)

    for i in range(1, C):
        greet((s, lax.rem(c + i, C)))

    @pl.loop(1, S)
    def _(i):
        greet((lax.rem(s + i, S), c))

    greet(left_dev)
    greet(right_dev)

    W, TG = r.wbuf, r.tgb

    def human_at(half, j):
        return pl.ds(pl.multiple_of(half * HALF_H + j * HW, LANES), HW)

    def mouse_at(half, j):
        return pl.ds(pl.multiple_of(half * HALF_M + j * MW, LANES), MW)

    HV, MV, CB = r.hwv, r.mwv, r.cbuf
    load_hw = pltpu.make_async_copy(r.hw, HV, r.ld.at[0])
    load_hw.start()
    load_counts = pltpu.make_async_copy(r.counts, CB, r.ld.at[1])
    load_counts.start()
    CM, CS = r.cmf, r.cm
    cr = CS.shape[1]
    for t in range(TAPS):
        CS[t] = r.cw[t]
        CM[t, c, 0:cr, :] = r.cw[t]
    CS[TAPS] = r.mix[...]
    CM[TAPS, c, 0:cr, :] = r.mix[...]
    for t in range(4):
        for p in range(C):
            CM[t, p, cr:LANES, :] = jnp.zeros((LANES - cr, width), BF16)
    r.gs2[...] = jnp.zeros(r.gs2.shape, F32)
    r.gs2[0:1, 0:cr] = r.gain2[...].reshape(1, cr)
    r.gs2[1:2, 0:cr] = r.shift2[...].reshape(1, cr)
    M0 = HUMAN // LANES * LANES
    OFF = HUMAN - M0
    HP = r.hbpad
    tracks = HUMAN + MOUSE
    HP[:, 0:tracks] = r.bias[...].reshape(1, tracks)
    HP[:, tracks:] = jnp.zeros((1, HP.shape[1] - tracks), F32)
    BR = r.bias_rows
    for m in range(2 * NCHUNK):
        BR[m : m + 1, 0:HW] = HP[:, m * HW : (m + 1) * HW]
        v = HP[:, M0 + m * LANES : M0 + (m + 2) * LANES]
        BR[m : m + 1, HW:CW] = pltpu.roll(v, 2 * LANES - OFF, 1)[:, :MW]

    def spread(ref, vecs):
        n = vecs[0].shape[1] // LANES
        for i, v in enumerate(vecs):
            for t in range(n):
                ref[i * n + t : i * n + t + 1, :] = v[:, t * LANES : (t + 1) * LANES]
        if ref.shape[0] > n * len(vecs):
            ref[n * len(vecs) :, :] = jnp.zeros((ref.shape[0] - n * len(vecs), LANES), F32)

    def collect(v, n):
        m = n // LANES
        return [jnp.concatenate([v[i * m + t : i * m + t + 1, :] for t in range(m)], axis=1) for i in range(2)]

    def sum_start(i):
        src, bufs = r.sa[i], r.ba[i]
        for p in range(1, C):
            put(src, bufs.at[c], r.ars.at[2 * i], r.arr.at[2 * i], (s, lax.rem(c + p, C)))
        bufs[c] = src[...]

    def sum_middle(i):
        src, bufs, far = r.sb[i], r.ba[i], r.bb[i]
        take(bufs.at[pl.ds(0, C - 1)], r.arr.at[2 * i])
        v = bufs[0]
        for p in range(1, C):
            v = v + bufs[p]
        src[...] = v

        @pl.loop(1, S)
        def _(p):
            put(src, far.at[s], r.ars.at[2 * i + 1], r.arr.at[2 * i + 1], (lax.rem(s + p, S), c))

        far[s] = v

    def sum_end(i, n):
        far = r.bb[i]
        take(far.at[pl.ds(0, S - 1)], r.arr.at[2 * i + 1])
        if S <= 8:
            v = far[0]
            for p in range(1, S):
                v = v + far[p]
        else:
            v = lax.fori_loop(1, S, lambda p, a: a + far[p], far[0])
        return v, *collect(v, n)

    BLK = 32

    def block(i, shift=0):
        return pl.ds(pl.multiple_of(i * BLK + shift, 16), BLK)

    def row_sums(terms):
        def step(i, carry):
            return tuple(a + jnp.sum(t, 0, keepdims=True) for a, t in zip(carry, terms(i), strict=True))

        return step

    zero_w = jnp.zeros((1, width), F32)

    def x_terms(i):
        v = r.x[block(i), :].astype(F32)
        return v, v * v

    s1, q1 = lax.fori_loop(0, rows // BLK, row_sums(x_terms), (zero_w, zero_w))
    spread(r.sa0, (s1, q1))
    load_hw.wait()
    full = (tracks - M0) // LANES - 1
    for p in range(4):
        for m in range(2 * NCHUNK):
            if m < full:
                v = HV[p, :, M0 + m * LANES : M0 + (m + 2) * LANES].astype(F32)
                v = pltpu.roll(v, 2 * LANES - OFF, 1)[:, :MW]
            elif M0 + m * LANES < tracks:
                v = HV[p, :, M0 + m * LANES : min(tracks, M0 + (m + 2) * LANES)].astype(F32)
                v = jnp.concatenate([v, jnp.zeros((v.shape[0], 2 * LANES - v.shape[1]), F32)], axis=1)
                v = pltpu.roll(v, 2 * LANES - OFF, 1)[:, :MW]
            else:
                v = jnp.zeros((HV.shape[1], MW), F32)
            MV[p, :, m * MW : (m + 1) * MW] = v.astype(BF16)

    @pl.loop(0, NCHUNK)
    def _(j):
        pltpu.make_async_copy(HV.at[:, :, human_at(k, j)], W.at[j, c, :, :, pl.ds(0, HW)], r.wl.at[j]).start()
        pltpu.make_async_copy(MV.at[:, :, mouse_at(k, j)], W.at[j, c, :, :, pl.ds(HW, MW)], r.wl.at[j]).start()

    pl.semaphore_wait(barrier, C - 1 + S - 1 + 2)

    sum_start(0)
    put(r.x.at[pl.ds(rows - HALO, HALO)], r.xl, r.hs.at[0], r.hr.at[0], right_dev)
    put(r.x.at[pl.ds(0, HALO)], r.xr, r.hs.at[1], r.hr.at[1], left_dev)
    half_w = width // 2
    put(CS.at[q], CM.at[q, c, pl.ds(0, cr)], r.cms.at[0], r.cmr.at[0], (s, xnb))
    put(
        CS.at[q_d, :, pl.ds(0, half_w)],
        CM.at[q_d, c, pl.ds(0, cr), pl.ds(0, half_w)],
        r.cms.at[1],
        r.cmr.at[1],
        (s, xnb),
    )
    put(CS, CM.at[:, c, pl.ds(0, cr)], r.cms.at[2], r.cmr.at[2], (s, other))
    for p in range(1, C):
        put(r.gs2, r.gsb.at[c], r.gss, r.gsr, (s, lax.rem(c + p, C)))
    r.gsb[c] = r.gs2[...]

    @pl.loop(0, NCHUNK)
    def _(j):
        put(
            HV.at[:, :, human_at(1 - k, j)], W.at[j, c, :, :, pl.ds(0, HW)],
            r.wps, r.wp.at[j], (s, other),
        )
        put(
            MV.at[:, :, mouse_at(1 - k, j)], W.at[j, c, :, :, pl.ds(HW, MW)],
            r.wps, r.wp.at[j], (s, other),
        )
    HALFC = CW // 2

    def heads_along_x(j):
        for h in range(2):
            dev = (s, xo * 2 + h)
            hc = pl.multiple_of(h * HALF_H + j * HW, LANES)
            put(HV.at[q, :, human_at(h, j)], W.at[j, c, q, :, pl.ds(0, HW)], r.wxs, r.wx.at[j], dev)
            put(MV.at[q, :, mouse_at(h, j)], W.at[j, c, q, :, pl.ds(HW, MW)], r.wxs, r.wx.at[j], dev)
            put(
                HV.at[q_d, :, pl.ds(hc, HALFC)], W.at[j, c, q_d, :, pl.ds(0, HALFC)],
                r.wxs, r.wx.at[j], dev,
            )

    def relay_heads(j):
        take(W.at[j, pl.ds(0, 3), 0], r.wx.at[j])
        far = pl.ds(xo * 2, 2)
        put(W.at[j, far, q], W.at[j, far, q], r.wrs.at[0], r.wy.at[j], (ynb, c))
        put(W.at[j, far, q], W.at[j, far, q], r.wrs.at[1], r.wz.at[j], (znb, c))
        put(
            W.at[j, far, q, :, pl.ds(HALFC, HALFC)], W.at[j, far, q, :, pl.ds(HALFC, HALFC)],
            r.wrs.at[2], r.wd.at[j], (dnb, c),
        )

    def at(slot):
        for stage, j in PLAN.get(slot, ()):
            if stage == 0:
                put(A.at[pl.ds(HALO - EDGE, ext)], r.actx, r.as_, r.ar_, (s, xnb))
            elif stage == 5:
                relay_heads(j)
            elif stage == 6:
                heads_along_x(j)
            elif fused and stage == 4:
                last(j)
            elif fused:
                (first, second, third)[stage - 1](j, j in X_FIRST)

    ext = rows + 2 * EDGE
    at(100)

    def pass_weights():
        take(CM.at[0, 0, pl.ds(0, cr)], r.cmr.at[0])
        put(CM.at[q, xnb, pl.ds(0, cr)], CM.at[q, xnb, pl.ds(0, cr)], r.cms.at[3], r.cmr.at[3], (ynb, c))
        put(CM.at[q, xnb, pl.ds(0, cr)], CM.at[q, xnb, pl.ds(0, cr)], r.cms.at[4], r.cmr.at[4], (znb, c))
        second = pl.ds(half_w, half_w)
        put(
            CM.at[q, xnb, pl.ds(0, cr), second], CM.at[q, xnb, pl.ds(0, cr), second],
            r.cms.at[5], r.cmr.at[5], (dnb, c),
        )

    def targets(half, dst, j):
        at = pl.multiple_of(half * HALF_H + j * HW, 8)
        am = pl.multiple_of(half * HALF_M + j * MW, 8)
        v = CB[pl.ds(at, MW), :]
        dst[:, 0:MW] = jnp.where(mine_h, v, CB[pl.ds(am, MW), :]).astype(F32).T.astype(BF16)
        ends = (half == 1) & (j == NCHUNK - 1)

        @pl.when(ends)
        def _():
            dst[:, MW:HW] = CT[...].astype(F32).T.astype(BF16)

        @pl.when(jnp.logical_not(ends))
        def _():
            dst[:, MW:HW] = CB[pl.ds(at + MW, HW - MW), :].astype(F32).T.astype(BF16)

    load_counts.wait()
    CT = r.ctail
    whole = HUMAN - (2 * HALF_H - HW + MW)
    CT[0:whole, :] = CB[HUMAN - whole : HUMAN, :]
    CT[whole:, :] = jnp.zeros((CT.shape[0] - whole, CT.shape[1]), jnp.int32)
    sum_middle(0)
    pass_weights()

    @pl.loop(0, NCHUNK)
    def _(j):
        targets(k, TG.at[j, k], j)

    _, t1, u1 = sum_end(0, width)
    mean1 = t1 * inv_bins
    scale1 = lax.rsqrt(u1 * inv_bins - mean1 * mean1 + EPS)
    gain1 = r.gain1[...].reshape(1, width)
    off1 = r.shift1[...].reshape(1, width)

    A = r.act

    def normed1_of(v):
        return (v - mean1) * scale1

    def act_rows(v):
        return gelu(normed1_of(v.astype(F32)) * gain1 + off1)

    @pl.loop(0, rows // BLK)
    def _(i):
        at = pl.multiple_of(i * BLK, BLK)
        A[pl.ds(at + HALO, BLK), :] = act_rows(r.x[pl.ds(at, BLK), :]).astype(BF16)

    take(r.xl, r.hr.at[0])
    A[0:HALO, :] = jnp.where(left_same, act_rows(r.xl[...]), 0.0).astype(BF16)
    take(r.xr, r.hr.at[1])
    A[rows + HALO : rows + 2 * HALO, :] = jnp.where(right_same, act_rows(r.xr[...]), 0.0).astype(BF16)

    at(101)
    take(CM.at[0, 0, pl.ds(0, cr), pl.ds(0, half_w)], r.cmr.at[1])
    take(CM.at[0, 0, pl.ds(0, cr)], r.cmr.at[3])
    take(CM.at[0, 0, pl.ds(0, cr)], r.cmr.at[4])
    take(CM.at[0, 0, pl.ds(0, cr), pl.ds(0, half_w)], r.cmr.at[5])
    put(CM.at[:, xnb, pl.ds(0, cr)], CM.at[:, xnb, pl.ds(0, cr)], r.cms.at[6], r.cmr.at[6], (s, other))
    take(CM.at[:, 0, pl.ds(0, cr)], r.cmr.at[2])
    take(CM.at[:, 0, pl.ds(0, cr)], r.cmr.at[6])

    PR = r.prod
    for t in range(TAPS):
        PR[t] = nt(A[...], CM[t].reshape(hp, width))
    CV = r.cv
    lo = HALO - EDGE
    CV[...] = (
        PR[0, lo - STEP : lo - STEP + ext, :] + PR[1, lo : lo + ext, :] + PR[2, lo + STEP : lo + STEP + ext, :]
    )
    at(102)
    zero_h = jnp.zeros((1, hp), F32)

    def c_terms(i):
        v = CV[block(i, EDGE), :]
        return v, v * v

    s2, q2 = lax.fori_loop(0, rows // BLK, row_sums(c_terms), (zero_h, zero_h))
    spread(r.sa1, (s2, q2))
    sum_start(1)
    at(103)

    @pl.loop(0, NCHUNK)
    def _(j):
        targets(1 - k, r.tgx.at[j], j)
        put(r.tgx.at[j], TG.at[j, k], r.tps, r.tp.at[j], (s, other))

    sum_middle(1)
    at(104)
    _, t2, u2 = sum_end(1, hp)
    mean2 = t2 * inv_bins
    scale2 = lax.rsqrt(u2 * inv_bins - mean2 * mean2 + EPS)
    take(r.gsb.at[pl.ds(0, C - 1)], r.gsr)
    gain2 = jnp.concatenate([r.gsb[p, 0:1, :] for p in range(C)], axis=1)
    off2 = jnp.concatenate([r.gsb[p, 1:2, :] for p in range(C)], axis=1)

    def normed2_of(v):
        return (v - mean2) * scale2

    A2 = r.a2

    @pl.loop(0, rows // BLK)
    def _(i):
        at = pl.multiple_of(i * BLK, BLK)
        v = normed2_of(CV[pl.ds(at + EDGE, BLK), :])
        A2[pl.ds(at, BLK), :] = gelu(v * gain2 + off2).astype(BF16)

    O = r.ob
    mixf = CM[3].reshape(hp, width)
    outputs = (r.x[...].astype(F32) + nn(A2[...], mixf)).astype(BF16)
    O[k] = outputs
    r.out[...] = outputs
    put(O.at[k], O.at[k], r.os, r.orr, (s, other))
    at(105)
    r.a2t[...] = A2[...].T
    take(O.at[0], r.orr)
    OT = r.ot
    OT[...] = O[...].reshape(2 * rows, width).T
    GO = r.go
    GO[...] = jnp.zeros(GO.shape, F32)
    WG, GL = r.wg, (r.gl0, r.gl1)
    LG = r.lg
    HB = r.hbs
    HB[...] = jnp.zeros(HB.shape, F32)
    Z = S // 2
    if fused:
        A1, R1, R2, R3 = r.acc1, r.r1, r.r2, r.r3
        two = A1.shape[3]
        own = two // 2

        def first(j, ax):
            if ax:
                put(WG.at[j, :, :, xo], R1.at[j], r.s1.at[j], r.g1r.at[j], (s, xnb))
            else:
                put(WG.at[j, :, 1 - y], R1.at[j], r.s1.at[j], r.g1r.at[j], (ynb, c))

        def second(j, ax):
            take(R1.at[j], r.g1r.at[j])
            got_h = x_h if ax else y_h

            def step(i, _):
                zz, b = i // 2, lax.rem(i, 2)
                a = (WG[j, zz, b, xi] if ax else WG[j, zz, y, b]).astype(F32)
                g = R1[j, zz, b].astype(F32)
                A1[j, zz, b, :, 0:HW] = (jnp.where(mine_h, a, 0.0) + jnp.where(got_h, g, 0.0)).astype(BF16)
                A1[j, zz, b, :, HW:CW] = (
                    jnp.where(mine_h, 0.0, a[:, :MW]) + jnp.where(got_h, 0.0, g[:, :MW])
                ).astype(BF16)
                return 0

            lax.fori_loop(0, S, step, 0)
            if ax:
                put(A1.at[j, :, 1 - y], R2.at[j], r.s2.at[j], r.g2r.at[j], (ynb, c))
            else:
                put(A1.at[j, :, xo], R2.at[j], r.s2.at[j], r.g2r.at[j], (s, xnb))

        def third(j, ax):
            take(R2.at[j], r.g2r.at[j])
            b = y if ax else xi
            for zz in range(Z):
                R2[j, zz] = (A1[j, zz, b].astype(F32) + R2[j, zz].astype(F32)).astype(BF16)
            R3[j, z] = R2[j, z]
            for p in range(1, Z):
                to = lax.rem(z + p, Z)
                put(R2.at[j, to], R3.at[j, z], r.s3.at[j], r.g3r.at[j], (to * 2 + y, c))

        def last(j):
            take(R3.at[j, pl.ds(0, Z - 1)], r.g3r.at[j])
            v = R3[j, 0].astype(F32)
            for p in range(1, Z):
                v = v + R3[j, p].astype(F32)
            r.fin[j] = v.reshape(2, own, CW)
            put(r.fin.at[j, 1 - k], r.fr.at[j], r.s4.at[j], r.g4r.at[j], (s, other))

    def chunk_arrives(j):
        take(W.at[j, 0], r.wl.at[j])
        take(W.at[j, 0], r.wp.at[j])
        take(W.at[j, pl.ds(0, 2), 0], r.wy.at[j])
        take(W.at[j, pl.ds(0, 2), 0], r.wz.at[j])
        take(W.at[j, pl.ds(0, 2), 0, :, pl.ds(0, HALFC)], r.wd.at[j])
        take(TG.at[j, 0], r.tp.at[j])

    def tracks_of(j):
        head = jnp.where(
            mine_h, W[j, :, :, :, 0:MW].reshape(width, MW), W[j, :, :, :, HW:CW].reshape(width, MW)
        )
        return jnp.concatenate([head, W[j, :, :, :, MW:HW].reshape(width, HW - MW)], axis=1)

    def chunk_grads(j):
        wv = tracks_of(j)
        for h in range(2):
            LG[h] = nn(O[h], wv)
        valid_n = jnp.where(mine_h, HUMAN - (k * HALF_H + j * HW), jnp.minimum(MOUSE - (k * HALF_M + j * MW), MW))
        valid = lax.broadcasted_iota(jnp.int32, (1, HW), 1) < valid_n
        brow = BR[pl.ds(k * NCHUNK + j, 1), :]
        bias = jnp.concatenate([jnp.where(mine_h, brow[:, :MW], brow[:, HW:]), brow[:, MW:HW]], axis=1)
        acc = jnp.zeros((8, HW), F32)
        for h in range(2):
            for i in range(rows // BLK):
                at = slice(i * BLK, (i + 1) * BLK)
                g = poisson_grad(LG[h, at, :] + bias, TG[j, h, at, :].astype(F32))
                g = jnp.where(valid, g, 0.0).astype(BF16)
                GL[j % 2][h, at, :] = g
                acc = acc + jnp.sum(g.astype(F32).reshape(BLK // 8, 8, HW), 0)
        bsum = jnp.sum(acc, 0, keepdims=True)
        HB[j : j + 1, 0:HW] = jnp.where(mine_h, bsum, 0.0)
        HB[j : j + 1, HW:CW] = jnp.where(mine_h, 0.0, bsum[:, :MW])

    def chunk_products(j):
        g = GL[j % 2][...].reshape(2 * rows, HW)
        GO[...] += nt(g, tracks_of(j)).reshape(GO.shape)
        WG[j] = nn(OT[...], g).astype(BF16).reshape(WG.shape[1:])

    at(0)
    for j in range(NCHUNK + 1):
        if j < NCHUNK:
            chunk_arrives(j)
            chunk_grads(j)
        if j > 0:
            chunk_products(j - 1)
        at(110 + j)

    put(GO.at[1 - k], r.gor, r.gos, r.gorr, (s, other))
    put(r.hbs, r.hbx, r.hbsem.at[0], r.hbrem.at[0], (s, xnb))
    at(1)

    if fused:
        CP, C1, C3, CF = ([getattr(r, f"{n}{i}") for i in range(3)] for n in ("cp", "c1", "c3", "cf"))

        def lanes(b):
            return pl.ds(pl.multiple_of(b * half_w, LANES), half_w)

        def weights_out(i, v):
            CP[i][...] = v.astype(BF16).reshape(CP[i].shape)
            put(CP[i].at[:, :, lanes(1 - y)], C1[i], r.ccs.at[4 * i], r.ccr.at[4 * i], (ynb, c))

        def weights_along_z(i):
            take(C1[i], r.ccr.at[4 * i])
            C1[i][...] = (C1[i][...].astype(F32) + CP[i][:, :, lanes(y)].astype(F32)).astype(BF16)
            C3[i][z] = C1[i][z]
            for p in range(1, Z):
                to = lax.rem(z + p, Z)
                put(C1[i].at[to], C3[i].at[z], r.ccs.at[4 * i + 1], r.ccr.at[4 * i + 1], (to * 2 + y, c))

        def weights_back_z(i):
            take(C3[i].at[pl.ds(0, Z - 1)], r.ccr.at[4 * i + 1])
            v = C3[i][0].astype(F32)
            for p in range(1, Z):
                v = v + C3[i][p].astype(F32)
            CF[i][z, :, lanes(y)] = v.astype(BF16)
            for p in range(1, Z):
                to = lax.rem(z + p, Z)
                mine = CF[i].at[z, :, lanes(y)]
                put(mine, mine, r.ccs.at[4 * i + 2], r.ccr.at[4 * i + 2], (to * 2 + y, c))

        def weights_back_y(i):
            take(CF[i].at[pl.ds(0, Z - 1), :, pl.ds(0, half_w)], r.ccr.at[4 * i + 2])
            mine = CF[i].at[:, :, lanes(y)]
            put(mine, mine, r.ccs.at[4 * i + 3], r.ccr.at[4 * i + 3], (ynb, c))

    G, GOR = r.gbe, r.gor
    take(GOR, r.gorr)

    @pl.loop(0, rows // BLK)
    def _(i):
        v = GO[k, block(i), :] + GOR[block(i), :]
        GOR[block(i), :] = v
        G[block(i, EDGE), :] = v.astype(BF16)

    put(G.at[pl.ds(EDGE, EDGE)], G.at[pl.ds(rows + EDGE, EDGE)], r.gs.at[0], r.gr.at[0], left_dev)
    put(G.at[pl.ds(rows, EDGE)], G.at[pl.ds(0, EDGE)], r.gs.at[1], r.gr.at[1], right_dev)
    GA, GP = r.ga, r.gp
    GA[EDGE : EDGE + rows, :] = nt(G[EDGE : EDGE + rows, :], mixf)

    def pull_two(at):
        v = normed2_of(CV[at, :])
        g = GA[at, :] * gelu_slope(v * gain2 + off2)
        GP[at, :] = g
        return g * v, g

    gs_, ss_ = lax.fori_loop(0, rows // BLK, row_sums(lambda i: pull_two(block(i, EDGE))), (zero_h, zero_h))
    spread(r.sa2, (gs_, ss_))
    sum_start(2)
    at(2)
    MP = r.mp
    mp = nn(r.a2t[...], G[EDGE : EDGE + rows, :]).astype(BF16).reshape(C, LANES, width)
    for p in range(C):
        MP[p % 2, p // 2] = mp[p, 0:cr, :]
    put(MP.at[1 - k], r.mr, r.mps.at[0], r.mpr.at[0], (s, other))
    at(3)
    sum_middle(2)
    HX = r.hbx
    take(HX, r.hbrem.at[0])
    HX[...] = HX[...] + HB[...]

    @pl.loop(1, S)
    def _(p):
        put(HX, r.hbf.at[s], r.hbsem.at[1], r.hbrem.at[1], (lax.rem(s + p, S), c))

    r.hbf[s] = HX[...]
    at(4)
    take(r.mr, r.mpr.at[0])
    MR = r.mr
    MR[...] = (MR[...].astype(F32) + MP[k].astype(F32)).astype(BF16)
    put(MR.at[xo], r.mx, r.mps.at[1], r.mpr.at[1], (s, xnb))
    at(5)
    take(r.xedge, r.gr.at[0])
    take(r.xedge, r.gr.at[1])
    for e in (0, rows + EDGE):
        GA[e : e + EDGE, :] = nt(G[e : e + EDGE, :], mixf)
        pull_two(slice(e, e + EDGE))
    at(6)
    total2, gsum2, ssum2 = sum_end(2, hp)
    r.tot[...] = total2
    r.g2[...] = r.tot[pl.ds(c, 1), 0:cr].reshape(cr)
    r.b2[...] = r.tot[pl.ds(C + c, 1), 0:cr].reshape(cr)
    coef2 = gain2 * scale2
    gmean2, smean2 = gsum2 * inv_bins, ssum2 * inv_bins
    GC, GB = r.gce, r.gcb

    def conv_grad(at):
        return (coef2 * (GP[at, :] - smean2 - normed2_of(CV[at, :]) * gmean2)).astype(BF16)

    hx = hp // 2

    @pl.loop(0, rows // BLK)
    def _(i):
        v = conv_grad(block(i, EDGE))
        GC[block(i, EDGE), :] = v.astype(F32)
        GB[0, block(i), :] = v[:, :hx]
        GB[1, block(i), :] = v[:, hx:]

    put(GB.at[xo], r.gcx, r.gbs, r.gbr, (s, xnb))
    take(r.mx, r.mpr.at[1])
    mix_sum = MR[xi].astype(F32) + r.mx[...].astype(F32)
    if fused:
        weights_out(0, mix_sum)
    else:
        r.mwg[...] = mix_sum
    GC[0:EDGE, :] = jnp.where(left_same, conv_grad(slice(0, EDGE)).astype(F32), 0.0)
    GC[rows + EDGE : ext, :] = jnp.where(right_same, conv_grad(slice(rows + EDGE, ext)).astype(F32), 0.0)
    at(7)


    G1 = r.ga1
    for t in range(TAPS):
        lo_t = EDGE + STEP - t * STEP
        part = nn(GC[lo_t : lo_t + rows, :].astype(BF16), CM[t].reshape(hp, width))
        G1[...] = part if t == 0 else G1[...] + part

    def pull_one(i):
        v = normed1_of(r.x[block(i), :].astype(F32))
        g = G1[block(i), :] * gelu_slope(v * gain1 + off1)
        G1[block(i), :] = g
        return g * v, g

    g1s, s1s = lax.fori_loop(0, rows // BLK, row_sums(pull_one), (zero_w, zero_w))
    spread(r.sa3, (g1s, s1s))
    sum_start(3)
    at(8)

    ZP, CG = r.zpad, r.cg
    pad = ZP.shape[0] - rows
    ZP[0 : pad // 2, :] = jnp.zeros((pad // 2, hx), F32)
    ZP[rows + pad // 2 :, :] = jnp.zeros((pad // 2, hx), F32)
    for part in range(2):
        if part == 1:
            take(r.actx, r.ar_)
            take(r.gcx, r.gbr)
        ZP[pad // 2 : pad // 2 + rows, :] = (GB[xi] if part == 0 else r.gcx[...]).astype(F32)
        rows_act = A[lo : lo + ext, :] if part == 0 else r.actx[...]
        for t in range(TAPS):
            lo_t = pad // 2 - EDGE + STEP - t * STEP
            v = nn(ZP[lo_t : lo_t + ext, :].T.astype(BF16), rows_act).reshape(2, LANES, width)
            CG[t] = v if part == 0 else CG[t] + v
    put(CG.at[:, 1 - k, pl.ds(0, cr)], r.cgr, r.cgs, r.cgrr, (s, other))
    at(9)
    if fused:
        weights_along_z(0)
    sum_middle(3)
    at(10)
    take(r.cgr, r.cgrr)
    conv_sum = [CG[t, k, 0:cr, :] + r.cgr[t] for t in range(TAPS)]
    if fused:
        weights_out(1, jnp.concatenate([conv_sum[0], conv_sum[1][0:64]], axis=0))
        weights_out(2, jnp.concatenate([conv_sum[1][64:], conv_sum[2]], axis=0))
        at(12)
    else:
        for t in range(TAPS):
            r.cwg[t] = conv_sum[t]
        r.wgo[...] = WG[...]

    take(r.hbf.at[pl.ds(0, S - 1)], r.hbrem.at[1])
    HB3 = r.hb3
    HB3[...] = lax.fori_loop(1, S, lambda p, a: a + r.hbf[p], r.hbf[0])
    put(HB3, r.hbp, r.hbsem.at[2], r.hbrem.at[2], (s, other))
    at(13)

    def input_gradient():
        total1, gsum1, ssum1 = sum_end(3, width)
        r.g1[...] = gsum1.reshape(width)
        r.b1[...] = ssum1.reshape(width)
        coef1 = gain1 * scale1
        gmean1, smean1 = gsum1 * inv_bins, ssum1 * inv_bins

        @pl.loop(0, rows // BLK)
        def _(i):
            v = normed1_of(r.x[block(i), :].astype(F32))
            r.ig[block(i), :] = GOR[block(i), :] + coef1 * (G1[block(i), :] - smean1 - v * gmean1)

    if fused:
        weights_along_z(1)
        weights_along_z(2)
        input_gradient()
        at(14)
        weights_back_z(0)
        weights_back_z(1)
        weights_back_z(2)
        at(15)
        weights_back_y(0)
        weights_back_y(1)
        weights_back_y(2)
        at(16)
        for i in range(3):
            take(CF[i].at[:, :, pl.ds(0, half_w)], r.ccr.at[4 * i + 3])
        r.mwg[...] = CF[0][...].reshape(cr, width).astype(F32)
        v = CF[1][...].reshape(cr + 64, width).astype(F32)
        r.cwg[0] = v[0:cr]
        r.cwg[1, 0:64, :] = v[cr:]
        v = CF[2][...].reshape(2 * cr - 64, width).astype(F32)
        r.cwg[1, 64:, :] = v[0 : cr - 64]
        r.cwg[2] = v[cr - 64 :]
        at(17)
    if not fused:
        input_gradient()
    take(r.hbp, r.hbrem.at[2])

    def in_order(dst, human, mouse):
        for m in range(M0 // HW):
            dst[:, m * HW : (m + 1) * HW] = human(m // NCHUNK, m % NCHUNK)
        edge = M0 // HW * HW
        v = human(edge // HALF_H, edge // HW % NCHUNK)
        if edge < M0:
            dst[:, edge:M0] = v[:, 0 : M0 - edge]
        before = v[:, M0 - edge : M0 - edge + LANES]
        lane = lax.broadcasted_iota(jnp.int32, (1, LANES), 1)
        for m in range(pl.cdiv(tracks - M0, LANES)):
            here = mouse(m // NCHUNK, m % NCHUNK) if m < 2 * NCHUNK else jnp.zeros_like(before)
            moved = pltpu.roll(here, OFF, 1)
            out = jnp.where(lane < OFF, before, moved)
            n = min(LANES, tracks - M0 - m * LANES)
            dst[:, M0 + m * LANES : M0 + m * LANES + n] = out[:, 0:n]
            before = moved

    HO = r.hbo
    HO[0] = jnp.where(k == 0, HB3[...], r.hbp[...])
    HO[1] = jnp.where(k == 0, r.hbp[...], HB3[...])
    in_order(r.hbrow, lambda h, j: HO[h, j : j + 1, 0:HW], lambda h, j: HO[h, j : j + 1, HW:CW])
    r.hb[...] = r.hbrow[...].reshape(tracks)
    if fused:
        for j in range(NCHUNK):
            take(r.fr.at[j], r.g4r.at[j])

        def piece(h, j, at, n):
            return jnp.where(k == h, r.fin[j, k, :, at : at + n], r.fr[j, :, at : at + n])

        in_order(r.hg, lambda h, j: piece(h, j, 0, HW), lambda h, j: piece(h, j, HW, MW))

    for i in range(4):
        take(r.ba[i].at[pl.ds(0, C - 1)], r.ars.at[2 * i])
        take(r.bb[i].at[pl.ds(0, S - 1)], r.ars.at[2 * i + 1])
    take(r.xl, r.hs.at[0])
    take(r.xr, r.hs.at[1])
    take(CM.at[0, 0, pl.ds(0, cr)], r.cms.at[0])
    take(CM.at[0, 0, pl.ds(0, cr), pl.ds(0, half_w)], r.cms.at[1])
    take(CS, r.cms.at[2])
    take(CM.at[0, 0, pl.ds(0, cr)], r.cms.at[3])
    take(CM.at[0, 0, pl.ds(0, cr)], r.cms.at[4])
    take(CM.at[0, 0, pl.ds(0, cr), pl.ds(0, half_w)], r.cms.at[5])
    take(CS, r.cms.at[6])
    take(r.gsb.at[pl.ds(0, C - 1)], r.gss)
    take(W.at[:, 0], r.wps)
    take(TG.at[:, 0], r.tps)
    take(W.at[:, pl.ds(0, 3), 0], r.wxs)
    take(W.at[:, pl.ds(0, 2), 0], r.wrs.at[0])
    take(W.at[:, pl.ds(0, 2), 0], r.wrs.at[1])
    take(W.at[:, 0, 0], r.wrs.at[2])
    take(r.actx, r.as_)
    take(O.at[0], r.os)
    take(GOR, r.gos)
    take(HX, r.hbsem.at[0])
    take(r.hbf.at[pl.ds(0, S - 1)], r.hbsem.at[1])
    take(HB3, r.hbsem.at[2])
    take(r.xedge, r.gs.at[0])
    take(r.xedge, r.gs.at[1])
    take(r.mr, r.mps.at[0])
    take(r.mx, r.mps.at[1])
    take(r.gcx, r.gbs)
    take(r.cgr, r.cgs)
    if fused:
        for i in range(3):
            take(C1[i], r.ccs.at[4 * i])
            take(C3[i].at[pl.ds(0, Z - 1)], r.ccs.at[4 * i + 1])
            take(CF[i].at[pl.ds(0, Z - 1), :, pl.ds(0, half_w)], r.ccs.at[4 * i + 2])
            take(CF[i].at[:, :, pl.ds(0, half_w)], r.ccs.at[4 * i + 3])
        for j in range(NCHUNK):
            take(R1.at[j], r.s1.at[j])
            take(R2.at[j], r.s2.at[j])
            take(R3.at[j, pl.ds(0, Z - 1)], r.s3.at[j])
            take(r.fr.at[j], r.s4.at[j])


def fused_step(seqs, chs, **ins):
    S, C = seqs, chs
    rows, width = ins["x"].shape
    n_dev = S * C
    hp = C * LANES
    cr = ins["mix"].shape[0]
    kr = ins["hw"].shape[1]
    tracks = ins["bias"].shape[0]
    ext = rows + 2 * EDGE
    Z = S // 2
    fused = width % (n_dev * 8) == 0 and Z == 4
    two = 2 * (width // n_dev)
    vm = pltpu.VMEM
    dma = pltpu.SemaphoreType.DMA
    any_ins = ("hw", "counts")
    outs = dict(
        out=((rows, width), BF16),
        ig=((rows, width), F32),
        g1=((width,), F32),
        b1=((width,), F32),
        cwg=((TAPS, cr, width), F32),
        g2=((cr,), F32),
        b2=((cr,), F32),
        mwg=((cr, width), F32),
        hb=((tracks,), F32),
    )
    if fused:
        outs["hg"] = ((two // 2, tracks), F32)
    else:
        outs["wgo"] = ((NCHUNK, Z, 2, 2, width // (4 * Z), HW), BF16)
    scratch = dict(
        xl=vm((HALO, width), BF16),
        xr=vm((HALO, width), BF16),
        xedge=vm((EDGE, width), BF16),
        gs2=vm((8, LANES), F32),
        gsb=vm((C, 8, LANES), F32),
        cm=vm((4, cr, width), BF16),
        cmf=vm((4, C, LANES, width), BF16),
        hwv=vm((4, kr, tracks), BF16),
        mwv=vm((4, kr, 2 * HALF_M), BF16),
        cbuf=vm((HUMAN, rows), jnp.int32),
        ctail=vm((HW - MW, rows), jnp.int32),
        hbpad=vm((1, HUMAN // LANES * LANES + (2 * NCHUNK + 1) * LANES), F32),
        bias_rows=vm((16, CW), F32),
        wbuf=vm((NCHUNK, 4, 4, kr, CW), BF16),
        tgb=vm((NCHUNK, 2, rows, HW), BF16),
        tgx=vm((NCHUNK, rows, HW), BF16),
        act=vm((rows + 2 * HALO, width), BF16),
        actx=vm((ext, width), BF16),
        prod=vm((TAPS, rows + 2 * HALO, hp), F32),
        cv=vm((ext, hp), F32),
        a2=vm((rows, hp), BF16),
        a2t=vm((hp, rows), BF16),
        ob=vm((2, rows, width), BF16),
        ot=vm((width, 2 * rows), BF16),
        lg=vm((2, rows, HW), F32),
        gl0=vm((2, rows, HW), BF16),
        gl1=vm((2, rows, HW), BF16),
        wg=vm((NCHUNK, Z, 2, 2, width // (4 * Z), HW), BF16),
        go=vm((2, rows, width), F32),
        gor=vm((rows, width), F32),
        hbs=vm((8, CW), F32),
        hbx=vm((8, CW), F32),
        hbf=vm((S, 8, CW), F32),
        hb3=vm((8, CW), F32),
        hbp=vm((8, CW), F32),
        hbo=vm((2, 8, CW), F32),
        hbrow=vm((1, tracks), F32),
        gbe=vm((ext, width), BF16),
        ga=vm((ext, hp), F32),
        gp=vm((ext, hp), F32),
        gce=vm((ext, hp), F32),
        gcb=vm((2, rows, hp // 2), BF16),
        gcx=vm((rows, hp // 2), BF16),
        ga1=vm((rows, width), F32),
        mp=vm((2, 2, cr, width), BF16),
        mr=vm((2, cr, width), BF16),
        mx=vm((cr, width), BF16),
        zpad=vm((rows + 64, hp // 2), F32),
        cg=vm((TAPS, 2, LANES, width), F32),
        cgr=vm((TAPS, cr, width), F32),
        tot=vm((8, LANES), F32),
    )
    for i, n in enumerate((16, 8, 8, 16)):
        scratch[f"sa{i}"] = vm((n, LANES), F32)
        scratch[f"sb{i}"] = vm((n, LANES), F32)
        scratch[f"ba{i}"] = vm((C, n, LANES), F32)
        scratch[f"bb{i}"] = vm((S, n, LANES), F32)
    sems = dict(
        ars=8, arr=8, hs=2, hr=2, cms=7, cmr=7, gss=0, gsr=0, ld=2, wl=7, wp=7, wx=7, wy=7, wz=7, wd=7, wps=0, wxs=0,
        wrs=3, tp=7, tps=0, as_=0, ar_=0, os=0, gos=0, gorr=0, hbsem=3, hbrem=3, gs=2, gr=2, mps=2, mpr=2, gbs=0,
        gbr=0, cgs=0, cgrr=0, orr=0,
    )
    if fused:
        scratch.update(
            acc1=vm((NCHUNK, Z, 2, two, CW), BF16),
            r1=vm((NCHUNK, Z, 2, two, HW), BF16),
            r2=vm((NCHUNK, Z, two, CW), BF16),
            r3=vm((NCHUNK, Z, two, CW), BF16),
            fin=vm((NCHUNK, 2, two // 2, CW), F32),
            fr=vm((NCHUNK, two // 2, CW), F32),
        )
        for i, n in enumerate((cr, cr + 64, 2 * cr - 64)):
            scratch[f"cp{i}"] = vm((Z, n // Z, width), BF16)
            scratch[f"c1{i}"] = vm((Z, n // Z, width // 2), BF16)
            scratch[f"c3{i}"] = vm((Z, n // Z, width // 2), BF16)
            scratch[f"cf{i}"] = vm((Z, n // Z, width), BF16)
        sems.update(s1=7, s2=7, s3=7, s4=7, g1r=7, g2r=7, g3r=7, g4r=7, ccs=12, ccr=12)
    for name, n in sems.items():
        scratch[name] = dma((n,)) if n else dma
    names = [*ins, *outs, *scratch]

    def space(name):
        if name == "species":
            return pl.BlockSpec(memory_space=pltpu.SMEM)
        return pl.BlockSpec(memory_space=pl.ANY if name in any_ins else pltpu.VMEM)

    got = pl.pallas_call(
        functools.partial(kernel_body, S, C, fused, names),
        out_shape=[jax.ShapeDtypeStruct(*v) for v in outs.values()],
        in_specs=[space(n) for n in ins],
        out_specs=[pl.BlockSpec(memory_space=pltpu.VMEM) for _ in outs],
        scratch_shapes=list(scratch.values()),
        compiler_params=pltpu.CompilerParams(
            collective_id=0, has_side_effects=True, vmem_limit_bytes=67_043_328
        ),
    )(*ins.values())
    return types.SimpleNamespace(**dict(zip(outs, got, strict=True))), fused


def handed_on(values):
    def body(*refs):
        n = len(values)
        sems = refs[2 * n]
        for i in range(n):
            pltpu.make_async_copy(refs[i], refs[n + i], sems.at[i]).start()
        for i in range(n):
            pltpu.make_async_copy(refs[i], refs[n + i], sems.at[i]).wait()

    return pl.pallas_call(
        body,
        out_shape=[jax.ShapeDtypeStruct(v.shape, v.dtype) for v in values],
        in_specs=[pl.BlockSpec(memory_space=pltpu.VMEM) for _ in values],
        out_specs=[pl.BlockSpec(memory_space=pl.ANY) for _ in values],
        scratch_shapes=[pltpu.SemaphoreType.DMA((len(values),))],
    )(*values)


def on_device(
    inputs, gain_one, shift_one, conv_weight, gain_two, shift_two, mix_weight, head_weight, head_bias, species, counts
):
    S, C = lax.axis_size("seq"), lax.axis_size("ch")
    s, c = lax.axis_index("seq"), lax.axis_index("ch")
    rows, width = inputs.shape
    depth, tracks = head_weight.shape
    o, fused = fused_step(
        S,
        C,
        x=inputs,
        gain1=gain_one,
        shift1=shift_one,
        cw=jnp.transpose(conv_weight, (0, 2, 1)),
        gain2=gain_two,
        shift2=shift_two,
        mix=mix_weight,
        hw=head_weight.reshape(4, depth // 4, tracks),
        bias=head_bias,
        species=species,
        counts=jnp.transpose(counts),
    )
    cwg, mwg = o.cwg, o.mwg
    if fused:
        head_weight_grad = o.hg
    else:
        cwg, mwg = lax.psum((cwg, mwg), "seq")
        part = o.wgo.reshape(NCHUNK, width, HW).astype(F32)
        part = jnp.transpose(part, (1, 0, 2))
        k = lax.rem(c, 2)
        human = jnp.zeros((width, 2, HALF_H), F32).at[:, k].set(part.reshape(width, HALF_H))
        mouse = jnp.zeros((width, 2, HALF_M), F32).at[:, k].set(part[:, :, :MW].reshape(width, HALF_M))
        first = (s * C + c // 2 * 2) * rows
        window = jnp.mod(first - SHIFT, rows * S * C) // WINDOW_BINS
        is_h = jnp.sum(jnp.where(jnp.arange(species.shape[0], dtype=jnp.int32) == window, species, 0)) == 0
        human = jnp.where(is_h, human.reshape(width, 2 * HALF_H)[:, :HUMAN], 0.0)
        mouse = jnp.where(is_h, 0.0, mouse.reshape(width, 2 * HALF_M)[:, :MOUSE])
        head_weight_grad = lax.psum_scatter(
            jnp.concatenate([human, mouse], axis=1), ("seq", "ch"), scatter_dimension=0, tiled=True
        )
    if fused:
        names = list(vars(o))
        o = types.SimpleNamespace(**dict(zip(names, handed_on(list(vars(o).values())), strict=True)))
        cwg, mwg, head_weight_grad = o.cwg, o.mwg, o.hg
    return (
        o.out,
        o.ig,
        o.g1,
        o.b1,
        jnp.transpose(cwg, (0, 2, 1)),
        o.g2,
        o.b2,
        mwg,
        head_weight_grad,
        o.hb,
    )


def solution(mesh):
    rows = P(("seq", "ch"), None)
    in_specs = (
        rows, P(), P(), P(None, None, "ch"), P("ch"), P("ch"), P("ch", None), P("ch", None), P(), P(), rows,
    )
    out_specs = (
        rows, rows, P(), P(), P(None, None, "ch"), P("ch"), P("ch"), P("ch", None), rows, P(),
    )
    return jax.shard_map(on_device, mesh=mesh, in_specs=in_specs, out_specs=out_specs, check_vma=False)
```

```python
import functools
import math
import types

import jax
import jax.numpy as jnp
from jax import lax
from jax.experimental import pallas as pl
from jax.experimental.pallas import tpu as pltpu
from jax.sharding import PartitionSpec as P

HUMAN = 5313
MOUSE = 1643
STEP = 11
TAPS = 3
WINDOW_BINS = 1024
SHIFT = 512
EPS = 1e-05

LANES = 128
NCHUNK = 7
HW = 384
MW = 128
CW = HW + MW
HALF_H = NCHUNK * HW
HALF_M = NCHUNK * MW
HALO = 32
EDGE = 16
MESH = pl.DeviceIdType.MESH
F32 = jnp.float32
BF16 = jnp.bfloat16
K0 = math.sqrt(2.0 / math.pi)
K1 = K0 * 0.044715


PLAN = {
    100: ((6, 4), (6, 0), (6, 3)),
    101: ((5, 4), (6, 1)),
    102: ((5, 0), (5, 3)),
    103: ((6, 2), (6, 5), (6, 6)),
    104: ((5, 1), (5, 2), (0, 0)),
    105: ((5, 5),),
    110: ((5, 6),),
    112: ((1, 1), (1, 0)),
    114: ((1, 2),),
    2: ((2, 1), (2, 2)),
    5: ((1, 5),),
    6: ((2, 0), (3, 1), (3, 2)),
    8: ((3, 0), (1, 4), (2, 5)),
    9: ((4, 1), (4, 2)),
    10: ((1, 3),),
    12: ((1, 6),),
    13: ((3, 5),),
    14: ((2, 4), (4, 0), (2, 3)),
    15: ((2, 6), (4, 5), (3, 3), (3, 4)),
    16: ((3, 6),),
    17: ((4, 3), (4, 4), (4, 6)),
}
X_FIRST = (2, 3, 6)


def nn(a, b):
    return lax.dot_general(a, b, (((1,), (0,)), ((), ())), preferred_element_type=F32)


def nt(a, b):
    return lax.dot_general(a, b, (((1,), (1,)), ((), ())), preferred_element_type=F32)


def gelu(v):
    return 0.5 * v * (1.0 + jnp.tanh(v * (K0 + K1 * (v * v))))


def gelu_slope(v):
    v2 = v * v
    th = jnp.tanh(v * (K0 + K1 * v2))
    return 0.5 * (1.0 + th) + 0.5 * v * (1.0 - th * th) * (K0 + 3.0 * K1 * v2)


def poisson_grad(logits, target):
    t = jnp.exp(-jnp.abs(logits))
    up = 1.0 + t
    series = t * (1.0 - t * (0.5 - t * (1.0 / 3.0 - t * 0.25)))
    rate = jnp.maximum(logits, 0.0) + jnp.where(t < 0.015625, series, jnp.log(up))
    return jnp.where(logits >= 0.0, 1.0, t) * (rate - target) / (up * rate)


def take(ref, sem):
    pltpu.make_async_copy(ref, ref, sem).wait()


def kernel_body(seqs, chs, fused, names, *refs):
    r = types.SimpleNamespace(**dict(zip(names, refs, strict=True)))
    r.sa, r.sb, r.ba, r.bb = ([getattr(r, f"{n}{i}") for i in range(4)] for n in ("sa", "sb", "ba", "bb"))
    S, C = seqs, chs
    s = lax.axis_index("seq")
    c = lax.axis_index("ch")
    xi = c // 2
    k = lax.rem(c, 2)
    other = c + 1 - 2 * k
    xnb = lax.rem(c + 2, C)
    xo = 1 - xi
    y = lax.rem(s, 2)
    z = s // 2
    ynb = s + 1 - 2 * y
    zb = lax.rem(z, 2)
    znb = s + 2 - 4 * zb
    dnb = znb + 1 - 2 * y
    q = lax.rem(s, 4)
    q_y = q + 1 - 2 * y
    q_z = q + 2 - 4 * zb
    q_d = q_z + 1 - 2 * y
    rows, width = r.x.shape
    n_dev = S * C
    total_bins = rows * n_dev
    inv_bins = 1.0 / total_bins
    me = s * C + c
    left = lax.rem(me + n_dev - 1, n_dev)
    right = lax.rem(me + 1, n_dev)
    left_dev = (left // C, lax.rem(left, C))
    right_dev = (right // C, lax.rem(right, C))
    row0 = me * rows
    window = lax.rem(row0 + total_bins - SHIFT, total_bins) // WINDOW_BINS
    left_same = lax.rem(row0 + total_bins - 1 + total_bins - SHIFT, total_bins) // WINDOW_BINS == window
    right_same = lax.rem(row0 + rows + total_bins - SHIFT, total_bins) // WINDOW_BINS == window

    def human_at_chip(seq, chip):
        first = (seq * C + chip * 2) * rows
        return r.species[lax.rem(first + total_bins - SHIFT, total_bins) // WINDOW_BINS] == 0

    mine_h = human_at_chip(s, xi)
    x_h = human_at_chip(s, xo)
    y_h = human_at_chip(ynb, xi)
    hp = C * LANES

    def put(src, dst, send, recv, dev):
        pltpu.make_async_remote_copy(
            src_ref=src, dst_ref=dst, send_sem=send, recv_sem=recv, device_id=dev, device_id_type=MESH
        ).start()

    barrier = pltpu.get_barrier_semaphore()

    def greet(dev):
        pl.semaphore_signal(barrier, inc=1, device_id=dev, device_id_type=MESH)

    for i in range(1, C):
        greet((s, lax.rem(c + i, C)))

    @pl.loop(1, S)
    def _(i):
        greet((lax.rem(s + i, S), c))

    greet(left_dev)
    greet(right_dev)

    W, TG = r.wbuf, r.tgb

    def human_at(half, j):
        return pl.ds(pl.multiple_of(half * HALF_H + j * HW, LANES), HW)

    def mouse_at(half, j):
        return pl.ds(pl.multiple_of(half * HALF_M + j * MW, LANES), MW)

    HV, MV, CB = r.hwv, r.mwv, r.cbuf
    load_hw = pltpu.make_async_copy(r.hw, HV, r.ld.at[0])
    load_hw.start()
    load_counts = pltpu.make_async_copy(r.counts, CB, r.ld.at[1])
    load_counts.start()
    CM, CS = r.cmf, r.cm
    cr = CS.shape[1]
    for t in range(TAPS):
        CS[t] = r.cw[t]
        CM[t, c, 0:cr, :] = r.cw[t]
    CS[TAPS] = r.mix[...]
    CM[TAPS, c, 0:cr, :] = r.mix[...]
    for t in range(4):
        for p in range(C):
            CM[t, p, cr:LANES, :] = jnp.zeros((LANES - cr, width), BF16)
    r.gs2[...] = jnp.zeros(r.gs2.shape, F32)
    r.gs2[0:1, 0:cr] = r.gain2[...].reshape(1, cr)
    r.gs2[1:2, 0:cr] = r.shift2[...].reshape(1, cr)
    M0 = HUMAN // LANES * LANES
    OFF = HUMAN - M0
    HP = r.hbpad
    tracks = HUMAN + MOUSE
    HP[:, 0:tracks] = r.bias[...].reshape(1, tracks)
    HP[:, tracks:] = jnp.zeros((1, HP.shape[1] - tracks), F32)
    BR = r.bias_rows
    for m in range(2 * NCHUNK):
        BR[m : m + 1, 0:HW] = HP[:, m * HW : (m + 1) * HW]
        v = HP[:, M0 + m * LANES : M0 + (m + 2) * LANES]
        BR[m : m + 1, HW:CW] = pltpu.roll(v, 2 * LANES - OFF, 1)[:, :MW]

    def spread(ref, vecs):
        n = vecs[0].shape[1] // LANES
        for i, v in enumerate(vecs):
            for t in range(n):
                ref[i * n + t : i * n + t + 1, :] = v[:, t * LANES : (t + 1) * LANES]
        if ref.shape[0] > n * len(vecs):
            ref[n * len(vecs) :, :] = jnp.zeros((ref.shape[0] - n * len(vecs), LANES), F32)

    def collect(v, n):
        m = n // LANES
        return [jnp.concatenate([v[i * m + t : i * m + t + 1, :] for t in range(m)], axis=1) for i in range(2)]

    def sum_start(i):
        src, bufs = r.sa[i], r.ba[i]
        for p in range(1, C):
            put(src, bufs.at[c], r.ars.at[2 * i], r.arr.at[2 * i], (s, lax.rem(c + p, C)))
        bufs[c] = src[...]

    def sum_middle(i):
        src, bufs, far = r.sb[i], r.ba[i], r.bb[i]
        take(bufs.at[pl.ds(0, C - 1)], r.arr.at[2 * i])
        v = bufs[0]
        for p in range(1, C):
            v = v + bufs[p]
        src[...] = v

        @pl.loop(1, S)
        def _(p):
            put(src, far.at[s], r.ars.at[2 * i + 1], r.arr.at[2 * i + 1], (lax.rem(s + p, S), c))

        far[s] = v

    def sum_end(i, n):
        far = r.bb[i]
        take(far.at[pl.ds(0, S - 1)], r.arr.at[2 * i + 1])
        if S <= 8:
            v = far[0]
            for p in range(1, S):
                v = v + far[p]
        else:
            v = lax.fori_loop(1, S, lambda p, a: a + far[p], far[0])
        return v, *collect(v, n)

    BLK = 32

    def block(i, shift=0):
        return pl.ds(pl.multiple_of(i * BLK + shift, 16), BLK)

    def row_sums(terms):
        def step(i, carry):
            return tuple(a + jnp.sum(t, 0, keepdims=True) for a, t in zip(carry, terms(i), strict=True))

        return step

    zero_w = jnp.zeros((1, width), F32)

    def x_terms(i):
        v = r.x[block(i), :].astype(F32)
        return v, v * v

    s1, q1 = lax.fori_loop(0, rows // BLK, row_sums(x_terms), (zero_w, zero_w))
    spread(r.sa0, (s1, q1))
    load_hw.wait()
    full = (tracks - M0) // LANES - 1
    for p in range(4):
        for m in range(2 * NCHUNK):
            if m < full:
                v = HV[p, :, M0 + m * LANES : M0 + (m + 2) * LANES].astype(F32)
                v = pltpu.roll(v, 2 * LANES - OFF, 1)[:, :MW]
            elif M0 + m * LANES < tracks:
                v = HV[p, :, M0 + m * LANES : min(tracks, M0 + (m + 2) * LANES)].astype(F32)
                v = jnp.concatenate([v, jnp.zeros((v.shape[0], 2 * LANES - v.shape[1]), F32)], axis=1)
                v = pltpu.roll(v, 2 * LANES - OFF, 1)[:, :MW]
            else:
                v = jnp.zeros((HV.shape[1], MW), F32)
            MV[p, :, m * MW : (m + 1) * MW] = v.astype(BF16)

    @pl.loop(0, NCHUNK)
    def _(j):
        pltpu.make_async_copy(HV.at[:, :, human_at(k, j)], W.at[j, c, :, :, pl.ds(0, HW)], r.wl.at[j]).start()
        pltpu.make_async_copy(MV.at[:, :, mouse_at(k, j)], W.at[j, c, :, :, pl.ds(HW, MW)], r.wl.at[j]).start()

    pl.semaphore_wait(barrier, C - 1 + S - 1 + 2)

    sum_start(0)
    put(r.x.at[pl.ds(rows - HALO, HALO)], r.xl, r.hs.at[0], r.hr.at[0], right_dev)
    put(r.x.at[pl.ds(0, HALO)], r.xr, r.hs.at[1], r.hr.at[1], left_dev)
    half_w = width // 2
    put(CS.at[q], CM.at[q, c, pl.ds(0, cr)], r.cms.at[0], r.cmr.at[0], (s, xnb))
    put(
        CS.at[q_d, :, pl.ds(0, half_w)],
        CM.at[q_d, c, pl.ds(0, cr), pl.ds(0, half_w)],
        r.cms.at[1],
        r.cmr.at[1],
        (s, xnb),
    )
    put(CS, CM.at[:, c, pl.ds(0, cr)], r.cms.at[2], r.cmr.at[2], (s, other))
    for p in range(1, C):
        put(r.gs2, r.gsb.at[c], r.gss, r.gsr, (s, lax.rem(c + p, C)))
    r.gsb[c] = r.gs2[...]

    @pl.loop(0, NCHUNK)
    def _(j):
        put(
            HV.at[:, :, human_at(1 - k, j)], W.at[j, c, :, :, pl.ds(0, HW)],
            r.wps, r.wp.at[j], (s, other),
        )
        put(
            MV.at[:, :, mouse_at(1 - k, j)], W.at[j, c, :, :, pl.ds(HW, MW)],
            r.wps, r.wp.at[j], (s, other),
        )
    HALFC = CW // 2

    def heads_along_x(j):
        for h in range(2):
            dev = (s, xo * 2 + h)
            hc = pl.multiple_of(h * HALF_H + j * HW, LANES)
            put(HV.at[q, :, human_at(h, j)], W.at[j, c, q, :, pl.ds(0, HW)], r.wxs, r.wx.at[j], dev)
            put(MV.at[q, :, mouse_at(h, j)], W.at[j, c, q, :, pl.ds(HW, MW)], r.wxs, r.wx.at[j], dev)
            put(
                HV.at[q_d, :, pl.ds(hc, HALFC)], W.at[j, c, q_d, :, pl.ds(0, HALFC)],
                r.wxs, r.wx.at[j], dev,
            )

    def relay_heads(j):
        take(W.at[j, pl.ds(0, 3), 0], r.wx.at[j])
        far = pl.ds(xo * 2, 2)
        put(W.at[j, far, q], W.at[j, far, q], r.wrs.at[0], r.wy.at[j], (ynb, c))
        put(W.at[j, far, q], W.at[j, far, q], r.wrs.at[1], r.wz.at[j], (znb, c))
        put(
            W.at[j, far, q, :, pl.ds(HALFC, HALFC)], W.at[j, far, q, :, pl.ds(HALFC, HALFC)],
            r.wrs.at[2], r.wd.at[j], (dnb, c),
        )

    def at(slot):
        for stage, j in PLAN.get(slot, ()):
            if stage == 0:
                put(A.at[pl.ds(HALO - EDGE, ext)], r.actx, r.as_, r.ar_, (s, xnb))
            elif stage == 5:
                relay_heads(j)
            elif stage == 6:
                heads_along_x(j)
            elif fused and stage == 4:
                last(j)
            elif fused:
                (first, second, third)[stage - 1](j, j in X_FIRST)

    ext = rows + 2 * EDGE
    at(100)

    def pass_weights():
        take(CM.at[0, 0, pl.ds(0, cr)], r.cmr.at[0])
        put(CM.at[q, xnb, pl.ds(0, cr)], CM.at[q, xnb, pl.ds(0, cr)], r.cms.at[3], r.cmr.at[3], (ynb, c))
        put(CM.at[q, xnb, pl.ds(0, cr)], CM.at[q, xnb, pl.ds(0, cr)], r.cms.at[4], r.cmr.at[4], (znb, c))
        second = pl.ds(half_w, half_w)
        put(
            CM.at[q, xnb, pl.ds(0, cr), second], CM.at[q, xnb, pl.ds(0, cr), second],
            r.cms.at[5], r.cmr.at[5], (dnb, c),
        )

    def targets(half, dst, j):
        at = pl.multiple_of(half * HALF_H + j * HW, 8)
        am = pl.multiple_of(half * HALF_M + j * MW, 8)
        v = CB[pl.ds(at, MW), :]
        dst[:, 0:MW] = jnp.where(mine_h, v, CB[pl.ds(am, MW), :]).astype(F32).T.astype(BF16)
        ends = (half == 1) & (j == NCHUNK - 1)

        @pl.when(ends)
        def _():
            dst[:, MW:HW] = CT[...].astype(F32).T.astype(BF16)

        @pl.when(jnp.logical_not(ends))
        def _():
            dst[:, MW:HW] = CB[pl.ds(at + MW, HW - MW), :].astype(F32).T.astype(BF16)

    load_counts.wait()
    CT = r.ctail
    whole = HUMAN - (2 * HALF_H - HW + MW)
    CT[0:whole, :] = CB[HUMAN - whole : HUMAN, :]
    CT[whole:, :] = jnp.zeros((CT.shape[0] - whole, CT.shape[1]), jnp.int32)
    sum_middle(0)
    pass_weights()

    @pl.loop(0, NCHUNK)
    def _(j):
        targets(k, TG.at[j, k], j)

    _, t1, u1 = sum_end(0, width)
    mean1 = t1 * inv_bins
    scale1 = lax.rsqrt(u1 * inv_bins - mean1 * mean1 + EPS)
    gain1 = r.gain1[...].reshape(1, width)
    off1 = r.shift1[...].reshape(1, width)

    A = r.act

    def normed1_of(v):
        return (v - mean1) * scale1

    def act_rows(v):
        return gelu(normed1_of(v.astype(F32)) * gain1 + off1)

    @pl.loop(0, rows // BLK)
    def _(i):
        at = pl.multiple_of(i * BLK, BLK)
        A[pl.ds(at + HALO, BLK), :] = act_rows(r.x[pl.ds(at, BLK), :]).astype(BF16)

    take(r.xl, r.hr.at[0])
    A[0:HALO, :] = jnp.where(left_same, act_rows(r.xl[...]), 0.0).astype(BF16)
    take(r.xr, r.hr.at[1])
    A[rows + HALO : rows + 2 * HALO, :] = jnp.where(right_same, act_rows(r.xr[...]), 0.0).astype(BF16)

    at(101)
    take(CM.at[0, 0, pl.ds(0, cr), pl.ds(0, half_w)], r.cmr.at[1])
    take(CM.at[0, 0, pl.ds(0, cr)], r.cmr.at[3])
    take(CM.at[0, 0, pl.ds(0, cr)], r.cmr.at[4])
    take(CM.at[0, 0, pl.ds(0, cr), pl.ds(0, half_w)], r.cmr.at[5])
    put(CM.at[:, xnb, pl.ds(0, cr)], CM.at[:, xnb, pl.ds(0, cr)], r.cms.at[6], r.cmr.at[6], (s, other))
    take(CM.at[:, 0, pl.ds(0, cr)], r.cmr.at[2])
    take(CM.at[:, 0, pl.ds(0, cr)], r.cmr.at[6])

    PR = r.prod
    for t in range(TAPS):
        PR[t] = nt(A[...], CM[t].reshape(hp, width))
    CV = r.cv
    lo = HALO - EDGE
    CV[...] = (
        PR[0, lo - STEP : lo - STEP + ext, :] + PR[1, lo : lo + ext, :] + PR[2, lo + STEP : lo + STEP + ext, :]
    )
    at(102)
    zero_h = jnp.zeros((1, hp), F32)

    def c_terms(i):
        v = CV[block(i, EDGE), :]
        return v, v * v

    s2, q2 = lax.fori_loop(0, rows // BLK, row_sums(c_terms), (zero_h, zero_h))
    spread(r.sa1, (s2, q2))
    sum_start(1)
    at(103)

    @pl.loop(0, NCHUNK)
    def _(j):
        targets(1 - k, r.tgx.at[j], j)
        put(r.tgx.at[j], TG.at[j, k], r.tps, r.tp.at[j], (s, other))

    sum_middle(1)
    at(104)
    _, t2, u2 = sum_end(1, hp)
    mean2 = t2 * inv_bins
    scale2 = lax.rsqrt(u2 * inv_bins - mean2 * mean2 + EPS)
    take(r.gsb.at[pl.ds(0, C - 1)], r.gsr)
    gain2 = jnp.concatenate([r.gsb[p, 0:1, :] for p in range(C)], axis=1)
    off2 = jnp.concatenate([r.gsb[p, 1:2, :] for p in range(C)], axis=1)

    def normed2_of(v):
        return (v - mean2) * scale2

    A2 = r.a2

    @pl.loop(0, rows // BLK)
    def _(i):
        at = pl.multiple_of(i * BLK, BLK)
        v = normed2_of(CV[pl.ds(at + EDGE, BLK), :])
        A2[pl.ds(at, BLK), :] = gelu(v * gain2 + off2).astype(BF16)

    O = r.ob
    mixf = CM[3].reshape(hp, width)
    outputs = (r.x[...].astype(F32) + nn(A2[...], mixf)).astype(BF16)
    O[k] = outputs
    r.out[...] = outputs
    put(O.at[k], O.at[k], r.os, r.orr, (s, other))
    at(105)
    r.a2t[...] = A2[...].T
    take(O.at[0], r.orr)
    OT = r.ot
    OT[...] = O[...].reshape(2 * rows, width).T
    GO = r.go
    GO[...] = jnp.zeros(GO.shape, F32)
    WG, GL = r.wg, (r.gl0, r.gl1)
    LG = r.lg
    HB = r.hbs
    HB[...] = jnp.zeros(HB.shape, F32)
    Z = S // 2
    if fused:
        A1, R1, R2, R3 = r.acc1, r.r1, r.r2, r.r3
        two = A1.shape[3]
        own = two // 2

        def first(j, ax):
            if ax:
                put(WG.at[j, :, :, xo], R1.at[j], r.s1.at[j], r.g1r.at[j], (s, xnb))
            else:
                put(WG.at[j, :, 1 - y], R1.at[j], r.s1.at[j], r.g1r.at[j], (ynb, c))

        def second(j, ax):
            take(R1.at[j], r.g1r.at[j])
            got_h = x_h if ax else y_h

            def step(i, _):
                zz, b = i // 2, lax.rem(i, 2)
                a = (WG[j, zz, b, xi] if ax else WG[j, zz, y, b]).astype(F32)
                g = R1[j, zz, b].astype(F32)
                A1[j, zz, b, :, 0:HW] = (jnp.where(mine_h, a, 0.0) + jnp.where(got_h, g, 0.0)).astype(BF16)
                A1[j, zz, b, :, HW:CW] = (
                    jnp.where(mine_h, 0.0, a[:, :MW]) + jnp.where(got_h, 0.0, g[:, :MW])
                ).astype(BF16)
                return 0

            lax.fori_loop(0, S, step, 0)
            if ax:
                put(A1.at[j, :, 1 - y], R2.at[j], r.s2.at[j], r.g2r.at[j], (ynb, c))
            else:
                put(A1.at[j, :, xo], R2.at[j], r.s2.at[j], r.g2r.at[j], (s, xnb))

        def third(j, ax):
            take(R2.at[j], r.g2r.at[j])
            b = y if ax else xi
            for zz in range(Z):
                R2[j, zz] = (A1[j, zz, b].astype(F32) + R2[j, zz].astype(F32)).astype(BF16)
            R3[j, z] = R2[j, z]
            for p in range(1, Z):
                to = lax.rem(z + p, Z)
                put(R2.at[j, to], R3.at[j, z], r.s3.at[j], r.g3r.at[j], (to * 2 + y, c))

        def last(j):
            take(R3.at[j, pl.ds(0, Z - 1)], r.g3r.at[j])
            v = R3[j, 0].astype(F32)
            for p in range(1, Z):
                v = v + R3[j, p].astype(F32)
            r.fin[j] = v.reshape(2, own, CW)
            put(r.fin.at[j, 1 - k], r.fr.at[j], r.s4.at[j], r.g4r.at[j], (s, other))

    def chunk_arrives(j):
        take(W.at[j, 0], r.wl.at[j])
        take(W.at[j, 0], r.wp.at[j])
        take(W.at[j, pl.ds(0, 2), 0], r.wy.at[j])
        take(W.at[j, pl.ds(0, 2), 0], r.wz.at[j])
        take(W.at[j, pl.ds(0, 2), 0, :, pl.ds(0, HALFC)], r.wd.at[j])
        take(TG.at[j, 0], r.tp.at[j])

    def tracks_of(j):
        head = jnp.where(
            mine_h, W[j, :, :, :, 0:MW].reshape(width, MW), W[j, :, :, :, HW:CW].reshape(width, MW)
        )
        return jnp.concatenate([head, W[j, :, :, :, MW:HW].reshape(width, HW - MW)], axis=1)

    def chunk_grads(j):
        wv = tracks_of(j)
        for h in range(2):
            LG[h] = nn(O[h], wv)
        valid_n = jnp.where(mine_h, HUMAN - (k * HALF_H + j * HW), jnp.minimum(MOUSE - (k * HALF_M + j * MW), MW))
        valid = lax.broadcasted_iota(jnp.int32, (1, HW), 1) < valid_n
        brow = BR[pl.ds(k * NCHUNK + j, 1), :]
        bias = jnp.concatenate([jnp.where(mine_h, brow[:, :MW], brow[:, HW:]), brow[:, MW:HW]], axis=1)
        acc = jnp.zeros((8, HW), F32)
        for h in range(2):
            for i in range(rows // BLK):
                at = slice(i * BLK, (i + 1) * BLK)
                g = poisson_grad(LG[h, at, :] + bias, TG[j, h, at, :].astype(F32))
                g = jnp.where(valid, g, 0.0).astype(BF16)
                GL[j % 2][h, at, :] = g
                acc = acc + jnp.sum(g.astype(F32).reshape(BLK // 8, 8, HW), 0)
        bsum = jnp.sum(acc, 0, keepdims=True)
        HB[j : j + 1, 0:HW] = jnp.where(mine_h, bsum, 0.0)
        HB[j : j + 1, HW:CW] = jnp.where(mine_h, 0.0, bsum[:, :MW])

    def chunk_products(j):
        g = GL[j % 2][...].reshape(2 * rows, HW)
        GO[...] += nt(g, tracks_of(j)).reshape(GO.shape)
        WG[j] = nn(OT[...], g).astype(BF16).reshape(WG.shape[1:])

    at(0)
    for j in range(NCHUNK + 1):
        if j < NCHUNK:
            chunk_arrives(j)
            chunk_grads(j)
        if j > 0:
            chunk_products(j - 1)
        at(110 + j)

    put(GO.at[1 - k], r.gor, r.gos, r.gorr, (s, other))
    put(r.hbs, r.hbx, r.hbsem.at[0], r.hbrem.at[0], (s, xnb))
    at(1)

    if fused:
        CP, C1, C3, CF = ([getattr(r, f"{n}{i}") for i in range(3)] for n in ("cp", "c1", "c3", "cf"))

        def lanes(b):
            return pl.ds(pl.multiple_of(b * half_w, LANES), half_w)

        def weights_out(i, v):
            CP[i][...] = v.astype(BF16).reshape(CP[i].shape)
            put(CP[i].at[:, :, lanes(1 - y)], C1[i], r.ccs.at[4 * i], r.ccr.at[4 * i], (ynb, c))

        def weights_along_z(i):
            take(C1[i], r.ccr.at[4 * i])
            C1[i][...] = (C1[i][...].astype(F32) + CP[i][:, :, lanes(y)].astype(F32)).astype(BF16)
            C3[i][z] = C1[i][z]
            for p in range(1, Z):
                to = lax.rem(z + p, Z)
                put(C1[i].at[to], C3[i].at[z], r.ccs.at[4 * i + 1], r.ccr.at[4 * i + 1], (to * 2 + y, c))

        def weights_back_z(i):
            take(C3[i].at[pl.ds(0, Z - 1)], r.ccr.at[4 * i + 1])
            v = C3[i][0].astype(F32)
            for p in range(1, Z):
                v = v + C3[i][p].astype(F32)
            CF[i][z, :, lanes(y)] = v.astype(BF16)
            for p in range(1, Z):
                to = lax.rem(z + p, Z)
                mine = CF[i].at[z, :, lanes(y)]
                put(mine, mine, r.ccs.at[4 * i + 2], r.ccr.at[4 * i + 2], (to * 2 + y, c))

        def weights_back_y(i):
            take(CF[i].at[pl.ds(0, Z - 1), :, pl.ds(0, half_w)], r.ccr.at[4 * i + 2])
            mine = CF[i].at[:, :, lanes(y)]
            put(mine, mine, r.ccs.at[4 * i + 3], r.ccr.at[4 * i + 3], (ynb, c))

    G, GOR = r.gbe, r.gor
    take(GOR, r.gorr)

    @pl.loop(0, rows // BLK)
    def _(i):
        v = GO[k, block(i), :] + GOR[block(i), :]
        GOR[block(i), :] = v
        G[block(i, EDGE), :] = v.astype(BF16)

    put(G.at[pl.ds(EDGE, EDGE)], G.at[pl.ds(rows + EDGE, EDGE)], r.gs.at[0], r.gr.at[0], left_dev)
    put(G.at[pl.ds(rows, EDGE)], G.at[pl.ds(0, EDGE)], r.gs.at[1], r.gr.at[1], right_dev)
    GA, GP = r.ga, r.gp
    GA[EDGE : EDGE + rows, :] = nt(G[EDGE : EDGE + rows, :], mixf)

    def pull_two(at):
        v = normed2_of(CV[at, :])
        g = GA[at, :] * gelu_slope(v * gain2 + off2)
        GP[at, :] = g
        return g * v, g

    gs_, ss_ = lax.fori_loop(0, rows // BLK, row_sums(lambda i: pull_two(block(i, EDGE))), (zero_h, zero_h))
    spread(r.sa2, (gs_, ss_))
    sum_start(2)
    at(2)
    MP = r.mp
    mp = nn(r.a2t[...], G[EDGE : EDGE + rows, :]).astype(BF16).reshape(C, LANES, width)
    for p in range(C):
        MP[p % 2, p // 2] = mp[p, 0:cr, :]
    put(MP.at[1 - k], r.mr, r.mps.at[0], r.mpr.at[0], (s, other))
    at(3)
    sum_middle(2)
    HX = r.hbx
    take(HX, r.hbrem.at[0])
    HX[...] = HX[...] + HB[...]

    @pl.loop(1, S)
    def _(p):
        put(HX, r.hbf.at[s], r.hbsem.at[1], r.hbrem.at[1], (lax.rem(s + p, S), c))

    r.hbf[s] = HX[...]
    at(4)
    take(r.mr, r.mpr.at[0])
    MR = r.mr
    MR[...] = (MR[...].astype(F32) + MP[k].astype(F32)).astype(BF16)
    put(MR.at[xo], r.mx, r.mps.at[1], r.mpr.at[1], (s, xnb))
    at(5)
    take(r.xedge, r.gr.at[0])
    take(r.xedge, r.gr.at[1])
    for e in (0, rows + EDGE):
        GA[e : e + EDGE, :] = nt(G[e : e + EDGE, :], mixf)
        pull_two(slice(e, e + EDGE))
    at(6)
    total2, gsum2, ssum2 = sum_end(2, hp)
    r.tot[...] = total2
    r.g2[...] = r.tot[pl.ds(c, 1), 0:cr].reshape(cr)
    r.b2[...] = r.tot[pl.ds(C + c, 1), 0:cr].reshape(cr)
    coef2 = gain2 * scale2
    gmean2, smean2 = gsum2 * inv_bins, ssum2 * inv_bins
    GC, GB = r.gce, r.gcb

    def conv_grad(at):
        return (coef2 * (GP[at, :] - smean2 - normed2_of(CV[at, :]) * gmean2)).astype(BF16)

    hx = hp // 2

    @pl.loop(0, rows // BLK)
    def _(i):
        v = conv_grad(block(i, EDGE))
        GC[block(i, EDGE), :] = v.astype(F32)
        GB[0, block(i), :] = v[:, :hx]
        GB[1, block(i), :] = v[:, hx:]

    put(GB.at[xo], r.gcx, r.gbs, r.gbr, (s, xnb))
    take(r.mx, r.mpr.at[1])
    mix_sum = MR[xi].astype(F32) + r.mx[...].astype(F32)
    if fused:
        weights_out(0, mix_sum)
    else:
        r.mwg[...] = mix_sum
    GC[0:EDGE, :] = jnp.where(left_same, conv_grad(slice(0, EDGE)).astype(F32), 0.0)
    GC[rows + EDGE : ext, :] = jnp.where(right_same, conv_grad(slice(rows + EDGE, ext)).astype(F32), 0.0)
    at(7)


    G1 = r.ga1
    for t in range(TAPS):
        lo_t = EDGE + STEP - t * STEP
        part = nn(GC[lo_t : lo_t + rows, :].astype(BF16), CM[t].reshape(hp, width))
        G1[...] = part if t == 0 else G1[...] + part

    def pull_one(i):
        v = normed1_of(r.x[block(i), :].astype(F32))
        g = G1[block(i), :] * gelu_slope(v * gain1 + off1)
        G1[block(i), :] = g
        return g * v, g

    g1s, s1s = lax.fori_loop(0, rows // BLK, row_sums(pull_one), (zero_w, zero_w))
    spread(r.sa3, (g1s, s1s))
    sum_start(3)
    at(8)

    ZP, CG = r.zpad, r.cg
    pad = ZP.shape[0] - rows
    ZP[0 : pad // 2, :] = jnp.zeros((pad // 2, hx), F32)
    ZP[rows + pad // 2 :, :] = jnp.zeros((pad // 2, hx), F32)
    for part in range(2):
        if part == 1:
            take(r.actx, r.ar_)
            take(r.gcx, r.gbr)
        ZP[pad // 2 : pad // 2 + rows, :] = (GB[xi] if part == 0 else r.gcx[...]).astype(F32)
        rows_act = A[lo : lo + ext, :] if part == 0 else r.actx[...]
        for t in range(TAPS):
            lo_t = pad // 2 - EDGE + STEP - t * STEP
            v = nn(ZP[lo_t : lo_t + ext, :].T.astype(BF16), rows_act).reshape(2, LANES, width)
            CG[t] = v if part == 0 else CG[t] + v
    put(CG.at[:, 1 - k, pl.ds(0, cr)], r.cgr, r.cgs, r.cgrr, (s, other))
    at(9)
    if fused:
        weights_along_z(0)
    sum_middle(3)
    at(10)
    take(r.cgr, r.cgrr)
    conv_sum = [CG[t, k, 0:cr, :] + r.cgr[t] for t in range(TAPS)]
    if fused:
        weights_out(1, jnp.concatenate([conv_sum[0], conv_sum[1][0:64]], axis=0))
        weights_out(2, jnp.concatenate([conv_sum[1][64:], conv_sum[2]], axis=0))
        at(12)
    else:
        for t in range(TAPS):
            r.cwg[t] = conv_sum[t]
        r.wgo[...] = WG[...]

    take(r.hbf.at[pl.ds(0, S - 1)], r.hbrem.at[1])
    HB3 = r.hb3
    HB3[...] = lax.fori_loop(1, S, lambda p, a: a + r.hbf[p], r.hbf[0])
    put(HB3, r.hbp, r.hbsem.at[2], r.hbrem.at[2], (s, other))
    at(13)

    def input_gradient():
        total1, gsum1, ssum1 = sum_end(3, width)
        r.g1[...] = gsum1.reshape(width)
        r.b1[...] = ssum1.reshape(width)
        coef1 = gain1 * scale1
        gmean1, smean1 = gsum1 * inv_bins, ssum1 * inv_bins

        @pl.loop(0, rows // BLK)
        def _(i):
            v = normed1_of(r.x[block(i), :].astype(F32))
            r.ig[block(i), :] = GOR[block(i), :] + coef1 * (G1[block(i), :] - smean1 - v * gmean1)

    if fused:
        weights_along_z(1)
        weights_along_z(2)
        input_gradient()
        at(14)
        weights_back_z(0)
        weights_back_z(1)
        weights_back_z(2)
        at(15)
        weights_back_y(0)
        weights_back_y(1)
        weights_back_y(2)
        at(16)
        for i in range(3):
            take(CF[i].at[:, :, pl.ds(0, half_w)], r.ccr.at[4 * i + 3])
        r.mwg[...] = CF[0][...].reshape(cr, width).astype(F32)
        v = CF[1][...].reshape(cr + 64, width).astype(F32)
        r.cwg[0] = v[0:cr]
        r.cwg[1, 0:64, :] = v[cr:]
        v = CF[2][...].reshape(2 * cr - 64, width).astype(F32)
        r.cwg[1, 64:, :] = v[0 : cr - 64]
        r.cwg[2] = v[cr - 64 :]
        at(17)
    if not fused:
        input_gradient()
    take(r.hbp, r.hbrem.at[2])

    def in_order(dst, human, mouse):
        for m in range(M0 // HW):
            dst[:, m * HW : (m + 1) * HW] = human(m // NCHUNK, m % NCHUNK)
        edge = M0 // HW * HW
        v = human(edge // HALF_H, edge // HW % NCHUNK)
        if edge < M0:
            dst[:, edge:M0] = v[:, 0 : M0 - edge]
        before = v[:, M0 - edge : M0 - edge + LANES]
        lane = lax.broadcasted_iota(jnp.int32, (1, LANES), 1)
        for m in range(pl.cdiv(tracks - M0, LANES)):
            here = mouse(m // NCHUNK, m % NCHUNK) if m < 2 * NCHUNK else jnp.zeros_like(before)
            moved = pltpu.roll(here, OFF, 1)
            out = jnp.where(lane < OFF, before, moved)
            n = min(LANES, tracks - M0 - m * LANES)
            dst[:, M0 + m * LANES : M0 + m * LANES + n] = out[:, 0:n]
            before = moved

    HO = r.hbo
    HO[0] = jnp.where(k == 0, HB3[...], r.hbp[...])
    HO[1] = jnp.where(k == 0, r.hbp[...], HB3[...])
    in_order(r.hbrow, lambda h, j: HO[h, j : j + 1, 0:HW], lambda h, j: HO[h, j : j + 1, HW:CW])
    r.hb[...] = r.hbrow[...].reshape(tracks)
    if fused:
        for j in range(NCHUNK):
            take(r.fr.at[j], r.g4r.at[j])

        def piece(h, j, at, n):
            return jnp.where(k == h, r.fin[j, k, :, at : at + n], r.fr[j, :, at : at + n])

        in_order(r.hg, lambda h, j: piece(h, j, 0, HW), lambda h, j: piece(h, j, HW, MW))

    for i in range(4):
        take(r.ba[i].at[pl.ds(0, C - 1)], r.ars.at[2 * i])
        take(r.bb[i].at[pl.ds(0, S - 1)], r.ars.at[2 * i + 1])
    take(r.xl, r.hs.at[0])
    take(r.xr, r.hs.at[1])
    take(CM.at[0, 0, pl.ds(0, cr)], r.cms.at[0])
    take(CM.at[0, 0, pl.ds(0, cr), pl.ds(0, half_w)], r.cms.at[1])
    take(CS, r.cms.at[2])
    take(CM.at[0, 0, pl.ds(0, cr)], r.cms.at[3])
    take(CM.at[0, 0, pl.ds(0, cr)], r.cms.at[4])
    take(CM.at[0, 0, pl.ds(0, cr), pl.ds(0, half_w)], r.cms.at[5])
    take(CS, r.cms.at[6])
    take(r.gsb.at[pl.ds(0, C - 1)], r.gss)
    take(W.at[:, 0], r.wps)
    take(TG.at[:, 0], r.tps)
    take(W.at[:, pl.ds(0, 3), 0], r.wxs)
    take(W.at[:, pl.ds(0, 2), 0], r.wrs.at[0])
    take(W.at[:, pl.ds(0, 2), 0], r.wrs.at[1])
    take(W.at[:, 0, 0], r.wrs.at[2])
    take(r.actx, r.as_)
    take(O.at[0], r.os)
    take(GOR, r.gos)
    take(HX, r.hbsem.at[0])
    take(r.hbf.at[pl.ds(0, S - 1)], r.hbsem.at[1])
    take(HB3, r.hbsem.at[2])
    take(r.xedge, r.gs.at[0])
    take(r.xedge, r.gs.at[1])
    take(r.mr, r.mps.at[0])
    take(r.mx, r.mps.at[1])
    take(r.gcx, r.gbs)
    take(r.cgr, r.cgs)
    if fused:
        for i in range(3):
            take(C1[i], r.ccs.at[4 * i])
            take(C3[i].at[pl.ds(0, Z - 1)], r.ccs.at[4 * i + 1])
            take(CF[i].at[pl.ds(0, Z - 1), :, pl.ds(0, half_w)], r.ccs.at[4 * i + 2])
            take(CF[i].at[:, :, pl.ds(0, half_w)], r.ccs.at[4 * i + 3])
        for j in range(NCHUNK):
            take(R1.at[j], r.s1.at[j])
            take(R2.at[j], r.s2.at[j])
            take(R3.at[j, pl.ds(0, Z - 1)], r.s3.at[j])
            take(r.fr.at[j], r.s4.at[j])


def fused_step(seqs, chs, **ins):
    S, C = seqs, chs
    rows, width = ins["x"].shape
    n_dev = S * C
    hp = C * LANES
    cr = ins["mix"].shape[0]
    kr = ins["hw"].shape[1]
    tracks = ins["bias"].shape[0]
    ext = rows + 2 * EDGE
    Z = S // 2
    fused = width % (n_dev * 8) == 0 and Z == 4
    two = 2 * (width // n_dev)
    vm = pltpu.VMEM
    dma = pltpu.SemaphoreType.DMA
    any_ins = ("hw", "counts")
    outs = dict(
        out=((rows, width), BF16),
        ig=((rows, width), F32),
        g1=((width,), F32),
        b1=((width,), F32),
        cwg=((TAPS, cr, width), F32),
        g2=((cr,), F32),
        b2=((cr,), F32),
        mwg=((cr, width), F32),
        hb=((tracks,), F32),
    )
    if fused:
        outs["hg"] = ((two // 2, tracks), F32)
    else:
        outs["wgo"] = ((NCHUNK, Z, 2, 2, width // (4 * Z), HW), BF16)
    scratch = dict(
        xl=vm((HALO, width), BF16),
        xr=vm((HALO, width), BF16),
        xedge=vm((EDGE, width), BF16),
        gs2=vm((8, LANES), F32),
        gsb=vm((C, 8, LANES), F32),
        cm=vm((4, cr, width), BF16),
        cmf=vm((4, C, LANES, width), BF16),
        hwv=vm((4, kr, tracks), BF16),
        mwv=vm((4, kr, 2 * HALF_M), BF16),
        cbuf=vm((HUMAN, rows), jnp.int32),
        ctail=vm((HW - MW, rows), jnp.int32),
        hbpad=vm((1, HUMAN // LANES * LANES + (2 * NCHUNK + 1) * LANES), F32),
        bias_rows=vm((16, CW), F32),
        wbuf=vm((NCHUNK, 4, 4, kr, CW), BF16),
        tgb=vm((NCHUNK, 2, rows, HW), BF16),
        tgx=vm((NCHUNK, rows, HW), BF16),
        act=vm((rows + 2 * HALO, width), BF16),
        actx=vm((ext, width), BF16),
        prod=vm((TAPS, rows + 2 * HALO, hp), F32),
        cv=vm((ext, hp), F32),
        a2=vm((rows, hp), BF16),
        a2t=vm((hp, rows), BF16),
        ob=vm((2, rows, width), BF16),
        ot=vm((width, 2 * rows), BF16),
        lg=vm((2, rows, HW), F32),
        gl0=vm((2, rows, HW), BF16),
        gl1=vm((2, rows, HW), BF16),
        wg=vm((NCHUNK, Z, 2, 2, width // (4 * Z), HW), BF16),
        go=vm((2, rows, width), F32),
        gor=vm((rows, width), F32),
        hbs=vm((8, CW), F32),
        hbx=vm((8, CW), F32),
        hbf=vm((S, 8, CW), F32),
        hb3=vm((8, CW), F32),
        hbp=vm((8, CW), F32),
        hbo=vm((2, 8, CW), F32),
        hbrow=vm((1, tracks), F32),
        gbe=vm((ext, width), BF16),
        ga=vm((ext, hp), F32),
        gp=vm((ext, hp), F32),
        gce=vm((ext, hp), F32),
        gcb=vm((2, rows, hp // 2), BF16),
        gcx=vm((rows, hp // 2), BF16),
        ga1=vm((rows, width), F32),
        mp=vm((2, 2, cr, width), BF16),
        mr=vm((2, cr, width), BF16),
        mx=vm((cr, width), BF16),
        zpad=vm((rows + 64, hp // 2), F32),
        cg=vm((TAPS, 2, LANES, width), F32),
        cgr=vm((TAPS, cr, width), F32),
        tot=vm((8, LANES), F32),
    )
    for i, n in enumerate((16, 8, 8, 16)):
        scratch[f"sa{i}"] = vm((n, LANES), F32)
        scratch[f"sb{i}"] = vm((n, LANES), F32)
        scratch[f"ba{i}"] = vm((C, n, LANES), F32)
        scratch[f"bb{i}"] = vm((S, n, LANES), F32)
    sems = dict(
        ars=8, arr=8, hs=2, hr=2, cms=7, cmr=7, gss=0, gsr=0, ld=2, wl=7, wp=7, wx=7, wy=7, wz=7, wd=7, wps=0, wxs=0,
        wrs=3, tp=7, tps=0, as_=0, ar_=0, os=0, gos=0, gorr=0, hbsem=3, hbrem=3, gs=2, gr=2, mps=2, mpr=2, gbs=0,
        gbr=0, cgs=0, cgrr=0, orr=0,
    )
    if fused:
        scratch.update(
            acc1=vm((NCHUNK, Z, 2, two, CW), BF16),
            r1=vm((NCHUNK, Z, 2, two, HW), BF16),
            r2=vm((NCHUNK, Z, two, CW), BF16),
            r3=vm((NCHUNK, Z, two, CW), BF16),
            fin=vm((NCHUNK, 2, two // 2, CW), F32),
            fr=vm((NCHUNK, two // 2, CW), F32),
        )
        for i, n in enumerate((cr, cr + 64, 2 * cr - 64)):
            scratch[f"cp{i}"] = vm((Z, n // Z, width), BF16)
            scratch[f"c1{i}"] = vm((Z, n // Z, width // 2), BF16)
            scratch[f"c3{i}"] = vm((Z, n // Z, width // 2), BF16)
            scratch[f"cf{i}"] = vm((Z, n // Z, width), BF16)
        sems.update(s1=7, s2=7, s3=7, s4=7, g1r=7, g2r=7, g3r=7, g4r=7, ccs=12, ccr=12)
    for name, n in sems.items():
        scratch[name] = dma((n,)) if n else dma
    names = [*ins, *outs, *scratch]

    def space(name):
        if name == "species":
            return pl.BlockSpec(memory_space=pltpu.SMEM)
        return pl.BlockSpec(memory_space=pl.ANY if name in any_ins else pltpu.VMEM)

    got = pl.pallas_call(
        functools.partial(kernel_body, S, C, fused, names),
        out_shape=[jax.ShapeDtypeStruct(*v) for v in outs.values()],
        in_specs=[space(n) for n in ins],
        out_specs=[pl.BlockSpec(memory_space=pltpu.VMEM) for _ in outs],
        scratch_shapes=list(scratch.values()),
        compiler_params=pltpu.CompilerParams(
            collective_id=0, has_side_effects=True, vmem_limit_bytes=67_043_328
        ),
    )(*ins.values())
    return types.SimpleNamespace(**dict(zip(outs, got, strict=True))), fused


def handed_on(values):
    n = len(values)

    def body(*refs):
        ins, outs, held = refs[:n], refs[n : 2 * n], refs[2 * n : 3 * n]
        come = [pltpu.make_async_copy(ins[i], held[i], refs[3 * n].at[i]) for i in range(n)]
        go = [pltpu.make_async_copy(held[i], outs[i], refs[3 * n + 1].at[i]) for i in range(n)]
        for copy in come:
            copy.start()
        for i in range(n):
            come[i].wait()
            go[i].start()
        for copy in go:
            copy.wait()

    return pl.pallas_call(
        body,
        out_shape=[jax.ShapeDtypeStruct(v.shape, v.dtype) for v in values],
        in_specs=[pl.BlockSpec(memory_space=pl.ANY) for _ in values],
        out_specs=[pl.BlockSpec(memory_space=pl.ANY) for _ in values],
        scratch_shapes=[pltpu.VMEM(v.shape, v.dtype) for v in values]
        + [pltpu.SemaphoreType.DMA((n,)), pltpu.SemaphoreType.DMA((n,))],
    )(*values)


def on_device(
    inputs, gain_one, shift_one, conv_weight, gain_two, shift_two, mix_weight, head_weight, head_bias, species, counts
):
    S, C = lax.axis_size("seq"), lax.axis_size("ch")
    s, c = lax.axis_index("seq"), lax.axis_index("ch")
    rows, width = inputs.shape
    depth, tracks = head_weight.shape
    o, fused = fused_step(
        S,
        C,
        x=inputs,
        gain1=gain_one,
        shift1=shift_one,
        cw=jnp.transpose(conv_weight, (0, 2, 1)),
        gain2=gain_two,
        shift2=shift_two,
        mix=mix_weight,
        hw=head_weight.reshape(4, depth // 4, tracks),
        bias=head_bias,
        species=species,
        counts=jnp.transpose(counts),
    )
    cwg, mwg = o.cwg, o.mwg
    if fused:
        head_weight_grad = o.hg
    else:
        cwg, mwg = lax.psum((cwg, mwg), "seq")
        part = o.wgo.reshape(NCHUNK, width, HW).astype(F32)
        part = jnp.transpose(part, (1, 0, 2))
        k = lax.rem(c, 2)
        human = jnp.zeros((width, 2, HALF_H), F32).at[:, k].set(part.reshape(width, HALF_H))
        mouse = jnp.zeros((width, 2, HALF_M), F32).at[:, k].set(part[:, :, :MW].reshape(width, HALF_M))
        first = (s * C + c // 2 * 2) * rows
        window = jnp.mod(first - SHIFT, rows * S * C) // WINDOW_BINS
        is_h = jnp.sum(jnp.where(jnp.arange(species.shape[0], dtype=jnp.int32) == window, species, 0)) == 0
        human = jnp.where(is_h, human.reshape(width, 2 * HALF_H)[:, :HUMAN], 0.0)
        mouse = jnp.where(is_h, 0.0, mouse.reshape(width, 2 * HALF_M)[:, :MOUSE])
        head_weight_grad = lax.psum_scatter(
            jnp.concatenate([human, mouse], axis=1), ("seq", "ch"), scatter_dimension=0, tiled=True
        )
    if fused:
        names = list(vars(o))
        o = types.SimpleNamespace(**dict(zip(names, handed_on(list(vars(o).values())), strict=True)))
        cwg, mwg, head_weight_grad = o.cwg, o.mwg, o.hg
    return (
        o.out,
        o.ig,
        o.g1,
        o.b1,
        jnp.transpose(cwg, (0, 2, 1)),
        o.g2,
        o.b2,
        mwg,
        head_weight_grad,
        o.hb,
    )


def solution(mesh):
    rows = P(("seq", "ch"), None)
    in_specs = (
        rows, P(), P(), P(None, None, "ch"), P("ch"), P("ch"), P("ch", None), P("ch", None), P(), P(), rows,
    )
    out_specs = (
        rows, rows, P(), P(), P(None, None, "ch"), P("ch"), P("ch"), P("ch", None), rows, P(),
    )
    return jax.shard_map(on_device, mesh=mesh, in_specs=in_specs, out_specs=out_specs, check_vma=False)
```

```python
import functools
import math
import types

import jax
import jax.numpy as jnp
from jax import lax
from jax.experimental import pallas as pl
from jax.experimental.pallas import tpu as pltpu
from jax.sharding import PartitionSpec as P

HUMAN = 5313
MOUSE = 1643
STEP = 11
TAPS = 3
WINDOW_BINS = 1024
SHIFT = 512
EPS = 1e-05

LANES = 128
NCHUNK = 7
HW = 384
MW = 128
CW = HW + MW
HALF_H = NCHUNK * HW
HALF_M = NCHUNK * MW
HALO = 32
EDGE = 16
MESH = pl.DeviceIdType.MESH
F32 = jnp.float32
BF16 = jnp.bfloat16
K0 = math.sqrt(2.0 / math.pi)
K1 = K0 * 0.044715


PLAN = {
    100: ((6, 4), (6, 0), (6, 3)),
    101: ((5, 4), (6, 1)),
    102: ((5, 0), (5, 3)),
    103: ((6, 2), (6, 5), (6, 6)),
    104: ((5, 1), (5, 2), (0, 0)),
    105: ((5, 5),),
    110: ((5, 6),),
    112: ((1, 1), (1, 0)),
    114: ((1, 2),),
    2: ((2, 1), (2, 2)),
    5: ((1, 5),),
    6: ((2, 0), (3, 1), (3, 2)),
    8: ((3, 0), (1, 4), (2, 5)),
    9: ((1, 3), (4, 1), (4, 2)),
    10: ((1, 6),),
    13: ((3, 5),),
    14: ((2, 4), (4, 0), (2, 3)),
    15: ((2, 6), (4, 5), (3, 3), (3, 4)),
    16: ((3, 6),),
    17: ((4, 3), (4, 4), (4, 6)),
}
X_FIRST = (2, 3, 6)


def nn(a, b):
    return lax.dot_general(a, b, (((1,), (0,)), ((), ())), preferred_element_type=F32)


def nt(a, b):
    return lax.dot_general(a, b, (((1,), (1,)), ((), ())), preferred_element_type=F32)


def gelu(v):
    return 0.5 * v * (1.0 + jnp.tanh(v * (K0 + K1 * (v * v))))


def gelu_slope(v):
    v2 = v * v
    th = jnp.tanh(v * (K0 + K1 * v2))
    return 0.5 * (1.0 + th) + 0.5 * v * (1.0 - th * th) * (K0 + 3.0 * K1 * v2)


def poisson_grad(logits, target):
    t = jnp.exp(-jnp.abs(logits))
    up = 1.0 + t
    series = t * (1.0 - t * (0.5 - t * (1.0 / 3.0 - t * 0.25)))
    rate = jnp.maximum(logits, 0.0) + jnp.where(t < 0.015625, series, jnp.log(up))
    return jnp.where(logits >= 0.0, 1.0, t) * (rate - target) / (up * rate)


def take(ref, sem):
    pltpu.make_async_copy(ref, ref, sem).wait()


def kernel_body(seqs, chs, fused, names, *refs):
    r = types.SimpleNamespace(**dict(zip(names, refs, strict=True)))
    r.sa, r.sb, r.ba, r.bb = ([getattr(r, f"{n}{i}") for i in range(4)] for n in ("sa", "sb", "ba", "bb"))
    S, C = seqs, chs
    s = lax.axis_index("seq")
    c = lax.axis_index("ch")
    xi = c // 2
    k = lax.rem(c, 2)
    other = c + 1 - 2 * k
    xnb = lax.rem(c + 2, C)
    xo = 1 - xi
    y = lax.rem(s, 2)
    z = s // 2
    ynb = s + 1 - 2 * y
    zb = lax.rem(z, 2)
    znb = s + 2 - 4 * zb
    dnb = znb + 1 - 2 * y
    q = lax.rem(s, 4)
    q_y = q + 1 - 2 * y
    q_z = q + 2 - 4 * zb
    q_d = q_z + 1 - 2 * y
    rows, width = r.x.shape
    n_dev = S * C
    total_bins = rows * n_dev
    inv_bins = 1.0 / total_bins
    me = s * C + c
    left = lax.rem(me + n_dev - 1, n_dev)
    right = lax.rem(me + 1, n_dev)
    left_dev = (left // C, lax.rem(left, C))
    right_dev = (right // C, lax.rem(right, C))
    row0 = me * rows
    window = lax.rem(row0 + total_bins - SHIFT, total_bins) // WINDOW_BINS
    left_same = lax.rem(row0 + total_bins - 1 + total_bins - SHIFT, total_bins) // WINDOW_BINS == window
    right_same = lax.rem(row0 + rows + total_bins - SHIFT, total_bins) // WINDOW_BINS == window

    def human_at_chip(seq, chip):
        first = (seq * C + chip * 2) * rows
        return r.species[lax.rem(first + total_bins - SHIFT, total_bins) // WINDOW_BINS] == 0

    mine_h = human_at_chip(s, xi)
    x_h = human_at_chip(s, xo)
    y_h = human_at_chip(ynb, xi)
    hp = C * LANES

    def put(src, dst, send, recv, dev):
        pltpu.make_async_remote_copy(
            src_ref=src, dst_ref=dst, send_sem=send, recv_sem=recv, device_id=dev, device_id_type=MESH
        ).start()

    barrier = pltpu.get_barrier_semaphore()

    def greet(dev):
        pl.semaphore_signal(barrier, inc=1, device_id=dev, device_id_type=MESH)

    for i in range(1, C):
        greet((s, lax.rem(c + i, C)))

    @pl.loop(1, S)
    def _(i):
        greet((lax.rem(s + i, S), c))

    greet(left_dev)
    greet(right_dev)

    W, TG = r.wbuf, r.tgb

    def human_at(half, j):
        return pl.ds(pl.multiple_of(half * HALF_H + j * HW, LANES), HW)

    def mouse_at(half, j):
        return pl.ds(pl.multiple_of(half * HALF_M + j * MW, LANES), MW)

    HV, MV, CB = r.hwv, r.mwv, r.cbuf
    load_hw = pltpu.make_async_copy(r.hw, HV, r.ld.at[0])
    load_hw.start()
    load_counts = pltpu.make_async_copy(r.counts, CB, r.ld.at[1])
    load_counts.start()
    CM, CS = r.cmf, r.cm
    cr = CS.shape[1]
    for t in range(TAPS):
        CS[t] = r.cw[t]
        CM[t, c, 0:cr, :] = r.cw[t]
    CS[TAPS] = r.mix[...]
    CM[TAPS, c, 0:cr, :] = r.mix[...]
    for t in range(4):
        for p in range(C):
            CM[t, p, cr:LANES, :] = jnp.zeros((LANES - cr, width), BF16)
    r.gs2[...] = jnp.zeros(r.gs2.shape, F32)
    r.gs2[0:1, 0:cr] = r.gain2[...].reshape(1, cr)
    r.gs2[1:2, 0:cr] = r.shift2[...].reshape(1, cr)
    M0 = HUMAN // LANES * LANES
    OFF = HUMAN - M0
    HP = r.hbpad
    tracks = HUMAN + MOUSE
    HP[:, 0:tracks] = r.bias[...].reshape(1, tracks)
    HP[:, tracks:] = jnp.zeros((1, HP.shape[1] - tracks), F32)
    BR = r.bias_rows
    for m in range(2 * NCHUNK):
        BR[m : m + 1, 0:HW] = HP[:, m * HW : (m + 1) * HW]
        v = HP[:, M0 + m * LANES : M0 + (m + 2) * LANES]
        BR[m : m + 1, HW:CW] = pltpu.roll(v, 2 * LANES - OFF, 1)[:, :MW]

    def spread(ref, vecs):
        n = vecs[0].shape[1] // LANES
        for i, v in enumerate(vecs):
            for t in range(n):
                ref[i * n + t : i * n + t + 1, :] = v[:, t * LANES : (t + 1) * LANES]
        if ref.shape[0] > n * len(vecs):
            ref[n * len(vecs) :, :] = jnp.zeros((ref.shape[0] - n * len(vecs), LANES), F32)

    def collect(v, n):
        m = n // LANES
        return [jnp.concatenate([v[i * m + t : i * m + t + 1, :] for t in range(m)], axis=1) for i in range(2)]

    def sum_start(i):
        src, bufs = r.sa[i], r.ba[i]
        for p in range(1, C):
            put(src, bufs.at[c], r.ars.at[2 * i], r.arr.at[2 * i], (s, lax.rem(c + p, C)))
        bufs[c] = src[...]

    def sum_middle(i):
        src, bufs, far = r.sb[i], r.ba[i], r.bb[i]
        take(bufs.at[pl.ds(0, C - 1)], r.arr.at[2 * i])
        v = bufs[0]
        for p in range(1, C):
            v = v + bufs[p]
        src[...] = v

        @pl.loop(1, S)
        def _(p):
            put(src, far.at[s], r.ars.at[2 * i + 1], r.arr.at[2 * i + 1], (lax.rem(s + p, S), c))

        far[s] = v

    def sum_end(i, n):
        far = r.bb[i]
        take(far.at[pl.ds(0, S - 1)], r.arr.at[2 * i + 1])
        if S <= 8:
            v = far[0]
            for p in range(1, S):
                v = v + far[p]
        else:
            v = lax.fori_loop(1, S, lambda p, a: a + far[p], far[0])
        return v, *collect(v, n)

    BLK = 32

    def block(i, shift=0):
        return pl.ds(pl.multiple_of(i * BLK + shift, 16), BLK)

    def row_sums(terms):
        def step(i, carry):
            return tuple(a + jnp.sum(t, 0, keepdims=True) for a, t in zip(carry, terms(i), strict=True))

        return step

    zero_w = jnp.zeros((1, width), F32)

    def x_terms(i):
        v = r.x[block(i), :].astype(F32)
        return v, v * v

    s1, q1 = lax.fori_loop(0, rows // BLK, row_sums(x_terms), (zero_w, zero_w))
    spread(r.sa0, (s1, q1))
    load_hw.wait()
    full = (tracks - M0) // LANES - 1
    for p in range(4):
        for m in range(2 * NCHUNK):
            if m < full:
                v = HV[p, :, M0 + m * LANES : M0 + (m + 2) * LANES].astype(F32)
                v = pltpu.roll(v, 2 * LANES - OFF, 1)[:, :MW]
            elif M0 + m * LANES < tracks:
                v = HV[p, :, M0 + m * LANES : min(tracks, M0 + (m + 2) * LANES)].astype(F32)
                v = jnp.concatenate([v, jnp.zeros((v.shape[0], 2 * LANES - v.shape[1]), F32)], axis=1)
                v = pltpu.roll(v, 2 * LANES - OFF, 1)[:, :MW]
            else:
                v = jnp.zeros((HV.shape[1], MW), F32)
            MV[p, :, m * MW : (m + 1) * MW] = v.astype(BF16)

    @pl.loop(0, NCHUNK)
    def _(j):
        pltpu.make_async_copy(HV.at[:, :, human_at(k, j)], W.at[j, c, :, :, pl.ds(0, HW)], r.wl.at[j]).start()
        pltpu.make_async_copy(MV.at[:, :, mouse_at(k, j)], W.at[j, c, :, :, pl.ds(HW, MW)], r.wl.at[j]).start()

    pl.semaphore_wait(barrier, C - 1 + S - 1 + 2)

    sum_start(0)
    put(r.x.at[pl.ds(rows - HALO, HALO)], r.xl, r.hs.at[0], r.hr.at[0], right_dev)
    put(r.x.at[pl.ds(0, HALO)], r.xr, r.hs.at[1], r.hr.at[1], left_dev)
    half_w = width // 2
    put(CS.at[q], CM.at[q, c, pl.ds(0, cr)], r.cms.at[0], r.cmr.at[0], (s, xnb))
    put(
        CS.at[q_d, :, pl.ds(0, half_w)],
        CM.at[q_d, c, pl.ds(0, cr), pl.ds(0, half_w)],
        r.cms.at[1],
        r.cmr.at[1],
        (s, xnb),
    )
    put(CS, CM.at[:, c, pl.ds(0, cr)], r.cms.at[2], r.cmr.at[2], (s, other))
    for p in range(1, C):
        put(r.gs2, r.gsb.at[c], r.gss, r.gsr, (s, lax.rem(c + p, C)))
    r.gsb[c] = r.gs2[...]

    @pl.loop(0, NCHUNK)
    def _(j):
        put(
            HV.at[:, :, human_at(1 - k, j)], W.at[j, c, :, :, pl.ds(0, HW)],
            r.wps, r.wp.at[j], (s, other),
        )
        put(
            MV.at[:, :, mouse_at(1 - k, j)], W.at[j, c, :, :, pl.ds(HW, MW)],
            r.wps, r.wp.at[j], (s, other),
        )
    HALFC = CW // 2

    def heads_along_x(j):
        for h in range(2):
            dev = (s, xo * 2 + h)
            hc = pl.multiple_of(h * HALF_H + j * HW, LANES)
            put(HV.at[q, :, human_at(h, j)], W.at[j, c, q, :, pl.ds(0, HW)], r.wxs, r.wx.at[j], dev)
            put(MV.at[q, :, mouse_at(h, j)], W.at[j, c, q, :, pl.ds(HW, MW)], r.wxs, r.wx.at[j], dev)
            put(
                HV.at[q_d, :, pl.ds(hc, HALFC)], W.at[j, c, q_d, :, pl.ds(0, HALFC)],
                r.wxs, r.wx.at[j], dev,
            )

    def relay_heads(j):
        take(W.at[j, pl.ds(0, 3), 0], r.wx.at[j])
        far = pl.ds(xo * 2, 2)
        put(W.at[j, far, q], W.at[j, far, q], r.wrs.at[0], r.wy.at[j], (ynb, c))
        put(W.at[j, far, q], W.at[j, far, q], r.wrs.at[1], r.wz.at[j], (znb, c))
        put(
            W.at[j, far, q, :, pl.ds(HALFC, HALFC)], W.at[j, far, q, :, pl.ds(HALFC, HALFC)],
            r.wrs.at[2], r.wd.at[j], (dnb, c),
        )

    def at(slot):
        for stage, j in PLAN.get(slot, ()):
            if stage == 0:
                put(A.at[pl.ds(HALO - EDGE, ext)], r.actx, r.as_, r.ar_, (s, xnb))
            elif stage == 5:
                relay_heads(j)
            elif stage == 6:
                heads_along_x(j)
            elif fused and stage == 4:
                last(j)
            elif fused:
                (first, second, third)[stage - 1](j, j in X_FIRST)

    ext = rows + 2 * EDGE
    at(100)

    def pass_weights():
        take(CM.at[0, 0, pl.ds(0, cr)], r.cmr.at[0])
        put(CM.at[q, xnb, pl.ds(0, cr)], CM.at[q, xnb, pl.ds(0, cr)], r.cms.at[3], r.cmr.at[3], (ynb, c))
        put(CM.at[q, xnb, pl.ds(0, cr)], CM.at[q, xnb, pl.ds(0, cr)], r.cms.at[4], r.cmr.at[4], (znb, c))
        second = pl.ds(half_w, half_w)
        put(
            CM.at[q, xnb, pl.ds(0, cr), second], CM.at[q, xnb, pl.ds(0, cr), second],
            r.cms.at[5], r.cmr.at[5], (dnb, c),
        )

    def targets(half, dst, j):
        at = pl.multiple_of(half * HALF_H + j * HW, 8)
        am = pl.multiple_of(half * HALF_M + j * MW, 8)
        v = CB[pl.ds(at, MW), :]
        dst[:, 0:MW] = jnp.where(mine_h, v, CB[pl.ds(am, MW), :]).astype(F32).T.astype(BF16)
        ends = (half == 1) & (j == NCHUNK - 1)

        @pl.when(ends)
        def _():
            dst[:, MW:HW] = CT[...].astype(F32).T.astype(BF16)

        @pl.when(jnp.logical_not(ends))
        def _():
            dst[:, MW:HW] = CB[pl.ds(at + MW, HW - MW), :].astype(F32).T.astype(BF16)

    load_counts.wait()
    CT = r.ctail
    whole = HUMAN - (2 * HALF_H - HW + MW)
    CT[0:whole, :] = CB[HUMAN - whole : HUMAN, :]
    CT[whole:, :] = jnp.zeros((CT.shape[0] - whole, CT.shape[1]), jnp.int32)
    sum_middle(0)
    pass_weights()

    @pl.loop(0, NCHUNK)
    def _(j):
        targets(k, TG.at[j, k], j)

    _, t1, u1 = sum_end(0, width)
    mean1 = t1 * inv_bins
    scale1 = lax.rsqrt(u1 * inv_bins - mean1 * mean1 + EPS)
    gain1 = r.gain1[...].reshape(1, width)
    off1 = r.shift1[...].reshape(1, width)

    A = r.act

    def normed1_of(v):
        return (v - mean1) * scale1

    def act_rows(v):
        return gelu(normed1_of(v.astype(F32)) * gain1 + off1)

    @pl.loop(0, rows // BLK)
    def _(i):
        at = pl.multiple_of(i * BLK, BLK)
        A[pl.ds(at + HALO, BLK), :] = act_rows(r.x[pl.ds(at, BLK), :]).astype(BF16)

    take(r.xl, r.hr.at[0])
    A[0:HALO, :] = jnp.where(left_same, act_rows(r.xl[...]), 0.0).astype(BF16)
    take(r.xr, r.hr.at[1])
    A[rows + HALO : rows + 2 * HALO, :] = jnp.where(right_same, act_rows(r.xr[...]), 0.0).astype(BF16)

    at(101)
    take(CM.at[0, 0, pl.ds(0, cr), pl.ds(0, half_w)], r.cmr.at[1])
    take(CM.at[0, 0, pl.ds(0, cr)], r.cmr.at[3])
    take(CM.at[0, 0, pl.ds(0, cr)], r.cmr.at[4])
    take(CM.at[0, 0, pl.ds(0, cr), pl.ds(0, half_w)], r.cmr.at[5])
    put(CM.at[:, xnb, pl.ds(0, cr)], CM.at[:, xnb, pl.ds(0, cr)], r.cms.at[6], r.cmr.at[6], (s, other))
    take(CM.at[:, 0, pl.ds(0, cr)], r.cmr.at[2])
    take(CM.at[:, 0, pl.ds(0, cr)], r.cmr.at[6])

    PR = r.prod
    for t in range(TAPS):
        PR[t] = nt(A[...], CM[t].reshape(hp, width))
    CV = r.cv
    lo = HALO - EDGE
    CV[...] = (
        PR[0, lo - STEP : lo - STEP + ext, :] + PR[1, lo : lo + ext, :] + PR[2, lo + STEP : lo + STEP + ext, :]
    )
    at(102)
    zero_h = jnp.zeros((1, hp), F32)

    def c_terms(i):
        v = CV[block(i, EDGE), :]
        return v, v * v

    s2, q2 = lax.fori_loop(0, rows // BLK, row_sums(c_terms), (zero_h, zero_h))
    spread(r.sa1, (s2, q2))
    sum_start(1)
    at(103)

    @pl.loop(0, NCHUNK)
    def _(j):
        targets(1 - k, r.tgx.at[j], j)
        put(r.tgx.at[j], TG.at[j, k], r.tps, r.tp.at[j], (s, other))

    sum_middle(1)
    at(104)
    _, t2, u2 = sum_end(1, hp)
    mean2 = t2 * inv_bins
    scale2 = lax.rsqrt(u2 * inv_bins - mean2 * mean2 + EPS)
    take(r.gsb.at[pl.ds(0, C - 1)], r.gsr)
    gain2 = jnp.concatenate([r.gsb[p, 0:1, :] for p in range(C)], axis=1)
    off2 = jnp.concatenate([r.gsb[p, 1:2, :] for p in range(C)], axis=1)

    def normed2_of(v):
        return (v - mean2) * scale2

    A2 = r.a2

    @pl.loop(0, rows // BLK)
    def _(i):
        at = pl.multiple_of(i * BLK, BLK)
        v = normed2_of(CV[pl.ds(at + EDGE, BLK), :])
        A2[pl.ds(at, BLK), :] = gelu(v * gain2 + off2).astype(BF16)

    O = r.ob
    mixf = CM[3].reshape(hp, width)
    outputs = (r.x[...].astype(F32) + nn(A2[...], mixf)).astype(BF16)
    O[k] = outputs
    r.out[...] = outputs
    put(O.at[k], O.at[k], r.os, r.orr, (s, other))
    at(105)
    r.a2t[...] = A2[...].T
    take(O.at[0], r.orr)
    OT = r.ot
    OT[...] = O[...].reshape(2 * rows, width).T
    GO = r.go
    GO[...] = jnp.zeros(GO.shape, F32)
    WG, GL = r.wg, (r.gl0, r.gl1)
    LG = r.lg
    HB = r.hbs
    HB[...] = jnp.zeros(HB.shape, F32)
    Z = S // 2
    if fused:
        A1, R1, R2, R3 = r.acc1, r.r1, r.r2, r.r3
        two = A1.shape[3]
        own = two // 2

        def first(j, ax):
            if ax:
                put(WG.at[j, :, :, xo], R1.at[j], r.s1.at[j], r.g1r.at[j], (s, xnb))
            else:
                put(WG.at[j, :, 1 - y], R1.at[j], r.s1.at[j], r.g1r.at[j], (ynb, c))

        def second(j, ax):
            take(R1.at[j], r.g1r.at[j])
            got_h = x_h if ax else y_h

            def step(i, _):
                zz, b = i // 2, lax.rem(i, 2)
                a = (WG[j, zz, b, xi] if ax else WG[j, zz, y, b]).astype(F32)
                g = R1[j, zz, b].astype(F32)
                A1[j, zz, b, :, 0:HW] = (jnp.where(mine_h, a, 0.0) + jnp.where(got_h, g, 0.0)).astype(BF16)
                A1[j, zz, b, :, HW:CW] = (
                    jnp.where(mine_h, 0.0, a[:, :MW]) + jnp.where(got_h, 0.0, g[:, :MW])
                ).astype(BF16)
                return 0

            lax.fori_loop(0, S, step, 0)
            if ax:
                put(A1.at[j, :, 1 - y], R2.at[j], r.s2.at[j], r.g2r.at[j], (ynb, c))
            else:
                put(A1.at[j, :, xo], R2.at[j], r.s2.at[j], r.g2r.at[j], (s, xnb))

        def third(j, ax):
            take(R2.at[j], r.g2r.at[j])
            b = y if ax else xi
            for zz in range(Z):
                R2[j, zz] = (A1[j, zz, b].astype(F32) + R2[j, zz].astype(F32)).astype(BF16)
            R3[j, z] = R2[j, z]
            for p in range(1, Z):
                to = lax.rem(z + p, Z)
                put(R2.at[j, to], R3.at[j, z], r.s3.at[j], r.g3r.at[j], (to * 2 + y, c))

        def last(j):
            take(R3.at[j, pl.ds(0, Z - 1)], r.g3r.at[j])
            v = R3[j, 0].astype(F32)
            for p in range(1, Z):
                v = v + R3[j, p].astype(F32)
            r.fin[j] = v.reshape(2, own, CW)
            put(r.fin.at[j, 1 - k], r.fr.at[j], r.s4.at[j], r.g4r.at[j], (s, other))

    def chunk_arrives(j):
        take(W.at[j, 0], r.wl.at[j])
        take(W.at[j, 0], r.wp.at[j])
        take(W.at[j, pl.ds(0, 2), 0], r.wy.at[j])
        take(W.at[j, pl.ds(0, 2), 0], r.wz.at[j])
        take(W.at[j, pl.ds(0, 2), 0, :, pl.ds(0, HALFC)], r.wd.at[j])
        take(TG.at[j, 0], r.tp.at[j])

    def tracks_of(j):
        head = jnp.where(
            mine_h, W[j, :, :, :, 0:MW].reshape(width, MW), W[j, :, :, :, HW:CW].reshape(width, MW)
        )
        return jnp.concatenate([head, W[j, :, :, :, MW:HW].reshape(width, HW - MW)], axis=1)

    def chunk_grads(j):
        wv = tracks_of(j)
        for h in range(2):
            LG[h] = nn(O[h], wv)
        valid_n = jnp.where(mine_h, HUMAN - (k * HALF_H + j * HW), jnp.minimum(MOUSE - (k * HALF_M + j * MW), MW))
        valid = lax.broadcasted_iota(jnp.int32, (1, HW), 1) < valid_n
        brow = BR[pl.ds(k * NCHUNK + j, 1), :]
        bias = jnp.concatenate([jnp.where(mine_h, brow[:, :MW], brow[:, HW:]), brow[:, MW:HW]], axis=1)
        acc = jnp.zeros((8, HW), F32)
        for h in range(2):
            for i in range(rows // BLK):
                at = slice(i * BLK, (i + 1) * BLK)
                g = poisson_grad(LG[h, at, :] + bias, TG[j, h, at, :].astype(F32))
                g = jnp.where(valid, g, 0.0).astype(BF16)
                GL[j % 2][h, at, :] = g
                acc = acc + jnp.sum(g.astype(F32).reshape(BLK // 8, 8, HW), 0)
        bsum = jnp.sum(acc, 0, keepdims=True)
        HB[j : j + 1, 0:HW] = jnp.where(mine_h, bsum, 0.0)
        HB[j : j + 1, HW:CW] = jnp.where(mine_h, 0.0, bsum[:, :MW])

    def chunk_products(j):
        g = GL[j % 2][...].reshape(2 * rows, HW)
        GO[...] += nt(g, tracks_of(j)).reshape(GO.shape)
        WG[j] = nn(OT[...], g).astype(BF16).reshape(WG.shape[1:])

    at(0)
    for j in range(NCHUNK + 1):
        if j < NCHUNK:
            chunk_arrives(j)
            chunk_grads(j)
        if j > 0:
            chunk_products(j - 1)
        at(110 + j)

    put(GO.at[1 - k], r.gor, r.gos, r.gorr, (s, other))
    put(r.hbs, r.hbx, r.hbsem.at[0], r.hbrem.at[0], (s, xnb))
    at(1)

    if fused:
        CP, C1, C3, CF = ([getattr(r, f"{n}{i}") for i in range(3)] for n in ("cp", "c1", "c3", "cf"))

        def lanes(b):
            return pl.ds(pl.multiple_of(b * half_w, LANES), half_w)

        def weights_out(i, v):
            CP[i][...] = v.astype(BF16).reshape(CP[i].shape)
            put(CP[i].at[:, :, lanes(1 - y)], C1[i], r.ccs.at[4 * i], r.ccr.at[4 * i], (ynb, c))

        def weights_along_z(i):
            take(C1[i], r.ccr.at[4 * i])
            C1[i][...] = (C1[i][...].astype(F32) + CP[i][:, :, lanes(y)].astype(F32)).astype(BF16)
            C3[i][z] = C1[i][z]
            for p in range(1, Z):
                to = lax.rem(z + p, Z)
                put(C1[i].at[to], C3[i].at[z], r.ccs.at[4 * i + 1], r.ccr.at[4 * i + 1], (to * 2 + y, c))

        def weights_back_z(i):
            take(C3[i].at[pl.ds(0, Z - 1)], r.ccr.at[4 * i + 1])
            v = C3[i][0].astype(F32)
            for p in range(1, Z):
                v = v + C3[i][p].astype(F32)
            CF[i][z, :, lanes(y)] = v.astype(BF16)
            for p in range(1, Z):
                to = lax.rem(z + p, Z)
                mine = CF[i].at[z, :, lanes(y)]
                put(mine, mine, r.ccs.at[4 * i + 2], r.ccr.at[4 * i + 2], (to * 2 + y, c))

        def weights_back_y(i):
            take(CF[i].at[pl.ds(0, Z - 1), :, pl.ds(0, half_w)], r.ccr.at[4 * i + 2])
            mine = CF[i].at[:, :, lanes(y)]
            put(mine, mine, r.ccs.at[4 * i + 3], r.ccr.at[4 * i + 3], (ynb, c))

    G, GOR = r.gbe, r.gor
    take(GOR, r.gorr)

    @pl.loop(0, rows // BLK)
    def _(i):
        v = GO[k, block(i), :] + GOR[block(i), :]
        GOR[block(i), :] = v
        G[block(i, EDGE), :] = v.astype(BF16)

    put(G.at[pl.ds(EDGE, EDGE)], G.at[pl.ds(rows + EDGE, EDGE)], r.gs.at[0], r.gr.at[0], left_dev)
    put(G.at[pl.ds(rows, EDGE)], G.at[pl.ds(0, EDGE)], r.gs.at[1], r.gr.at[1], right_dev)
    GA, GP = r.ga, r.gp
    GA[EDGE : EDGE + rows, :] = nt(G[EDGE : EDGE + rows, :], mixf)

    def pull_two(at):
        v = normed2_of(CV[at, :])
        g = GA[at, :] * gelu_slope(v * gain2 + off2)
        GP[at, :] = g
        return g * v, g

    gs_, ss_ = lax.fori_loop(0, rows // BLK, row_sums(lambda i: pull_two(block(i, EDGE))), (zero_h, zero_h))
    spread(r.sa2, (gs_, ss_))
    sum_start(2)
    at(2)
    MP = r.mp
    mp = nn(r.a2t[...], G[EDGE : EDGE + rows, :]).astype(BF16).reshape(C, LANES, width)
    for p in range(C):
        MP[p % 2, p // 2] = mp[p, 0:cr, :]
    put(MP.at[1 - k], r.mr, r.mps.at[0], r.mpr.at[0], (s, other))
    at(3)
    sum_middle(2)
    HX = r.hbx
    take(HX, r.hbrem.at[0])
    HX[...] = HX[...] + HB[...]

    @pl.loop(1, S)
    def _(p):
        put(HX, r.hbf.at[s], r.hbsem.at[1], r.hbrem.at[1], (lax.rem(s + p, S), c))

    r.hbf[s] = HX[...]
    at(4)
    take(r.mr, r.mpr.at[0])
    MR = r.mr
    MR[...] = (MR[...].astype(F32) + MP[k].astype(F32)).astype(BF16)
    put(MR.at[xo], r.mx, r.mps.at[1], r.mpr.at[1], (s, xnb))
    at(5)
    take(r.xedge, r.gr.at[0])
    take(r.xedge, r.gr.at[1])
    for e in (0, rows + EDGE):
        GA[e : e + EDGE, :] = nt(G[e : e + EDGE, :], mixf)
        pull_two(slice(e, e + EDGE))
    at(6)
    total2, gsum2, ssum2 = sum_end(2, hp)
    r.tot[...] = total2
    r.g2[...] = r.tot[pl.ds(c, 1), 0:cr].reshape(cr)
    r.b2[...] = r.tot[pl.ds(C + c, 1), 0:cr].reshape(cr)
    coef2 = gain2 * scale2
    gmean2, smean2 = gsum2 * inv_bins, ssum2 * inv_bins
    GC, GB = r.gce, r.gcb

    def conv_grad(at):
        return (coef2 * (GP[at, :] - smean2 - normed2_of(CV[at, :]) * gmean2)).astype(BF16)

    hx = hp // 2

    @pl.loop(0, rows // BLK)
    def _(i):
        v = conv_grad(block(i, EDGE))
        GC[block(i, EDGE), :] = v.astype(F32)
        GB[0, block(i), :] = v[:, :hx]
        GB[1, block(i), :] = v[:, hx:]

    put(GB.at[xo], r.gcx, r.gbs, r.gbr, (s, xnb))
    take(r.mx, r.mpr.at[1])
    mix_sum = MR[xi].astype(F32) + r.mx[...].astype(F32)
    if fused:
        weights_out(0, mix_sum)
    else:
        r.mwg[...] = mix_sum
    GC[0:EDGE, :] = jnp.where(left_same, conv_grad(slice(0, EDGE)).astype(F32), 0.0)
    GC[rows + EDGE : ext, :] = jnp.where(right_same, conv_grad(slice(rows + EDGE, ext)).astype(F32), 0.0)
    at(7)


    G1 = r.ga1
    for t in range(TAPS):
        lo_t = EDGE + STEP - t * STEP
        part = nn(GC[lo_t : lo_t + rows, :].astype(BF16), CM[t].reshape(hp, width))
        G1[...] = part if t == 0 else G1[...] + part

    def pull_one(i):
        v = normed1_of(r.x[block(i), :].astype(F32))
        g = G1[block(i), :] * gelu_slope(v * gain1 + off1)
        G1[block(i), :] = g
        return g * v, g

    g1s, s1s = lax.fori_loop(0, rows // BLK, row_sums(pull_one), (zero_w, zero_w))
    spread(r.sa3, (g1s, s1s))
    sum_start(3)
    at(8)

    ZP, CG = r.zpad, r.cg
    pad = ZP.shape[0] - rows
    ZP[0 : pad // 2, :] = jnp.zeros((pad // 2, hx), F32)
    ZP[rows + pad // 2 :, :] = jnp.zeros((pad // 2, hx), F32)
    for part in range(2):
        if part == 1:
            take(r.actx, r.ar_)
            take(r.gcx, r.gbr)
        ZP[pad // 2 : pad // 2 + rows, :] = (GB[xi] if part == 0 else r.gcx[...]).astype(F32)
        rows_act = A[lo : lo + ext, :] if part == 0 else r.actx[...]
        for t in range(TAPS):
            lo_t = pad // 2 - EDGE + STEP - t * STEP
            v = nn(ZP[lo_t : lo_t + ext, :].T.astype(BF16), rows_act).reshape(2, LANES, width)
            CG[t] = v if part == 0 else CG[t] + v
    put(CG.at[:, 1 - k, pl.ds(0, cr)], r.cgr, r.cgs, r.cgrr, (s, other))
    at(9)
    if fused:
        weights_along_z(0)
    sum_middle(3)
    at(10)
    take(r.cgr, r.cgrr)
    conv_sum = [CG[t, k, 0:cr, :] + r.cgr[t] for t in range(TAPS)]
    if fused:
        weights_out(1, jnp.concatenate([conv_sum[0], conv_sum[1][0:64]], axis=0))
        weights_out(2, jnp.concatenate([conv_sum[1][64:], conv_sum[2]], axis=0))
        at(12)
    else:
        for t in range(TAPS):
            r.cwg[t] = conv_sum[t]
        r.wgo[...] = WG[...]

    take(r.hbf.at[pl.ds(0, S - 1)], r.hbrem.at[1])
    HB3 = r.hb3
    HB3[...] = lax.fori_loop(1, S, lambda p, a: a + r.hbf[p], r.hbf[0])
    put(HB3, r.hbp, r.hbsem.at[2], r.hbrem.at[2], (s, other))
    at(13)

    def input_gradient():
        total1, gsum1, ssum1 = sum_end(3, width)
        r.g1[...] = gsum1.reshape(width)
        r.b1[...] = ssum1.reshape(width)
        coef1 = gain1 * scale1
        gmean1, smean1 = gsum1 * inv_bins, ssum1 * inv_bins

        @pl.loop(0, rows // BLK)
        def _(i):
            v = normed1_of(r.x[block(i), :].astype(F32))
            r.ig[block(i), :] = GOR[block(i), :] + coef1 * (G1[block(i), :] - smean1 - v * gmean1)

    if fused:
        weights_along_z(1)
        weights_along_z(2)
        input_gradient()
        at(14)
        weights_back_z(0)
        weights_back_z(1)
        weights_back_z(2)
        at(15)
        weights_back_y(0)
        weights_back_y(1)
        weights_back_y(2)
        at(16)
        for i in range(3):
            take(CF[i].at[:, :, pl.ds(0, half_w)], r.ccr.at[4 * i + 3])
        r.mwg[...] = CF[0][...].reshape(cr, width).astype(F32)
        v = CF[1][...].reshape(cr + 64, width).astype(F32)
        r.cwg[0] = v[0:cr]
        r.cwg[1, 0:64, :] = v[cr:]
        v = CF[2][...].reshape(2 * cr - 64, width).astype(F32)
        r.cwg[1, 64:, :] = v[0 : cr - 64]
        r.cwg[2] = v[cr - 64 :]
        at(17)
    if not fused:
        input_gradient()
    take(r.hbp, r.hbrem.at[2])

    def in_order(dst, human, mouse):
        for m in range(M0 // HW):
            dst[:, m * HW : (m + 1) * HW] = human(m // NCHUNK, m % NCHUNK)
        edge = M0 // HW * HW
        v = human(edge // HALF_H, edge // HW % NCHUNK)
        if edge < M0:
            dst[:, edge:M0] = v[:, 0 : M0 - edge]
        before = v[:, M0 - edge : M0 - edge + LANES]
        lane = lax.broadcasted_iota(jnp.int32, (1, LANES), 1)
        for m in range(pl.cdiv(tracks - M0, LANES)):
            here = mouse(m // NCHUNK, m % NCHUNK) if m < 2 * NCHUNK else jnp.zeros_like(before)
            moved = pltpu.roll(here, OFF, 1)
            out = jnp.where(lane < OFF, before, moved)
            n = min(LANES, tracks - M0 - m * LANES)
            dst[:, M0 + m * LANES : M0 + m * LANES + n] = out[:, 0:n]
            before = moved

    HO = r.hbo
    HO[0] = jnp.where(k == 0, HB3[...], r.hbp[...])
    HO[1] = jnp.where(k == 0, r.hbp[...], HB3[...])
    in_order(r.hbrow, lambda h, j: HO[h, j : j + 1, 0:HW], lambda h, j: HO[h, j : j + 1, HW:CW])
    r.hb[...] = r.hbrow[...].reshape(tracks)
    if fused:
        for j in range(NCHUNK):
            take(r.fr.at[j], r.g4r.at[j])

        def piece(h, j, at, n):
            return jnp.where(k == h, r.fin[j, k, :, at : at + n], r.fr[j, :, at : at + n])

        in_order(r.hg, lambda h, j: piece(h, j, 0, HW), lambda h, j: piece(h, j, HW, MW))

    for i in range(4):
        take(r.ba[i].at[pl.ds(0, C - 1)], r.ars.at[2 * i])
        take(r.bb[i].at[pl.ds(0, S - 1)], r.ars.at[2 * i + 1])
    take(r.xl, r.hs.at[0])
    take(r.xr, r.hs.at[1])
    take(CM.at[0, 0, pl.ds(0, cr)], r.cms.at[0])
    take(CM.at[0, 0, pl.ds(0, cr), pl.ds(0, half_w)], r.cms.at[1])
    take(CS, r.cms.at[2])
    take(CM.at[0, 0, pl.ds(0, cr)], r.cms.at[3])
    take(CM.at[0, 0, pl.ds(0, cr)], r.cms.at[4])
    take(CM.at[0, 0, pl.ds(0, cr), pl.ds(0, half_w)], r.cms.at[5])
    take(CS, r.cms.at[6])
    take(r.gsb.at[pl.ds(0, C - 1)], r.gss)
    take(W.at[:, 0], r.wps)
    take(TG.at[:, 0], r.tps)
    take(W.at[:, pl.ds(0, 3), 0], r.wxs)
    take(W.at[:, pl.ds(0, 2), 0], r.wrs.at[0])
    take(W.at[:, pl.ds(0, 2), 0], r.wrs.at[1])
    take(W.at[:, 0, 0], r.wrs.at[2])
    take(r.actx, r.as_)
    take(O.at[0], r.os)
    take(GOR, r.gos)
    take(HX, r.hbsem.at[0])
    take(r.hbf.at[pl.ds(0, S - 1)], r.hbsem.at[1])
    take(HB3, r.hbsem.at[2])
    take(r.xedge, r.gs.at[0])
    take(r.xedge, r.gs.at[1])
    take(r.mr, r.mps.at[0])
    take(r.mx, r.mps.at[1])
    take(r.gcx, r.gbs)
    take(r.cgr, r.cgs)
    if fused:
        for i in range(3):
            take(C1[i], r.ccs.at[4 * i])
            take(C3[i].at[pl.ds(0, Z - 1)], r.ccs.at[4 * i + 1])
            take(CF[i].at[pl.ds(0, Z - 1), :, pl.ds(0, half_w)], r.ccs.at[4 * i + 2])
            take(CF[i].at[:, :, pl.ds(0, half_w)], r.ccs.at[4 * i + 3])
        for j in range(NCHUNK):
            take(R1.at[j], r.s1.at[j])
            take(R2.at[j], r.s2.at[j])
            take(R3.at[j, pl.ds(0, Z - 1)], r.s3.at[j])
            take(r.fr.at[j], r.s4.at[j])


def fused_step(seqs, chs, **ins):
    S, C = seqs, chs
    rows, width = ins["x"].shape
    n_dev = S * C
    hp = C * LANES
    cr = ins["mix"].shape[0]
    kr = ins["hw"].shape[1]
    tracks = ins["bias"].shape[0]
    ext = rows + 2 * EDGE
    Z = S // 2
    fused = width % (n_dev * 8) == 0 and Z == 4
    two = 2 * (width // n_dev)
    vm = pltpu.VMEM
    dma = pltpu.SemaphoreType.DMA
    any_ins = ("hw", "counts")
    outs = dict(
        out=((rows, width), BF16),
        ig=((rows, width), F32),
        g1=((width,), F32),
        b1=((width,), F32),
        cwg=((TAPS, cr, width), F32),
        g2=((cr,), F32),
        b2=((cr,), F32),
        mwg=((cr, width), F32),
        hb=((tracks,), F32),
    )
    if fused:
        outs["hg"] = ((two // 2, tracks), F32)
    else:
        outs["wgo"] = ((NCHUNK, Z, 2, 2, width // (4 * Z), HW), BF16)
    scratch = dict(
        xl=vm((HALO, width), BF16),
        xr=vm((HALO, width), BF16),
        xedge=vm((EDGE, width), BF16),
        gs2=vm((8, LANES), F32),
        gsb=vm((C, 8, LANES), F32),
        cm=vm((4, cr, width), BF16),
        cmf=vm((4, C, LANES, width), BF16),
        hwv=vm((4, kr, tracks), BF16),
        mwv=vm((4, kr, 2 * HALF_M), BF16),
        cbuf=vm((HUMAN, rows), jnp.int32),
        ctail=vm((HW - MW, rows), jnp.int32),
        hbpad=vm((1, HUMAN // LANES * LANES + (2 * NCHUNK + 1) * LANES), F32),
        bias_rows=vm((16, CW), F32),
        wbuf=vm((NCHUNK, 4, 4, kr, CW), BF16),
        tgb=vm((NCHUNK, 2, rows, HW), BF16),
        tgx=vm((NCHUNK, rows, HW), BF16),
        act=vm((rows + 2 * HALO, width), BF16),
        actx=vm((ext, width), BF16),
        prod=vm((TAPS, rows + 2 * HALO, hp), F32),
        cv=vm((ext, hp), F32),
        a2=vm((rows, hp), BF16),
        a2t=vm((hp, rows), BF16),
        ob=vm((2, rows, width), BF16),
        ot=vm((width, 2 * rows), BF16),
        lg=vm((2, rows, HW), F32),
        gl0=vm((2, rows, HW), BF16),
        gl1=vm((2, rows, HW), BF16),
        wg=vm((NCHUNK, Z, 2, 2, width // (4 * Z), HW), BF16),
        go=vm((2, rows, width), F32),
        gor=vm((rows, width), F32),
        hbs=vm((8, CW), F32),
        hbx=vm((8, CW), F32),
        hbf=vm((S, 8, CW), F32),
        hb3=vm((8, CW), F32),
        hbp=vm((8, CW), F32),
        hbo=vm((2, 8, CW), F32),
        hbrow=vm((1, tracks), F32),
        gbe=vm((ext, width), BF16),
        ga=vm((ext, hp), F32),
        gp=vm((ext, hp), F32),
        gce=vm((ext, hp), F32),
        gcb=vm((2, rows, hp // 2), BF16),
        gcx=vm((rows, hp // 2), BF16),
        ga1=vm((rows, width), F32),
        mp=vm((2, 2, cr, width), BF16),
        mr=vm((2, cr, width), BF16),
        mx=vm((cr, width), BF16),
        zpad=vm((rows + 64, hp // 2), F32),
        cg=vm((TAPS, 2, LANES, width), F32),
        cgr=vm((TAPS, cr, width), F32),
        tot=vm((8, LANES), F32),
    )
    for i, n in enumerate((16, 8, 8, 16)):
        scratch[f"sa{i}"] = vm((n, LANES), F32)
        scratch[f"sb{i}"] = vm((n, LANES), F32)
        scratch[f"ba{i}"] = vm((C, n, LANES), F32)
        scratch[f"bb{i}"] = vm((S, n, LANES), F32)
    sems = dict(
        ars=8, arr=8, hs=2, hr=2, cms=7, cmr=7, gss=0, gsr=0, ld=2, wl=7, wp=7, wx=7, wy=7, wz=7, wd=7, wps=0, wxs=0,
        wrs=3, tp=7, tps=0, as_=0, ar_=0, os=0, gos=0, gorr=0, hbsem=3, hbrem=3, gs=2, gr=2, mps=2, mpr=2, gbs=0,
        gbr=0, cgs=0, cgrr=0, orr=0,
    )
    if fused:
        scratch.update(
            acc1=vm((NCHUNK, Z, 2, two, CW), BF16),
            r1=vm((NCHUNK, Z, 2, two, HW), BF16),
            r2=vm((NCHUNK, Z, two, CW), BF16),
            r3=vm((NCHUNK, Z, two, CW), BF16),
            fin=vm((NCHUNK, 2, two // 2, CW), F32),
            fr=vm((NCHUNK, two // 2, CW), F32),
        )
        for i, n in enumerate((cr, cr + 64, 2 * cr - 64)):
            scratch[f"cp{i}"] = vm((Z, n // Z, width), BF16)
            scratch[f"c1{i}"] = vm((Z, n // Z, width // 2), BF16)
            scratch[f"c3{i}"] = vm((Z, n // Z, width // 2), BF16)
            scratch[f"cf{i}"] = vm((Z, n // Z, width), BF16)
        sems.update(s1=7, s2=7, s3=7, s4=7, g1r=7, g2r=7, g3r=7, g4r=7, ccs=12, ccr=12)
    for name, n in sems.items():
        scratch[name] = dma((n,)) if n else dma
    names = [*ins, *outs, *scratch]

    def space(name):
        if name == "species":
            return pl.BlockSpec(memory_space=pltpu.SMEM)
        return pl.BlockSpec(memory_space=pl.ANY if name in any_ins else pltpu.VMEM)

    got = pl.pallas_call(
        functools.partial(kernel_body, S, C, fused, names),
        out_shape=[jax.ShapeDtypeStruct(*v) for v in outs.values()],
        in_specs=[space(n) for n in ins],
        out_specs=[pl.BlockSpec(memory_space=pltpu.VMEM) for _ in outs],
        scratch_shapes=list(scratch.values()),
        compiler_params=pltpu.CompilerParams(
            collective_id=0, has_side_effects=True, vmem_limit_bytes=67_043_328
        ),
    )(*ins.values())
    return types.SimpleNamespace(**dict(zip(outs, got, strict=True))), fused


def handed_on(values):
    n = len(values)

    def body(*refs):
        ins, outs, held = refs[:n], refs[n : 2 * n], refs[2 * n : 3 * n]
        come = [pltpu.make_async_copy(ins[i], held[i], refs[3 * n].at[i]) for i in range(n)]
        go = [pltpu.make_async_copy(held[i], outs[i], refs[3 * n + 1].at[i]) for i in range(n)]
        for copy in come:
            copy.start()
        for i in range(n):
            come[i].wait()
            go[i].start()
        for copy in go:
            copy.wait()

    return pl.pallas_call(
        body,
        out_shape=[jax.ShapeDtypeStruct(v.shape, v.dtype) for v in values],
        in_specs=[pl.BlockSpec(memory_space=pl.ANY) for _ in values],
        out_specs=[pl.BlockSpec(memory_space=pl.ANY) for _ in values],
        scratch_shapes=[pltpu.VMEM(v.shape, v.dtype) for v in values]
        + [pltpu.SemaphoreType.DMA((n,)), pltpu.SemaphoreType.DMA((n,))],
    )(*values)


def on_device(
    inputs, gain_one, shift_one, conv_weight, gain_two, shift_two, mix_weight, head_weight, head_bias, species, counts
):
    S, C = lax.axis_size("seq"), lax.axis_size("ch")
    s, c = lax.axis_index("seq"), lax.axis_index("ch")
    rows, width = inputs.shape
    depth, tracks = head_weight.shape
    o, fused = fused_step(
        S,
        C,
        x=inputs,
        gain1=gain_one,
        shift1=shift_one,
        cw=jnp.transpose(conv_weight, (0, 2, 1)),
        gain2=gain_two,
        shift2=shift_two,
        mix=mix_weight,
        hw=head_weight.reshape(4, depth // 4, tracks),
        bias=head_bias,
        species=species,
        counts=jnp.transpose(counts),
    )
    cwg, mwg = o.cwg, o.mwg
    if fused:
        head_weight_grad = o.hg
    else:
        cwg, mwg = lax.psum((cwg, mwg), "seq")
        part = o.wgo.reshape(NCHUNK, width, HW).astype(F32)
        part = jnp.transpose(part, (1, 0, 2))
        k = lax.rem(c, 2)
        human = jnp.zeros((width, 2, HALF_H), F32).at[:, k].set(part.reshape(width, HALF_H))
        mouse = jnp.zeros((width, 2, HALF_M), F32).at[:, k].set(part[:, :, :MW].reshape(width, HALF_M))
        first = (s * C + c // 2 * 2) * rows
        window = jnp.mod(first - SHIFT, rows * S * C) // WINDOW_BINS
        is_h = jnp.sum(jnp.where(jnp.arange(species.shape[0], dtype=jnp.int32) == window, species, 0)) == 0
        human = jnp.where(is_h, human.reshape(width, 2 * HALF_H)[:, :HUMAN], 0.0)
        mouse = jnp.where(is_h, 0.0, mouse.reshape(width, 2 * HALF_M)[:, :MOUSE])
        head_weight_grad = lax.psum_scatter(
            jnp.concatenate([human, mouse], axis=1), ("seq", "ch"), scatter_dimension=0, tiled=True
        )
    if fused:
        names = list(vars(o))
        o = types.SimpleNamespace(**dict(zip(names, handed_on(list(vars(o).values())), strict=True)))
        cwg, mwg, head_weight_grad = o.cwg, o.mwg, o.hg
    return (
        o.out,
        o.ig,
        o.g1,
        o.b1,
        jnp.transpose(cwg, (0, 2, 1)),
        o.g2,
        o.b2,
        mwg,
        head_weight_grad,
        o.hb,
    )


def solution(mesh):
    rows = P(("seq", "ch"), None)
    in_specs = (
        rows, P(), P(), P(None, None, "ch"), P("ch"), P("ch"), P("ch", None), P("ch", None), P(), P(), rows,
    )
    out_specs = (
        rows, rows, P(), P(), P(None, None, "ch"), P("ch"), P("ch"), P("ch", None), rows, P(),
    )
    return jax.shard_map(on_device, mesh=mesh, in_specs=in_specs, out_specs=out_specs, check_vma=False)
```
